32 devices in a mesh: groups: 2 (over y), tile: 4 (over z), tracer: 4 (over x, core).
Axes of the slice: x: 2, y: 2, z: 4, core: 2. Of those that a mesh axis runs over, the one named last changes fastest.
Arguments:
- species_amounts: float32 [64, 32, 128, 128], P(('groups', 'tracer'), None, 'tile'), parts along dimension 0, may hold values from 0.2 to 2
- face_currents: float32 [2, 64, 128, 128], P(None, 'groups', 'tile'), parts along dimension 1, may hold values from -1 to 1
- thermal_anomaly: float32 [64, 128, 128], P(('groups', 'tracer'), 'tile'), parts along dimension 0, may hold values from -4 to 4
- layer_total_per_profile: int32 [256, 128], P(('groups', 'tile')), parts along dimension 0, may hold values from 0 to 32
- consumed_species: int32 [32], replicated, may hold values from 0 to 31, each once
- attenuation_factor: float32 [32], replicated, may hold values from 0.009375 to 0.09375
- intake_speedup: float32 [32], replicated, may hold values from 0.3 to 3
- incoming_sunshine: float32 [256, 128], P(('groups', 'tile')), parts along dimension 0, may hold values from 0.5 to 2
Outputs:
- tracers_out: float32 [64, 32, 128, 128], P('groups', 'tracer', 'tile'), parts along dimension 0
- velocity_out: float32 [2, 64, 128, 128], P(None, ('groups', 'tracer'), 'tile'), parts along dimension 1
- temperature_out: float32 [64, 128, 128], P(('groups', 'tracer'), 'tile'), parts along dimension 0
The draws below stay inside these ranges and needn't reach their ends.
There are 2 independent parts, one for each index of `groups`. The reference program is written for one: setup_inputs(seed, part) draws one part's arguments, and reference() takes and returns one part's arrays. A program takes and returns all parts, laid end to end along the dimension named above; an argument that names none is the same for every part. Nothing has to cross between parts.
Inputs may be any that keep to these rules, and one draw needn't show every extreme that they name: Levels 0 to layer_total_per_profile - 1 of a column are sea, deeper levels are land; 0 marks a land column. `consumed_species`: A permutation of the 32 tracers.
All inputs are finite; a program needn't handle non-finite values.
Results may differ from the reference program's by a relative error of at most 0.0003.
Values sent between devices are 32-bit elements; how exact they have to be, the bound alone decides.
A program may use at most 64 MiB of HBM per device.

```python
import math
import jax
import jax.numpy as jnp
from jax import lax

NTR = 32
DEPTH_LAYERS = 32
GRID_MERIDIONAL = 128
GRID_ZONAL = 128


def place_ends(entries, rng, smallest, largest):
    extent = entries.shape
    place = [jax.random.randint(jax.random.fold_in(rng, axis), (), 0, extent[axis]) for axis in range(len(extent))]
    entries = entries.at[tuple(place)].set(smallest)
    longest = extent.index(max(extent))
    place[longest] = (place[longest] + 1) % extent[longest]
    return entries.at[tuple(place)].set(largest)


def level_of(rng, shape, shards, least, largest):
    loudness = 1.0
    for axis_at, parts in shards:
        draws = jax.random.uniform(jax.random.fold_in(jax.random.fold_in(rng, 6), axis_at), (parts,), jnp.float32, least / len(shards), largest / len(shards))
        loudness = loudness * jnp.repeat(jnp.exp(draws), shape[axis_at] // parts).reshape((-1,) + (1,) * (len(shape) - 1 - axis_at))
    return loudness


def scatter_about(stream_key, dims, deviation, bound, pieces=(), held_as=jnp.bfloat16):
    loudness = level_of(stream_key, dims, pieces, -0.22, 0.18) if pieces else 1.0
    array = jax.random.normal(stream_key, dims, jnp.float32) * deviation * loudness
    return jnp.minimum(jnp.maximum(array, -bound), bound).astype(held_as)


def setup_inputs(seed: int = 0, part: int = 0) -> dict:
    key_list = jax.random.split(jax.random.key(seed), 9)
    part_splits = jax.random.split(jax.random.fold_in(key_list[8], part), 9)
    return {
        "species_amounts": jnp.clip(jnp.exp(math.log(2.0) - 2.3025851 * jax.random.uniform(part_splits[0], (NTR, DEPTH_LAYERS, GRID_ZONAL, GRID_MERIDIONAL), jnp.float32) ** level_of(part_splits[0], (NTR, DEPTH_LAYERS, GRID_ZONAL, GRID_MERIDIONAL), ((0, 4), (2, 4)), -0.2, 0.2)), 0.2, 2.0),
        "face_currents": jnp.clip(jax.random.uniform(part_splits[1], (2, DEPTH_LAYERS, GRID_ZONAL, GRID_MERIDIONAL), jnp.float32, -1.0, 1.0) * level_of(part_splits[1], (2, DEPTH_LAYERS, GRID_ZONAL, GRID_MERIDIONAL), ((2, 4),), -0.4, 0.0), -1.0, 1.0),
        "thermal_anomaly": scatter_about(part_splits[2], (DEPTH_LAYERS, GRID_ZONAL, GRID_MERIDIONAL), 1.0, 4.0, ((0, 4), (1, 4)), jnp.float32),
        "layer_total_per_profile": place_ends(jax.random.randint(part_splits[3], (GRID_ZONAL, GRID_MERIDIONAL), 0, DEPTH_LAYERS + 1), jax.random.fold_in(part_splits[3], 1), 0, DEPTH_LAYERS).astype(jnp.int32),
        "consumed_species": jax.random.permutation(key_list[4], NTR).astype(jnp.int32),
        "attenuation_factor": jnp.clip(jnp.exp(jax.random.uniform(key_list[5], (NTR,), jnp.float32, math.log(0.009375), math.log(0.09375))), 0.009375, 0.09375),
        "intake_speedup": jnp.clip(jnp.exp(jax.random.uniform(key_list[6], (NTR,), jnp.float32, math.log(0.3), math.log(3.0))), 0.3, 3.0),
        "incoming_sunshine": jnp.clip(jnp.exp(math.log(2.0) - 1.3862944 * jax.random.uniform(part_splits[7], (GRID_ZONAL, GRID_MERIDIONAL), jnp.float32) ** level_of(part_splits[7], (GRID_ZONAL, GRID_MERIDIONAL), ((0, 4),), -0.2, 0.2)), 0.5, 2.0),
    }


sub_step = 0.45
step_duration = 0.2
gravity = 0.5
viscosity = 0.2
coriolis_base = 0.5
beta_plane = 0.5
spreading_coefficient = 0.2
water_clear = 0.05
column_optical = 3.0
warming_coefficient = 5.0
light_half = 0.3
nutrient_half = 0.5


def wraparound_border(values, margin, along):
    length = values.shape[along]
    leading = lax.slice_in_dim(values, length - margin, length, axis=along)
    trailing = lax.slice_in_dim(values, 0, margin, axis=along)
    return jnp.concatenate([leading, values, trailing], axis=along)


def shift_south(values):
    return jnp.concatenate([jnp.zeros_like(values[..., :1]), values[..., :-1]], axis=-1)


def shift_north(values, offset=1):
    return jnp.concatenate([values[..., offset:], jnp.zeros_like(values[..., :offset])], axis=-1)


def wet_levels(depth_ext, first_level, level_count):
    levels = first_level + jnp.arange(level_count, dtype=jnp.int32)
    return (levels[:, None, None] < depth_ext[None]).astype(jnp.float32)


def limiter(left_slope, right_slope):
    smaller = jnp.minimum(jnp.abs(left_slope), jnp.abs(right_slope))
    return jnp.where(left_slope * right_slope > 0.0, jnp.sign(left_slope) * smaller, 0.0)


def face_flux(behind, centre, forward, beyond, speed):
    positive = speed * (centre + 0.5 * limiter(centre - behind, forward - centre))
    negative = speed * (forward - 0.5 * limiter(forward - centre, beyond - forward))
    return jnp.where(speed > 0.0, positive, negative)


def face_speeds(velocity_with_halo_border, wet_ext):
    east_speed = velocity_with_halo_border[0][:, :-1] * wet_ext[:, :-1] * wet_ext[:, 1:]
    north_speed = velocity_with_halo_border[1] * wet_ext * shift_north(wet_ext)
    return east_speed, north_speed


def flux_substep(extended, east_speed, north_speed):
    length = extended.shape[2]
    east_flux = face_flux(extended[:, :, 0:length - 3], extended[:, :, 1:length - 2],
                          extended[:, :, 2:length - 1], extended[:, :, 3:length],
                          east_speed[:, 1:length - 2])
    middle = extended[:, :, 2:length - 2]
    north_flux = face_flux(shift_south(middle), middle, shift_north(middle), shift_north(middle, 2),
                           north_speed[:, 2:length - 2])
    spread = (east_flux[:, :, 1:] - east_flux[:, :, :-1]) + (north_flux - shift_south(north_flux))
    return middle - sub_step * spread


def laplacian(values):
    inner = values[:, 1:-1]
    return values[:, 2:] + values[:, :-2] + shift_north(inner) + shift_south(inner) - 4.0 * inner


def velocity_advance(flow_one, marine_mask_profile, thermal_profile_alone):
    east_vel = flow_one[0]
    north_vel = flow_one[1]
    ocean_profiles = east_vel.shape[1] - 2
    coriolis_y = coriolis_base + beta_plane * jnp.arange(east_vel.shape[2], dtype=jnp.float32) / east_vel.shape[2]
    centre_u = east_vel[:, 1:ocean_profiles + 1]
    centre_v = north_vel[:, 1:ocean_profiles + 1]
    v_bar = 0.25 * (centre_v + north_vel[:, 2:] + shift_south(centre_v) + shift_south(north_vel[:, 2:]))
    u_bar = 0.25 * (centre_u + east_vel[:, :-2] + shift_north(centre_u) + shift_north(east_vel[:, :-2]))
    marine_mask_interior = marine_mask_profile[:, 1:ocean_profiles + 1]
    east_open = marine_mask_interior * marine_mask_profile[:, 2:]
    north_open = marine_mask_interior * shift_north(marine_mask_interior)
    heat_mid = thermal_profile_alone[:, 1:ocean_profiles + 1]
    new_east = east_open * (centre_u + step_duration * (coriolis_y * v_bar - gravity * (thermal_profile_alone[:, 2:] - heat_mid)
                                                    + viscosity * laplacian(east_vel)))
    new_north = north_open * (centre_v + step_duration * (-coriolis_y * u_bar - gravity * (shift_north(heat_mid) - heat_mid)
                                                      + viscosity * laplacian(north_vel)))
    return jnp.stack([new_east, new_north]), laplacian(thermal_profile_alone)


def optical_thickness(by_cells, attenuation_factor):
    summed = jnp.tensordot(attenuation_factor, jnp.abs(by_cells), axes=1, precision=lax.Precision.HIGHEST)
    return (water_clear + summed) * (column_optical / DEPTH_LAYERS)


def react(by_cells, optical, overhead, wet_mask, incoming_sunshine, intake_speedup, consumed_species):
    depth_tau = overhead[None] + (jnp.cumsum(optical, axis=0) - optical)
    reaching = incoming_sunshine[None] * jnp.exp(-depth_tau)
    absorbed_part = 1.0 - jnp.exp(-optical)
    captured_radiance = reaching * absorbed_part * wet_mask
    mean_light = reaching * absorbed_part / optical
    light_limit = mean_light / (mean_light + light_half)
    pairing = (consumed_species[:, None] == jnp.arange(by_cells.shape[0], dtype=jnp.int32)[None]).astype(jnp.float32)
    nutrient = jnp.tensordot(pairing, by_cells, axes=1, precision=lax.Precision.HIGHEST)
    uptake = intake_speedup[:, None, None, None] * light_limit[None] * by_cells * nutrient / (nutrient_half + jnp.abs(nutrient))
    consumed = jnp.tensordot(pairing.T, uptake, axes=1, precision=lax.Precision.HIGHEST)
    updated = by_cells + wet_mask[None] * (uptake - consumed)
    return updated, captured_radiance


def reference(species_amounts, face_currents, thermal_anomaly, layer_total_per_profile, consumed_species, attenuation_factor, intake_speedup, incoming_sunshine):
    wet_ext = wet_levels(wraparound_border(layer_total_per_profile, 2, 0), 0, DEPTH_LAYERS)
    velocity_with_halo_border = wraparound_border(face_currents, 2, 2)
    east_speed, north_speed = face_speeds(velocity_with_halo_border, wet_ext)

    def advect_one(single):
        values = single[None]
        for repeat in range(2):
            values = flux_substep(wraparound_border(values, 2, 2), east_speed, north_speed)
        return values[0]

    advected = lax.map(advect_one, species_amounts)
    marine_mask_profile = wet_ext[:, 1:-1]
    advanced_face_speeds, thermal_second_derivative = velocity_advance(velocity_with_halo_border[:, :, 1:-1], marine_mask_profile, wraparound_border(thermal_anomaly, 1, 1))
    marine_mask_interior = marine_mask_profile[:, 1:-1]
    optical = optical_thickness(advected, attenuation_factor)
    overhead = jnp.zeros(optical.shape[1:], jnp.float32)
    updated, captured_radiance = react(advected, optical, overhead, marine_mask_interior, incoming_sunshine, intake_speedup, consumed_species)
    advanced_thermal_field = marine_mask_interior * (thermal_anomaly + step_duration * spreading_coefficient * thermal_second_derivative + warming_coefficient * captured_radiance)
    return updated, advanced_face_speeds, advanced_thermal_field
```

```python
import functools

import jax
import jax.numpy as jnp
from jax import lax
from jax.experimental import pallas as pl
from jax.experimental.pallas import tpu as pltpu
from jax.sharding import PartitionSpec as P

MESH = pl.DeviceIdType.MESH

sub_step = 0.45
step_duration = 0.2
gravity = 0.5
viscosity = 0.2
coriolis_base = 0.5
beta_plane = 0.5
spreading_coefficient = 0.2
water_clear = 0.05
column_optical = 3.0
warming_coefficient = 5.0
light_half = 0.3
nutrient_half = 0.5

PAD = 8
EDGE = 4
TILE = 8


def lane_index(shape):
    return lax.broadcasted_iota(jnp.int32, shape, len(shape) - 1)


def east(x):
    return pltpu.roll(x, x.shape[0] - 1, 0)


def west(x):
    return pltpu.roll(x, 1, 0)


def north(x):
    return jnp.where(lane_index(x.shape) == x.shape[1] - 1, 0.0, pltpu.roll(x, x.shape[1] - 1, 1))


def south(x):
    return jnp.where(lane_index(x.shape) == 0, 0.0, pltpu.roll(x, 1, 1))


def minmod(a, b):
    return jnp.maximum(jnp.minimum(a, b), 0.0) + jnp.minimum(jnp.maximum(a, b), 0.0)


def laplacian(x):
    return east(x) + west(x) + north(x) + south(x) - 4.0 * x


def substep(c, es, ns, lane):
    last = c.shape[1] - 1
    d = east(c) - c
    half = 0.5 * minmod(west(d), d)
    flux = es * jnp.where(es > 0.0, c + half, east(c - half))
    spread = flux - west(flux)
    d = jnp.where(lane == last, 0.0, pltpu.roll(c, last, 1)) - c
    half = 0.5 * minmod(jnp.where(lane == 0, c, pltpu.roll(d, 1, 1)), d)
    flux = ns * jnp.where(ns > 0.0, c + half, pltpu.roll(c - half, last, 1))
    return c - (spread + (flux - pltpu.roll(flux, 1, 1)))


def react_level(count, level, depth, sun, tau, cells, c, eaten, eater, att, rate, scale, sat, pull, put):
    total = jnp.full(depth.shape, water_clear, jnp.float32)
    for t in range(count):
        x = cells[t, c]
        size = jnp.abs(x)
        total = total + att[t] * size
        sat[t] = x / (nutrient_half + size)
        pull[t] = rate[t] * x
    optical = total * scale
    wet = jnp.where(level < depth, 1.0, 0.0)
    caught = sun * jnp.exp(-tau) * (1.0 - jnp.exp(-optical))
    mean_light = caught / optical
    gain = wet * (mean_light / (mean_light + light_half))
    for t in range(count):
        change = pull[t] * sat[eaten[t]] - pull[eater[t]] * sat[t]
        put(t, cells[t, c] + gain * change)
    return wet, caught, tau + optical


def transport_kernel(
    tiles, ranks, cores, q,
    sp, fc, th, dep, sun, eaten, att, rate,
    cells, vel, heat, aux,
    ext, fext, hext, dext, adv, tot, pre, over, sat, pull, eater,
    h_send, h_recv, f_send, f_recv, s_send, s_recv,
    d_send, d_recv, i_send, i_recv, e_send, e_recv, o_send, o_recv,
    l_sem, lf_sem, ls_sem,
):
    nt, nl, rows, width = sp.shape
    per = nl // ranks
    nc = per // q
    count = ranks * nt
    chips = ranks // cores
    cross = ranks - cores
    full = rows + 2 * PAD
    r = lax.axis_index("tracer")
    z = lax.axis_index("tile")
    a, b = r // cores, lax.rem(r, cores)
    up, down = lax.rem(z + 1, tiles), lax.rem(z + tiles - 1, tiles)

    def target(s):
        ka, kb = lax.rem(1 + s // cores, chips), cores - 1 - lax.rem(s, cores)
        return lax.rem(a + ka, chips) * cores + lax.rem(b + kb, cores)

    def source(s):
        ka, kb = lax.rem(1 + s // cores, chips), cores - 1 - lax.rem(s, cores)
        return lax.rem(a + chips - ka, chips) * cores + lax.rem(b + cores - kb, cores)

    def first_level(s, c):
        return target(s) * per + c * q

    mine = pl.ds(r * nt, nt)
    low_rows = pl.ds(0, EDGE)
    high_rows = pl.ds(rows - EDGE, EDGE)
    from_low = pl.ds(PAD - EDGE, EDGE)
    from_high = pl.ds(PAD + rows, EDGE)
    body = pl.ds(PAD, rows)
    inner = pl.ds(TILE, rows - 2 * TILE)

    def pair(src, dst, lead, send, recv, at):
        return (
            pltpu.make_async_remote_copy(
                src.at[lead + (high_rows,)], dst.at[lead + (from_low,)],
                send.at[at + (0,)], recv.at[at + (0,)],
                device_id={"tile": up}, device_id_type=MESH,
            ),
            pltpu.make_async_remote_copy(
                src.at[lead + (low_rows,)], dst.at[lead + (from_high,)],
                send.at[at + (1,)], recv.at[at + (1,)],
                device_id={"tile": down}, device_id_type=MESH,
            ),
        )

    def edges(s, c):
        n = s * nc + c
        lead = (slice(None), pl.ds(first_level(s, c), q))
        return (
            pair(fc, fext, lead, f_send, f_recv, (n,))
            + pair(sp, ext, lead, h_send, h_recv, (n,))
        )

    def heat_edges():
        return pair(th, hext, (slice(None),), s_send, s_recv, (0,))

    def depth_edges():
        return pair(dep, dext, (), s_send, s_recv, (1,))

    def local(s, c):
        n = s * nc + c
        lev = pl.ds(first_level(s, c), q)
        return (
            pltpu.make_async_copy(fc.at[:, lev], fext.at[:, lev, body], lf_sem.at[n]),
            pltpu.make_async_copy(sp.at[:, lev], ext.at[:, lev, body], l_sem.at[n]),
        )

    def block_copy(s, c, rank):
        n = s * nc + c
        return pltpu.make_async_remote_copy(
            adv.at[:, pl.ds(first_level(s, c), q)],
            cells.at[pl.ds(rank * nt, nt), pl.ds(c * q, q)],
            d_send.at[n], d_recv.at[n],
            device_id={"tracer": target(s)}, device_id_type=MESH,
        )

    def inner_copy(s, i, rank):
        return pltpu.make_async_remote_copy(
            adv.at[:, first_level(s, 0) + i, inner],
            cells.at[pl.ds(rank * nt, nt), i, inner],
            i_send.at[s, i], i_recv.at[s, i],
            device_id={"tracer": target(s)}, device_id_type=MESH,
        )

    def outer_copy(s, side, rank):
        part = pl.ds(side * (rows - TILE), TILE)
        return pltpu.make_async_remote_copy(
            adv.at[:, pl.ds(first_level(s, 0), q), part],
            cells.at[pl.ds(rank * nt, nt), pl.ds(0, q), part],
            e_send.at[s, side], e_recv.at[s, side],
            device_id={"tracer": target(s)}, device_id_type=MESH,
        )

    def over_copy(s, place):
        return pltpu.make_async_remote_copy(
            pre.at[target(s)], over.at[place], o_send.at[s], o_recv.at[s],
            device_id={"tracer": target(s)}, device_id_type=MESH,
        )

    def in_cross(m):
        return lax.rem(m, cross), m // cross

    def in_near(m):
        return cross + m // nc, lax.rem(m, nc)

    barrier = pltpu.get_barrier_semaphore()
    for place in (up, down):
        pl.semaphore_signal(barrier, inc=1, device_id={"tile": place}, device_id_type=MESH)
    for s in range(ranks - 1):
        pl.semaphore_signal(barrier, inc=1, device_id={"tracer": target(s)}, device_id_type=MESH)

    dep_local = pltpu.make_async_copy(dep, dext.at[body], ls_sem.at[0])
    th_local = pltpu.make_async_copy(th, hext.at[:, body], ls_sem.at[1])
    sun_local = pltpu.make_async_copy(sun, aux.at[1], ls_sem.at[2])
    dep_local.start()

    def start_local(order):
        def step(m, carry):
            for copy in local(*order(m)):
                copy.start()
            return carry
        return step

    lax.fori_loop(0, cross * nc, start_local(in_cross), 0)
    lax.fori_loop(0, cores * nc, start_local(in_near), 0)
    th_local.start()
    sun_local.start()

    tot[...] = jnp.zeros_like(tot)
    dep_local.wait()

    def advect(lev, block, base, size, skip, first, keep, put):
        window = pl.ds(base, size)
        kept = pl.ds(first, keep)
        lane = lane_index((size, width))
        wet = jnp.where(lev < dext[window], 1.0, 0.0)
        es = sub_step * (fext[0, lev, window] * wet * east(wet))
        ns = sub_step * (fext[1, lev, window] * wet * north(wet))

        def one_tracer(t, acc):
            c = substep(ext[t, lev, window], es, ns, lane)
            c = substep(c, es, ns, lane)[skip:skip + keep]
            put(t, lev, kept, c)
            return acc + att[r * nt + t] * jnp.abs(c)

        tot[block, kept] = lax.fori_loop(0, nt, one_tracer, tot[block, kept], unroll=True)

    def put_adv(t, lev, kept, c):
        adv[t, lev, kept] = c

    def put_cells(t, lev, kept, c):
        cells[r * nt + t, lev - r * per, kept] = c

    def advance_inner(s, i):
        lev = first_level(s, 0) + i
        advect(lev, target(s), PAD, rows, TILE, TILE, rows - 2 * TILE, put_adv)

    def advance_outer(s, i, side):
        lev = first_level(s, 0) + i
        base = pl.multiple_of(side * (rows - PAD), TILE)
        first = pl.multiple_of(side * (rows - TILE), TILE)
        advect(lev, target(s), base, TILE + 2 * PAD, PAD, first, TILE, put_adv)

    def wait_local(s, c):
        for copy in local(s, c):
            copy.wait()

    def advance(s, c, put):
        wait_local(s, c)
        for copy in edges(s, c):
            copy.wait_recv()
        block = target(s)
        level_0 = first_level(s, c)

        def one_level(i, carry):
            advect(level_0 + i, block, 0, full, PAD, 0, rows, put)
            return carry

        lax.fori_loop(0, q, one_level, 0)

    def start_edges(order):
        def step(m, carry):
            for copy in edges(*order(m)):
                copy.start()
            return carry
        return step

    def inner_step(m, carry):
        s, i = m // q, lax.rem(m, q)

        @pl.when(i == 0)
        def _():
            wait_local(s, 0)

        advance_inner(s, i)

        @pl.when(m == 0)
        def _():
            pl.semaphore_wait(barrier, 2 + ranks - 1)
            for copy in depth_edges():
                copy.start()

        inner_copy(s, i, r).start()

        @pl.when(m == 0)
        def _():
            lax.fori_loop(0, cross, start_edges(in_cross), 0)

        return carry

    lax.fori_loop(0, cross * q, inner_step, 0)
    lax.fori_loop(cross, cross * nc, start_edges(in_cross), 0)
    lax.fori_loop(0, cores * nc, start_edges(in_near), 0)
    for copy in heat_edges():
        copy.start()
    for copy in depth_edges():
        copy.wait()

    def outer_step(s, carry):
        for copy in edges(s, 0):
            copy.wait_recv()

        def part(m, carry):
            advance_outer(s, lax.rem(m, q), m // q)
            return carry

        lax.fori_loop(0, 2 * q, part, 0)
        for side in range(2):
            outer_copy(s, side, r).start()
        return carry

    lax.fori_loop(0, cross, outer_step, 0)

    def away_step(m, carry):
        far = m < cross * nc
        k = m - cross * nc
        s = jnp.where(far, lax.rem(m, cross), cross + k // nc)
        c = jnp.where(far, m // cross, lax.rem(k, nc))
        advance(s, c, put_adv)

        @pl.when(jnp.logical_or(jnp.logical_not(far), c < nc - 1))
        def _():
            block_copy(s, c, r).start()

        return carry

    lax.fori_loop(cross, (ranks - 1) * nc, away_step, 0)

    def own_step(c, carry):
        advance(ranks - 1, c, put_cells)
        return carry

    lax.fori_loop(0, nc, own_step, 0)

    above = jnp.zeros((rows, width), jnp.float32)
    for place in range(ranks):
        pre[place] = above
        above = above + tot[place]
    for s in range(ranks - 1):
        over_copy(s, r).start()

    def late_step(s, carry):
        block_copy(s, nc - 1, r).start()
        return carry

    lax.fori_loop(0, cross, late_step, 0)

    th_local.wait()
    sun_local.wait()
    for copy in heat_edges():
        copy.wait()
    lane = lane_index((full, width))
    coriolis = coriolis_base + beta_plane * lane.astype(jnp.float32) / width

    def momentum(i, carry):
        lev = r * per + i
        u, v, heat_ext = fext[0, lev], fext[1, lev], hext[i]
        wet = jnp.where(lev < dext[...], 1.0, 0.0)
        v_east, u_west = east(v), west(u)
        v_bar = 0.25 * (v + v_east + south(v) + south(v_east))
        u_bar = 0.25 * (u + u_west + north(u) + north(u_west))
        new_u = u + step_duration * (
            coriolis * v_bar - gravity * (east(heat_ext) - heat_ext) + viscosity * laplacian(u)
        )
        new_v = v + step_duration * (
            -coriolis * u_bar - gravity * (north(heat_ext) - heat_ext) + viscosity * laplacian(v)
        )
        vel[0, i] = (wet * east(wet) * new_u)[PAD:PAD + rows]
        vel[1, i] = (wet * north(wet) * new_v)[PAD:PAD + rows]
        warmer = heat_ext + step_duration * spreading_coefficient * laplacian(heat_ext)
        heat[i] = warmer[PAD:PAD + rows]
        return carry

    lax.fori_loop(0, per, momentum, 0)

    def invert(s, carry):
        who = jnp.int32(0)
        for t in range(count):
            who = jnp.where(eaten[t] == s, jnp.int32(t), who)
        eater[s] = who
        return carry

    lax.fori_loop(0, count, invert, 0)

    depth = dext[PAD:PAD + rows].astype(jnp.float32)
    aux[2] = depth
    scale = column_optical / nl
    above = pre[r]
    for s in range(ranks - 1):
        over_copy(s, source(s)).wait_recv()
        above = above + over[source(s)]
    aux[0] = (above + (r * per).astype(jnp.float32) * water_clear) * scale

    def wait_far(c):
        def step(s, carry):
            block_copy(s, c, source(s)).wait_recv()
            return carry
        return step

    def react_chunk(c, carry):
        @pl.when(c == 0)
        def _():
            for s in range(cross):
                for i in range(q):
                    inner_copy(s, i, source(s)).wait_recv()
                for side in range(2):
                    outer_copy(s, side, source(s)).wait_recv()
            lax.fori_loop(cross, ranks - 1, wait_far(0), 0)

        @pl.when(c > 0)
        def _():
            lax.fori_loop(0, ranks - 1, wait_far(c), 0)

        def one_level(j, carry):
            i = c * q + j

            def put(t, x):
                cells[t, i] = x

            level = (r * per + i).astype(jnp.float32)
            wet, caught, below = react_level(
                count, level, aux[2], aux[1], aux[0], cells, i,
                eaten, eater, att, rate, scale, sat, pull, put,
            )
            aux[0] = below
            heat[i] = wet * (heat[i] + warming_coefficient * (caught * wet))
            return carry

        lax.fori_loop(0, q, one_level, 0)
        return carry

    lax.fori_loop(0, nc - 1, react_chunk, 0)

    def drain_edges(m, carry):
        for copy in edges(m // nc, lax.rem(m, nc)):
            copy.wait_send()
        return carry

    lax.fori_loop(0, ranks * nc, drain_edges, 0)
    for s in range(ranks - 1):
        over_copy(s, r).wait_send()
    for s in range(cross):
        for i in range(q):
            inner_copy(s, i, r).wait_send()
        for side in range(2):
            outer_copy(s, side, r).wait_send()

    def drain_far(m, carry):
        block_copy(lax.rem(m, cross), m // cross, r).wait_send()
        return carry

    lax.fori_loop(cross, cross * nc, drain_far, 0)

    def drain_near(m, carry):
        block_copy(cross + m // nc, lax.rem(m, nc), r).wait_send()
        return carry

    lax.fori_loop(0, (cores - 1) * nc, drain_near, 0)
    lax.fori_loop(0, ranks - 1, wait_far(nc - 1), 0)


def finish_kernel(
    levels, q,
    cells, vel, heat, aux, eaten, att, rate,
    out, vel_out, temp_out,
    last, warm, sat, pull, eater, sem, last_sem,
):
    count, per = cells.shape[:2]
    r = lax.axis_index("tracer")
    done = per - q
    scale = column_optical / levels
    copies = [
        pltpu.make_async_copy(cells.at[:, pl.ds(0, done)], out.at[:, pl.ds(0, done)], sem.at[0]),
        pltpu.make_async_copy(vel, vel_out, sem.at[1]),
        pltpu.make_async_copy(heat.at[pl.ds(0, done)], temp_out.at[pl.ds(0, done)], sem.at[2]),
    ]
    for copy in copies:
        copy.start()
    for t in range(count):
        eater[eaten[t]] = t

    def level_copy(j):
        return pltpu.make_async_copy(last.at[j], out.at[:, done + j], last_sem.at[j])

    def one_level(j, tau):
        def put(t, x):
            last[j, t] = x

        level = (r * per + done + j).astype(jnp.float32)
        wet, caught, below = react_level(
            count, level, aux[2], aux[1], tau, cells, done + j,
            eaten, eater, att, rate, scale, sat, pull, put,
        )
        warm[j] = wet * (heat[done + j] + warming_coefficient * (caught * wet))
        level_copy(j).start()
        return below

    lax.fori_loop(0, q, one_level, aux[0])
    warm_copy = pltpu.make_async_copy(warm, temp_out.at[pl.ds(done, q)], sem.at[3])
    warm_copy.start()
    for copy in copies:
        copy.wait()
    for j in range(q):
        level_copy(j).wait()
    warm_copy.wait()


def solution(mesh):
    tiles, ranks = mesh.shape["tile"], mesh.shape["tracer"]
    cores = 2 if ranks % 2 == 0 else 1

    def on_device(
        species_amounts,
        face_currents,
        thermal_anomaly,
        layer_total_per_profile,
        consumed_species,
        attenuation_factor,
        intake_speedup,
        incoming_sunshine,
    ):
        nt, nl, rows, width = species_amounts.shape
        per = nl // ranks
        q = 2 if per % 2 == 0 else 1
        chunks = nl // q
        count = ranks * nt
        cross = ranks - cores
        full = rows + 2 * PAD
        f32 = jnp.float32
        any_space = pl.BlockSpec(memory_space=pl.ANY)
        vmem = pl.BlockSpec(memory_space=pltpu.VMEM)
        smem = pl.BlockSpec(memory_space=pltpu.SMEM)
        dma = pltpu.SemaphoreType.DMA
        cells, vel, heat, aux = pl.pallas_call(
            functools.partial(transport_kernel, tiles, ranks, cores, q),
            out_shape=(
                pltpu.VMEM((count, per, rows, width), f32),
                pltpu.VMEM((2, per, rows, width), f32),
                pltpu.VMEM((per, rows, width), f32),
                pltpu.VMEM((3, rows, width), f32),
            ),
            in_specs=[any_space] * 5 + [smem] * 3,
            out_specs=(vmem, vmem, vmem, vmem),
            scratch_shapes=[
                pltpu.VMEM((nt, nl, full, width), f32),
                pltpu.VMEM((2, nl, full, width), f32),
                pltpu.VMEM((per, full, width), f32),
                pltpu.VMEM((full, width), jnp.int32),
                pltpu.VMEM((nt, nl, rows, width), f32),
                pltpu.VMEM((ranks, rows, width), f32),
                pltpu.VMEM((ranks, rows, width), f32),
                pltpu.VMEM((ranks, rows, width), f32),
                pltpu.VMEM((count, rows, width), f32),
                pltpu.VMEM((count, rows, width), f32),
                pltpu.SMEM((count,), jnp.int32),
                dma((chunks, 2)), dma((chunks, 2)),
                dma((chunks, 2)), dma((chunks, 2)),
                dma((2, 2)), dma((2, 2)),
                dma((chunks,)), dma((chunks,)),
                dma((cross, q)), dma((cross, q)),
                dma((cross, 2)), dma((cross, 2)),
                dma((ranks,)), dma((ranks,)),
                dma((chunks,)), dma((chunks,)), dma((3,)),
            ],
            compiler_params=pltpu.CompilerParams(
                collective_id=0, has_side_effects=True, vmem_limit_bytes=48 << 20
            ),
            name="transport",
        )(
            species_amounts, face_currents, thermal_anomaly,
            layer_total_per_profile, incoming_sunshine,
            consumed_species, attenuation_factor, intake_speedup,
        )
        return pl.pallas_call(
            functools.partial(finish_kernel, nl, q),
            out_shape=(
                jax.ShapeDtypeStruct((count, per, rows, width), f32),
                jax.ShapeDtypeStruct((2, per, rows, width), f32),
                jax.ShapeDtypeStruct((per, rows, width), f32),
            ),
            in_specs=[vmem] * 4 + [smem] * 3,
            out_specs=(any_space, any_space, any_space),
            scratch_shapes=[
                pltpu.VMEM((q, count, rows, width), f32),
                pltpu.VMEM((q, rows, width), f32),
                pltpu.VMEM((count, rows, width), f32),
                pltpu.VMEM((count, rows, width), f32),
                pltpu.SMEM((count,), jnp.int32),
                dma((4,)), dma((q,)),
            ],
            compiler_params=pltpu.CompilerParams(vmem_limit_bytes=32 << 20),
            name="finish",
        )(
            cells, vel, heat, aux,
            consumed_species, attenuation_factor, intake_speedup,
        )

    return jax.shard_map(
        on_device,
        mesh=mesh,
        in_specs=(
            P(("groups", "tracer"), None, "tile", None),
            P(None, "groups", "tile", None),
            P(("groups", "tracer"), "tile", None),
            P(("groups", "tile"), None),
            P(),
            P(),
            P(),
            P(("groups", "tile"), None),
        ),
        out_specs=(
            P("groups", "tracer", "tile", None),
            P(None, ("groups", "tracer"), "tile", None),
            P(("groups", "tracer"), "tile", None),
        ),
        check_vma=False,
    )
```

```python
import functools

import jax
import jax.numpy as jnp
from jax import lax
from jax.experimental import pallas as pl
from jax.experimental.pallas import tpu as pltpu
from jax.sharding import PartitionSpec as P

MESH = pl.DeviceIdType.MESH

sub_step = 0.45
step_duration = 0.2
gravity = 0.5
viscosity = 0.2
coriolis_base = 0.5
beta_plane = 0.5
spreading_coefficient = 0.2
water_clear = 0.05
column_optical = 3.0
warming_coefficient = 5.0
light_half = 0.3
nutrient_half = 0.5

PAD = 8
EDGE = 4
TILE = 8

HBM = pltpu.HBM


def lane_index(shape):
    return lax.broadcasted_iota(jnp.int32, shape, len(shape) - 1)


def east(x):
    return pltpu.roll(x, x.shape[0] - 1, 0)


def west(x):
    return pltpu.roll(x, 1, 0)


def north(x):
    return jnp.where(lane_index(x.shape) == x.shape[1] - 1, 0.0, pltpu.roll(x, x.shape[1] - 1, 1))


def south(x):
    return jnp.where(lane_index(x.shape) == 0, 0.0, pltpu.roll(x, 1, 1))


def minmod(a, b):
    return jnp.maximum(jnp.minimum(a, b), 0.0) + jnp.minimum(jnp.maximum(a, b), 0.0)


def laplacian(x):
    return east(x) + west(x) + north(x) + south(x) - 4.0 * x


def substep(c, es, ns, lane):
    last = c.shape[1] - 1
    d = east(c) - c
    half = 0.5 * minmod(west(d), d)
    flux = es * jnp.where(es > 0.0, c + half, east(c - half))
    spread = flux - west(flux)
    d = jnp.where(lane == last, 0.0, pltpu.roll(c, last, 1)) - c
    half = 0.5 * minmod(jnp.where(lane == 0, c, pltpu.roll(d, 1, 1)), d)
    flux = ns * jnp.where(ns > 0.0, c + half, pltpu.roll(c - half, last, 1))
    return c - (spread + (flux - pltpu.roll(flux, 1, 1)))


def react_level(count, level, depth, sun, tau, cells, c, eaten, eater, att, rate, scale, sat, pull, put):
    total = jnp.full(depth.shape, water_clear, jnp.float32)
    for t in range(count):
        x = cells[t, c]
        size = jnp.abs(x)
        total = total + att[t] * size
        sat[t] = x / (nutrient_half + size)
        pull[t] = rate[t] * x
    optical = total * scale
    wet = jnp.where(level < depth, 1.0, 0.0)
    caught = sun * jnp.exp(-tau) * (1.0 - jnp.exp(-optical))
    mean_light = caught / optical
    gain = wet * (mean_light / (mean_light + light_half))
    for t in range(count):
        change = pull[t] * sat[eaten[t]] - pull[eater[t]] * sat[t]
        put(t, cells[t, c] + gain * change)
    return wet, caught, tau + optical


def transport_kernel(
    tiles, ranks, cores, q,
    sp, fc, th, dep, sun, eaten_in, att_in, rate_in,
    cells, vel, heat, aux,
    eaten, att, rate, ext, fext, hext, dext, adv, tot, pre, over, sat, pull, eater,
    h_send, h_recv, f_send, f_recv, s_send, s_recv,
    d_send, d_recv, i_send, i_recv, e_send, e_recv, o_send, o_recv,
    l_sem, lf_sem, ls_sem, t_sem,
):
    nt, nl, rows, width = sp.shape
    per = nl // ranks
    nc = per // q
    count = ranks * nt
    chips = ranks // cores
    cross = ranks - cores
    full = rows + 2 * PAD
    r = lax.axis_index("tracer")
    z = lax.axis_index("tile")
    a, b = r // cores, lax.rem(r, cores)
    up, down = lax.rem(z + 1, tiles), lax.rem(z + tiles - 1, tiles)

    def target(s):
        ka, kb = lax.rem(1 + s // cores, chips), cores - 1 - lax.rem(s, cores)
        return lax.rem(a + ka, chips) * cores + lax.rem(b + kb, cores)

    def source(s):
        ka, kb = lax.rem(1 + s // cores, chips), cores - 1 - lax.rem(s, cores)
        return lax.rem(a + chips - ka, chips) * cores + lax.rem(b + cores - kb, cores)

    def first_level(s, c):
        return target(s) * per + c * q

    mine = pl.ds(r * nt, nt)
    low_rows = pl.ds(0, EDGE)
    high_rows = pl.ds(rows - EDGE, EDGE)
    from_low = pl.ds(PAD - EDGE, EDGE)
    from_high = pl.ds(PAD + rows, EDGE)
    body = pl.ds(PAD, rows)
    inner = pl.ds(EDGE, rows - 2 * EDGE)

    def pair(src, dst, lead, send, recv, at):
        return (
            pltpu.make_async_remote_copy(
                src.at[lead + (high_rows,)], dst.at[lead + (from_low,)],
                send.at[at + (0,)], recv.at[at + (0,)],
                device_id={"tile": up}, device_id_type=MESH,
            ),
            pltpu.make_async_remote_copy(
                src.at[lead + (low_rows,)], dst.at[lead + (from_high,)],
                send.at[at + (1,)], recv.at[at + (1,)],
                device_id={"tile": down}, device_id_type=MESH,
            ),
        )

    def edges(s, c):
        n = s * nc + c
        lead = (slice(None), pl.ds(first_level(s, c), q))
        return (
            pair(fc, fext, lead, f_send, f_recv, (n,))
            + pair(sp, ext, lead, h_send, h_recv, (n,))
        )

    def heat_edges():
        return pair(th, hext, (slice(None),), s_send, s_recv, (0,))

    def depth_edges():
        return pair(dep, dext, (), s_send, s_recv, (1,))

    def local(s, c):
        n = s * nc + c
        lev = pl.ds(first_level(s, c), q)
        return (
            pltpu.make_async_copy(fc.at[:, lev], fext.at[:, lev, body], lf_sem.at[n]),
            pltpu.make_async_copy(sp.at[:, lev], ext.at[:, lev, body], l_sem.at[n]),
        )

    def block_copy(s, c, rank):
        n = s * nc + c
        return pltpu.make_async_remote_copy(
            adv.at[:, pl.ds(first_level(s, c), q)],
            cells.at[pl.ds(rank * nt, nt), pl.ds(c * q, q)],
            d_send.at[n], d_recv.at[n],
            device_id={"tracer": target(s)}, device_id_type=MESH,
        )

    def inner_copy(s, i, rank):
        return pltpu.make_async_remote_copy(
            adv.at[:, first_level(s, 0) + i, inner],
            cells.at[pl.ds(rank * nt, nt), i, inner],
            i_send.at[s, i], i_recv.at[s, i],
            device_id={"tracer": target(s)}, device_id_type=MESH,
        )

    def outer_copy(s, side, rank):
        part = pl.ds(side * (rows - EDGE), EDGE)
        return pltpu.make_async_remote_copy(
            adv.at[:, pl.ds(first_level(s, 0), q), part],
            cells.at[pl.ds(rank * nt, nt), pl.ds(0, q), part],
            e_send.at[s, side], e_recv.at[s, side],
            device_id={"tracer": target(s)}, device_id_type=MESH,
        )

    def over_copy(s, place):
        return pltpu.make_async_remote_copy(
            pre.at[target(s)], over.at[place], o_send.at[s], o_recv.at[s],
            device_id={"tracer": target(s)}, device_id_type=MESH,
        )

    def in_cross(m):
        return lax.rem(m, cross), m // cross

    def in_near(m):
        return cross + m // nc, lax.rem(m, nc)

    barrier = pltpu.get_barrier_semaphore()
    for place in (up, down):
        pl.semaphore_signal(barrier, inc=1, device_id={"tile": place}, device_id_type=MESH)
    for s in range(ranks - 1):
        pl.semaphore_signal(barrier, inc=1, device_id={"tracer": target(s)}, device_id_type=MESH)

    dep_local = pltpu.make_async_copy(dep, dext.at[body], ls_sem.at[0])
    th_local = pltpu.make_async_copy(th, hext.at[:, body], ls_sem.at[1])
    sun_local = pltpu.make_async_copy(sun, aux.at[1], ls_sem.at[2])
    tables = [
        pltpu.make_async_copy(src, dst, t_sem.at[k])
        for k, (src, dst) in enumerate(((eaten_in, eaten), (att_in, att), (rate_in, rate)))
    ]
    dep_local.start()
    tables[1].start()

    def start_local(order):
        def step(m, carry):
            for copy in local(*order(m)):
                copy.start()
            return carry
        return step

    lax.fori_loop(0, cross * nc, start_local(in_cross), 0)
    lax.fori_loop(0, cores * nc, start_local(in_near), 0)
    th_local.start()
    sun_local.start()
    tables[0].start()
    tables[2].start()

    tot[...] = jnp.zeros_like(tot)
    dep_local.wait()
    tables[1].wait()

    def advect(lev, block, base, size, skip, first, keep, put):
        window = pl.ds(base, size)
        kept = pl.ds(first, keep)
        lane = lane_index((size, width))
        wet = jnp.where(lev < dext[window], 1.0, 0.0)
        es = sub_step * (fext[0, lev, window] * wet * east(wet))
        ns = sub_step * (fext[1, lev, window] * wet * north(wet))

        def one_tracer(t, acc):
            c = substep(ext[t, lev, window], es, ns, lane)
            c = substep(c, es, ns, lane)[skip:skip + keep]
            put(t, lev, kept, c)
            return acc + att[r * nt + t] * jnp.abs(c)

        tot[block, kept] = lax.fori_loop(0, nt, one_tracer, tot[block, kept], unroll=True)

    def put_adv(t, lev, kept, c):
        adv[t, lev, kept] = c

    def put_cells(t, lev, kept, c):
        cells[r * nt + t, lev - r * per, kept] = c

    def advance_inner(s, i):
        lev = first_level(s, 0) + i
        advect(lev, target(s), PAD, rows, EDGE, EDGE, rows - 2 * EDGE, put_adv)

    def advance_outer(s, i, side):
        lev = first_level(s, 0) + i
        base = side * (rows - PAD)
        skip, first = (TILE + EDGE, rows - EDGE) if side else (PAD, 0)
        advect(lev, target(s), base, TILE + 2 * PAD, skip, first, EDGE, put_adv)

    def wait_local(s, c):
        for copy in local(s, c):
            copy.wait()

    def advance(s, c, put):
        wait_local(s, c)
        for copy in edges(s, c):
            copy.wait_recv()
        block = target(s)
        level_0 = first_level(s, c)

        def one_level(i, carry):
            advect(level_0 + i, block, 0, full, PAD, 0, rows, put)
            return carry

        lax.fori_loop(0, q, one_level, 0)

    def start_edges(order):
        def step(m, carry):
            for copy in edges(*order(m)):
                copy.start()
            return carry
        return step

    def inner_step(m, carry):
        s, i = m // q, lax.rem(m, q)

        @pl.when(i == 0)
        def _():
            wait_local(s, 0)

        advance_inner(s, i)

        @pl.when(m == 0)
        def _():
            pl.semaphore_wait(barrier, 2 + ranks - 1)
            for copy in depth_edges():
                copy.start()

        inner_copy(s, i, r).start()

        @pl.when(m == 0)
        def _():
            lax.fori_loop(0, cross, start_edges(in_cross), 0)

        return carry

    lax.fori_loop(0, cross * q, inner_step, 0)
    lax.fori_loop(cross, cross * nc, start_edges(in_cross), 0)
    lax.fori_loop(0, cores * nc, start_edges(in_near), 0)
    for copy in heat_edges():
        copy.start()
    for copy in depth_edges():
        copy.wait()

    def outer_step(s, carry):
        for copy in edges(s, 0):
            copy.wait_recv()

        def part(i, carry):
            for side in range(2):
                advance_outer(s, i, side)
            return carry

        lax.fori_loop(0, q, part, 0)
        for side in range(2):
            outer_copy(s, side, r).start()
        return carry

    lax.fori_loop(0, cross, outer_step, 0)

    def away_step(m, carry):
        far = m < cross * nc
        k = m - cross * nc
        s = jnp.where(far, lax.rem(m, cross), cross + k // nc)
        c = jnp.where(far, m // cross, lax.rem(k, nc))
        advance(s, c, put_adv)

        @pl.when(m != cross * nc - 1)
        def _():
            block_copy(s, c, r).start()

        return carry

    lax.fori_loop(cross, (ranks - 1) * nc, away_step, 0)

    def own_step(c, carry):
        advance(ranks - 1, c, put_cells)
        return carry

    lax.fori_loop(0, nc, own_step, 0)

    above = jnp.zeros((rows, width), jnp.float32)
    for place in range(ranks):
        pre[place] = above
        above = above + tot[place]
    for s in range(ranks - 1):
        over_copy(s, r).start()

    block_copy(cross - 1, nc - 1, r).start()

    th_local.wait()
    sun_local.wait()
    for copy in heat_edges():
        copy.wait()
    lane = lane_index((full, width))
    coriolis = coriolis_base + beta_plane * lane.astype(jnp.float32) / width

    def momentum(i, carry):
        lev = r * per + i
        u, v, heat_ext = fext[0, lev], fext[1, lev], hext[i]
        wet = jnp.where(lev < dext[...], 1.0, 0.0)
        v_east, u_west = east(v), west(u)
        v_bar = 0.25 * (v + v_east + south(v) + south(v_east))
        u_bar = 0.25 * (u + u_west + north(u) + north(u_west))
        new_u = u + step_duration * (
            coriolis * v_bar - gravity * (east(heat_ext) - heat_ext) + viscosity * laplacian(u)
        )
        new_v = v + step_duration * (
            -coriolis * u_bar - gravity * (north(heat_ext) - heat_ext) + viscosity * laplacian(v)
        )
        vel[0, i] = (wet * east(wet) * new_u)[PAD:PAD + rows]
        vel[1, i] = (wet * north(wet) * new_v)[PAD:PAD + rows]
        warmer = heat_ext + step_duration * spreading_coefficient * laplacian(heat_ext)
        heat[i] = warmer[PAD:PAD + rows]
        return carry

    lax.fori_loop(0, per, momentum, 0)

    tables[0].wait()
    tables[2].wait()

    def invert(s, carry):
        who = jnp.int32(0)
        for t in range(count):
            who = jnp.where(eaten[t] == s, jnp.int32(t), who)
        eater[s] = who
        return carry

    lax.fori_loop(0, count, invert, 0)

    depth = dext[PAD:PAD + rows].astype(jnp.float32)
    aux[2] = depth
    scale = column_optical / nl
    above = pre[r]
    for s in range(ranks - 1):
        over_copy(s, source(s)).wait_recv()
        above = above + over[source(s)]
    aux[0] = (above + (r * per).astype(jnp.float32) * water_clear) * scale

    def wait_far(c):
        def step(s, carry):
            block_copy(s, c, source(s)).wait_recv()
            return carry
        return step

    def react_chunk(c, carry):
        @pl.when(c == 0)
        def _():
            for s in range(cross):
                for i in range(q):
                    inner_copy(s, i, source(s)).wait_recv()
                for side in range(2):
                    outer_copy(s, side, source(s)).wait_recv()
            lax.fori_loop(cross, ranks - 1, wait_far(0), 0)

        @pl.when(c > 0)
        def _():
            lax.fori_loop(0, ranks - 1, wait_far(c), 0)

        def one_level(j, carry):
            i = c * q + j

            def put(t, x):
                cells[t, i] = x

            level = (r * per + i).astype(jnp.float32)
            wet, caught, below = react_level(
                count, level, aux[2], aux[1], aux[0], cells, i,
                eaten, eater, att, rate, scale, sat, pull, put,
            )
            aux[0] = below
            heat[i] = wet * (heat[i] + warming_coefficient * (caught * wet))
            return carry

        lax.fori_loop(0, q, one_level, 0)
        return carry

    lax.fori_loop(0, nc - 1, react_chunk, 0)

    def drain_edges(m, carry):
        for copy in edges(m // nc, lax.rem(m, nc)):
            copy.wait_send()
        return carry

    lax.fori_loop(0, ranks * nc, drain_edges, 0)
    for s in range(ranks - 1):
        over_copy(s, r).wait_send()
    for s in range(cross):
        for i in range(q):
            inner_copy(s, i, r).wait_send()
        for side in range(2):
            outer_copy(s, side, r).wait_send()

    def drain_far(m, carry):
        block_copy(lax.rem(m, cross), m // cross, r).wait_send()
        return carry

    lax.fori_loop(cross, cross * nc, drain_far, 0)

    def drain_near(m, carry):
        block_copy(cross + m // nc, lax.rem(m, nc), r).wait_send()
        return carry

    lax.fori_loop(0, (cores - 1) * nc, drain_near, 0)
    lax.fori_loop(0, ranks - 1, wait_far(nc - 1), 0)


def finish_kernel(
    levels, q,
    cells, vel, heat, aux, eaten, att, rate,
    out, vel_out, temp_out,
    last, warm, sat, pull, eater, sem, last_sem,
):
    count, per = cells.shape[:2]
    r = lax.axis_index("tracer")
    done = per - q
    scale = column_optical / levels
    copies = [
        pltpu.make_async_copy(cells.at[:, pl.ds(0, done)], out.at[:, pl.ds(0, done)], sem.at[0]),
        pltpu.make_async_copy(vel, vel_out, sem.at[1]),
        pltpu.make_async_copy(heat.at[pl.ds(0, done)], temp_out.at[pl.ds(0, done)], sem.at[2]),
    ]
    for copy in copies:
        copy.start()
    for t in range(count):
        eater[eaten[t]] = t

    def level_copy(j):
        return pltpu.make_async_copy(last.at[j], out.at[:, done + j], last_sem.at[j])

    def one_level(j, tau):
        def put(t, x):
            last[j, t] = x

        level = (r * per + done + j).astype(jnp.float32)
        wet, caught, below = react_level(
            count, level, aux[2], aux[1], tau, cells, done + j,
            eaten, eater, att, rate, scale, sat, pull, put,
        )
        warm[j] = wet * (heat[done + j] + warming_coefficient * (caught * wet))
        level_copy(j).start()
        return below

    lax.fori_loop(0, q, one_level, aux[0])
    warm_copy = pltpu.make_async_copy(warm, temp_out.at[pl.ds(done, q)], sem.at[3])
    warm_copy.start()
    for copy in copies:
        copy.wait()
    for j in range(q):
        level_copy(j).wait()
    warm_copy.wait()


def solution(mesh):
    tiles, ranks = mesh.shape["tile"], mesh.shape["tracer"]
    cores = 2 if ranks % 2 == 0 else 1

    def on_device(
        species_amounts,
        face_currents,
        thermal_anomaly,
        layer_total_per_profile,
        consumed_species,
        attenuation_factor,
        intake_speedup,
        incoming_sunshine,
    ):
        nt, nl, rows, width = species_amounts.shape
        per = nl // ranks
        q = 2 if per % 2 == 0 else 1
        chunks = nl // q
        count = ranks * nt
        cross = ranks - cores
        full = rows + 2 * PAD
        f32 = jnp.float32
        any_space = pl.BlockSpec(memory_space=pl.ANY)
        vmem = pl.BlockSpec(memory_space=pltpu.VMEM)
        smem = pl.BlockSpec(memory_space=pltpu.SMEM)
        dma = pltpu.SemaphoreType.DMA
        cells, vel, heat, aux = pl.pallas_call(
            functools.partial(transport_kernel, tiles, ranks, cores, q),
            out_shape=(
                pltpu.VMEM((count, per, rows, width), f32),
                pltpu.VMEM((2, per, rows, width), f32),
                pltpu.VMEM((per, rows, width), f32),
                pltpu.VMEM((3, rows, width), f32),
            ),
            in_specs=[any_space] * 8,
            out_specs=(vmem, vmem, vmem, vmem),
            scratch_shapes=[
                pltpu.SMEM((count,), jnp.int32),
                pltpu.SMEM((count,), f32),
                pltpu.SMEM((count,), f32),
                pltpu.VMEM((nt, nl, full, width), f32),
                pltpu.VMEM((2, nl, full, width), f32),
                pltpu.VMEM((per, full, width), f32),
                pltpu.VMEM((full, width), jnp.int32),
                pltpu.VMEM((nt, nl, rows, width), f32),
                pltpu.VMEM((ranks, rows, width), f32),
                pltpu.VMEM((ranks, rows, width), f32),
                pltpu.VMEM((ranks, rows, width), f32),
                pltpu.VMEM((count, rows, width), f32),
                pltpu.VMEM((count, rows, width), f32),
                pltpu.SMEM((count,), jnp.int32),
                dma((chunks, 2)), dma((chunks, 2)),
                dma((chunks, 2)), dma((chunks, 2)),
                dma((2, 2)), dma((2, 2)),
                dma((chunks,)), dma((chunks,)),
                dma((cross, q)), dma((cross, q)),
                dma((cross, 2)), dma((cross, 2)),
                dma((ranks,)), dma((ranks,)),
                dma((chunks,)), dma((chunks,)), dma((3,)), dma((3,)),
            ],
            compiler_params=pltpu.CompilerParams(
                collective_id=0, has_side_effects=True, vmem_limit_bytes=48 << 20
            ),
            name="transport",
        )(
            *(pltpu.with_memory_space_constraint(x, HBM) for x in (
                species_amounts, face_currents, thermal_anomaly,
                layer_total_per_profile, incoming_sunshine,
                consumed_species, attenuation_factor, intake_speedup,
            ))
        )
        return pl.pallas_call(
            functools.partial(finish_kernel, nl, q),
            out_shape=(
                jax.ShapeDtypeStruct((count, per, rows, width), f32),
                jax.ShapeDtypeStruct((2, per, rows, width), f32),
                jax.ShapeDtypeStruct((per, rows, width), f32),
            ),
            in_specs=[vmem] * 4 + [smem] * 3,
            out_specs=(any_space, any_space, any_space),
            scratch_shapes=[
                pltpu.VMEM((q, count, rows, width), f32),
                pltpu.VMEM((q, rows, width), f32),
                pltpu.VMEM((count, rows, width), f32),
                pltpu.VMEM((count, rows, width), f32),
                pltpu.SMEM((count,), jnp.int32),
                dma((4,)), dma((q,)),
            ],
            compiler_params=pltpu.CompilerParams(vmem_limit_bytes=32 << 20),
            name="finish",
        )(
            cells, vel, heat, aux,
            consumed_species, attenuation_factor, intake_speedup,
        )

    return jax.shard_map(
        on_device,
        mesh=mesh,
        in_specs=(
            P(("groups", "tracer"), None, "tile", None),
            P(None, "groups", "tile", None),
            P(("groups", "tracer"), "tile", None),
            P(("groups", "tile"), None),
            P(),
            P(),
            P(),
            P(("groups", "tile"), None),
        ),
        out_specs=(
            P("groups", "tracer", "tile", None),
            P(None, ("groups", "tracer"), "tile", None),
            P(("groups", "tracer"), "tile", None),
        ),
        check_vma=False,
    )
```

```python
import functools

import jax
import jax.numpy as jnp
from jax import lax
from jax.experimental import pallas as pl
from jax.experimental.pallas import tpu as pltpu
from jax.sharding import PartitionSpec as P

MESH = pl.DeviceIdType.MESH

sub_step = 0.45
step_duration = 0.2
gravity = 0.5
viscosity = 0.2
coriolis_base = 0.5
beta_plane = 0.5
spreading_coefficient = 0.2
water_clear = 0.05
column_optical = 3.0
warming_coefficient = 5.0
light_half = 0.3
nutrient_half = 0.5

PAD = 8
EDGE = 4
TILE = 8
LOW_FLOW, HIGH_FLOW = 3, 2

HBM = pltpu.HBM


def lane_index(shape):
    return lax.broadcasted_iota(jnp.int32, shape, len(shape) - 1)


def east(x):
    return pltpu.roll(x, x.shape[0] - 1, 0)


def west(x):
    return pltpu.roll(x, 1, 0)


def north(x):
    return jnp.where(lane_index(x.shape) == x.shape[1] - 1, 0.0, pltpu.roll(x, x.shape[1] - 1, 1))


def south(x):
    return jnp.where(lane_index(x.shape) == 0, 0.0, pltpu.roll(x, 1, 1))


def minmod(a, b):
    return jnp.maximum(jnp.minimum(a, b), 0.0) + jnp.minimum(jnp.maximum(a, b), 0.0)


def laplacian(x):
    return east(x) + west(x) + north(x) + south(x) - 4.0 * x


def substep(c, es, ns, lane):
    last = c.shape[1] - 1
    d = east(c) - c
    half = 0.5 * minmod(west(d), d)
    flux = es * jnp.where(es > 0.0, c + half, east(c - half))
    spread = flux - west(flux)
    d = jnp.where(lane == last, 0.0, pltpu.roll(c, last, 1)) - c
    half = 0.5 * minmod(jnp.where(lane == 0, c, pltpu.roll(d, 1, 1)), d)
    flux = ns * jnp.where(ns > 0.0, c + half, pltpu.roll(c - half, last, 1))
    return c - (spread + (flux - pltpu.roll(flux, 1, 1)))


def react_level(count, level, depth, sun, tau, cells, c, eaten, eater, att, rate, scale, sat, pull, put):
    total = jnp.full(depth.shape, water_clear, jnp.float32)
    for t in range(count):
        x = cells[t, c]
        size = jnp.abs(x)
        total = total + att[t] * size
        sat[t] = x / (nutrient_half + size)
        pull[t] = rate[t] * x
    optical = total * scale
    wet = jnp.where(level < depth, 1.0, 0.0)
    caught = sun * jnp.exp(-tau) * (1.0 - jnp.exp(-optical))
    mean_light = caught / optical
    gain = wet * (mean_light / (mean_light + light_half))
    for t in range(count):
        change = pull[t] * sat[eaten[t]] - pull[eater[t]] * sat[t]
        put(t, cells[t, c] + gain * change)
    return wet, caught, tau + optical


def transport_kernel(
    tiles, ranks, cores, q, early,
    sp, fc, th, dep, sun, eaten_in, att_in, rate_in,
    cells, vel, heat, aux,
    eaten, att, rate, ext, fext, hext, dext, adv, tot, pre, part, joined, over, sat, pull, eater,
    h_send, h_recv, f_send, f_recv, s_send, s_recv,
    d_send, d_recv, i_send, i_recv, e_send, e_recv, o_send, o_recv, p_send, p_recv,
    l_sem, lf_sem, ls_sem, t_sem, ready,
):
    nt, nl, rows, width = sp.shape
    per = nl // ranks
    nc = per // q
    count = ranks * nt
    chips = ranks // cores
    cross = ranks - cores
    full = rows + 2 * PAD
    r = lax.axis_index("tracer")
    z = lax.axis_index("tile")
    a, b = r // cores, lax.rem(r, cores)
    up, down = lax.rem(z + 1, tiles), lax.rem(z + tiles - 1, tiles)

    def target(s):
        ka, kb = lax.rem(1 + s // cores, chips), cores - 1 - lax.rem(s, cores)
        return lax.rem(a + ka, chips) * cores + lax.rem(b + kb, cores)

    def source(s):
        ka, kb = lax.rem(1 + s // cores, chips), cores - 1 - lax.rem(s, cores)
        return lax.rem(a + chips - ka, chips) * cores + lax.rem(b + cores - kb, cores)

    def first_level(s, c):
        return target(s) * per + c * q

    mine = pl.ds(r * nt, nt)
    body = pl.ds(PAD, rows)
    inner = pl.ds(EDGE, rows - 2 * EDGE)

    def pair(src, dst, lead, send, recv, at, low=EDGE, high=EDGE):
        return (
            pltpu.make_async_remote_copy(
                src.at[lead + (pl.ds(rows - low, low),)],
                dst.at[lead + (pl.ds(PAD - low, low),)],
                send.at[at + (0,)], recv.at[at + (0,)],
                device_id={"tile": up}, device_id_type=MESH,
            ),
            pltpu.make_async_remote_copy(
                src.at[lead + (pl.ds(0, high),)],
                dst.at[lead + (pl.ds(PAD + rows, high),)],
                send.at[at + (1,)], recv.at[at + (1,)],
                device_id={"tile": down}, device_id_type=MESH,
            ),
        )

    def edges(s, c):
        n = s * nc + c
        lead = (slice(None), pl.ds(first_level(s, c), q))
        return (
            pair(fc, fext, lead, f_send, f_recv, (n,), LOW_FLOW, HIGH_FLOW)
            + pair(sp, ext, lead, h_send, h_recv, (n,))
        )

    def heat_edges():
        return pair(th, hext, (slice(None),), s_send, s_recv, (0,))

    def depth_edges():
        return pair(dep, dext, (), s_send, s_recv, (1,))

    def local(s, c):
        n = s * nc + c
        lev = pl.ds(first_level(s, c), q)
        return (
            pltpu.make_async_copy(fc.at[:, lev], fext.at[:, lev, body], lf_sem.at[n]),
            pltpu.make_async_copy(sp.at[:, lev], ext.at[:, lev, body], l_sem.at[n]),
        )

    def block_copy(s, c, rank):
        n = s * nc + c
        return pltpu.make_async_remote_copy(
            adv.at[:, pl.ds(first_level(s, c), q)],
            cells.at[pl.ds(rank * nt, nt), pl.ds(c * q, q)],
            d_send.at[n], d_recv.at[n],
            device_id={"tracer": target(s)}, device_id_type=MESH,
        )

    def inner_copy(s, c, i, rank):
        return pltpu.make_async_remote_copy(
            adv.at[:, first_level(s, c) + i, inner],
            cells.at[pl.ds(rank * nt, nt), c * q + i, inner],
            i_send.at[c, s, i], i_recv.at[c, s, i],
            device_id={"tracer": target(s)}, device_id_type=MESH,
        )

    def outer_copy(s, c, side, rank):
        edge = pl.ds(side * (rows - EDGE), EDGE)
        return pltpu.make_async_remote_copy(
            adv.at[:, pl.ds(first_level(s, c), q), edge],
            cells.at[pl.ds(rank * nt, nt), pl.ds(c * q, q), edge],
            e_send.at[c, s, side], e_recv.at[c, s, side],
            device_id={"tracer": target(s)}, device_id_type=MESH,
        )

    partner = a * cores + cores - 1 - b

    def part_copy():
        return pltpu.make_async_remote_copy(
            pre.at[:, cores - 1 - b], part, p_send.at[0], p_recv.at[0],
            device_id={"tracer": partner}, device_id_type=MESH,
        )

    def over_copy(k):
        there = lax.rem(a + k, chips)
        return pltpu.make_async_remote_copy(
            joined.at[there], over.at[k - 1], o_send.at[k - 1], o_recv.at[k - 1],
            device_id={"tracer": there * cores + b}, device_id_type=MESH,
        )

    def gets_over(k):
        return lax.rem(a + k, chips) * cores + b > 0

    def in_cross(m):
        return lax.rem(m, cross), m // cross

    def in_near(m):
        return cross + m // nc, lax.rem(m, nc)

    last_core = a * cores + cores - 1
    late = b == cores - 1
    barrier = pltpu.get_barrier_semaphore()
    for s in range(cross):
        pl.semaphore_signal(barrier, inc=1, device_id={"tracer": target(s)}, device_id_type=MESH)
    if cores > 1:
        @pl.when(jnp.logical_not(late))
        def _():
            pl.semaphore_signal(barrier, inc=1, device_id={"tracer": last_core}, device_id_type=MESH)
    for place in (up, down):
        pl.semaphore_signal(
            barrier, inc=1, device_id={"tile": place, "tracer": last_core}, device_id_type=MESH
        )

    dep_local = pltpu.make_async_copy(dep, dext.at[body], ls_sem.at[0])
    th_local = pltpu.make_async_copy(th, hext.at[:, body], ls_sem.at[1])
    sun_local = pltpu.make_async_copy(sun, aux.at[1], ls_sem.at[2])
    tables = [
        pltpu.make_async_copy(src, dst, t_sem.at[k])
        for k, (src, dst) in enumerate(((eaten_in, eaten), (att_in, att), (rate_in, rate)))
    ]
    dep_local.start()
    tables[1].start()

    def start_local(order):
        def step(m, carry):
            for copy in local(*order(m)):
                copy.start()
            return carry
        return step

    lax.fori_loop(0, early * cross, start_local(in_cross), 0)

    tot[...] = jnp.zeros_like(tot)
    dep_local.wait()
    tables[1].wait()

    def advect(lev, block, base, size, skip, first, keep, put):
        window = pl.ds(base, size)
        kept = pl.ds(first, keep)
        lane = lane_index((size, width))
        wet = jnp.where(lev < dext[window], 1.0, 0.0)
        es = sub_step * (fext[0, lev, window] * wet * east(wet))
        ns = sub_step * (fext[1, lev, window] * wet * north(wet))

        def one_tracer(t, acc):
            c = substep(ext[t, lev, window], es, ns, lane)
            c = substep(c, es, ns, lane)[skip:skip + keep]
            put(t, lev, kept, c)
            return acc + att[r * nt + t] * jnp.abs(c)

        tot[block, kept] = lax.fori_loop(0, nt, one_tracer, tot[block, kept], unroll=True)

    def put_adv(t, lev, kept, c):
        adv[t, lev, kept] = c

    def put_cells(t, lev, kept, c):
        cells[r * nt + t, lev - r * per, kept] = c

    def advance_inner(s, c, i):
        lev = first_level(s, c) + i
        advect(lev, target(s), PAD, rows, EDGE, EDGE, rows - 2 * EDGE, put_adv)

    def advance_outer(s, c, i, side):
        lev = first_level(s, c) + i
        base = side * (rows - PAD)
        skip, first = (TILE + EDGE, rows - EDGE) if side else (PAD, 0)
        advect(lev, target(s), base, TILE + 2 * PAD, skip, first, EDGE, put_adv)

    def wait_local(s, c):
        for copy in local(s, c):
            copy.wait()

    def advance(s, c, put):
        wait_local(s, c)
        for copy in edges(s, c):
            copy.wait_recv()
        block = target(s)
        level_0 = first_level(s, c)

        def one_level(i, carry):
            advect(level_0 + i, block, 0, full, PAD, 0, rows, put)
            return carry

        lax.fori_loop(0, q, one_level, 0)

    def start_edges(order):
        def step(m, carry):
            for copy in edges(*order(m)):
                copy.start()
            return carry
        return step

    turn = jnp.where(late, 0, min(early * cross * q, cross * q + q) - 1)

    def inner_step(m, carry):
        k, i = m // q, lax.rem(m, q)
        s, c = in_cross(k)

        @pl.when(i == 0)
        def _():
            wait_local(s, c)

        advance_inner(s, c, i)

        @pl.when(m == 0)
        def _():
            pl.semaphore_wait(barrier, jnp.where(late, cross + cores - 1 + 2 * cores, cross))

        inner_copy(s, c, i, r).start()

        @pl.when(m == turn)
        def _():
            if cores > 1:
                @pl.when(late)
                def _():
                    pl.semaphore_signal(
                        ready, inc=1, device_id={"tracer": partner}, device_id_type=MESH
                    )

                @pl.when(jnp.logical_not(late))
                def _():
                    pl.semaphore_wait(ready, 1)

            for copy in depth_edges():
                copy.start()
            lax.fori_loop(0, cross, start_edges(in_cross), 0)

        return carry

    lax.fori_loop(0, early * cross * q, inner_step, 0)
    lax.fori_loop(cross, cross * nc, start_edges(in_cross), 0)
    lax.fori_loop(early * cross, cross * nc, start_local(in_cross), 0)
    lax.fori_loop(0, cores * nc, start_edges(in_near), 0)
    lax.fori_loop(0, cores * nc, start_local(in_near), 0)
    for copy in heat_edges():
        copy.start()
    th_local.start()
    sun_local.start()
    tables[0].start()
    tables[2].start()
    for copy in depth_edges():
        copy.wait()

    def outer_step(k, carry):
        s, c = in_cross(k)
        for copy in edges(s, c):
            copy.wait_recv()

        def sides(i, carry):
            for side in range(2):
                advance_outer(s, c, i, side)
            return carry

        lax.fori_loop(0, q, sides, 0)
        for side in range(2):
            outer_copy(s, c, side, r).start()
        return carry

    lax.fori_loop(0, early * cross, outer_step, 0)

    def away_step(m, carry):
        far = m < cross * nc
        k = m - cross * nc
        s = jnp.where(far, lax.rem(m, cross), cross + k // nc)
        c = jnp.where(far, m // cross, lax.rem(k, nc))
        advance(s, c, put_adv)

        @pl.when(m != cross * nc - 1)
        def _():
            block_copy(s, c, r).start()

        return carry

    lax.fori_loop(early * cross, (ranks - 1) * nc, away_step, 0)

    def own_step(c, carry):
        advance(ranks - 1, c, put_cells)
        return carry

    lax.fori_loop(0, nc, own_step, 0)

    above = jnp.zeros((rows, width), jnp.float32)
    for place in range(ranks):
        pre[place // cores, place % cores] = above
        above = above + tot[place]
    if cores > 1:
        part_copy().start()
        part_copy().wait()
        for k in range(chips):
            joined[k] = pre[k, b] + part[k]
    else:
        for k in range(chips):
            joined[k] = pre[k, b]
    for k in range(1, chips):
        @pl.when(gets_over(k))
        def _():
            over_copy(k).start()

    block_copy(cross - 1, nc - 1, r).start()

    th_local.wait()
    sun_local.wait()
    for copy in heat_edges():
        copy.wait()
    lane = lane_index((full, width))
    coriolis = coriolis_base + beta_plane * lane.astype(jnp.float32) / width

    def momentum(i, carry):
        lev = r * per + i
        u, v, heat_ext = fext[0, lev], fext[1, lev], hext[i]
        wet = jnp.where(lev < dext[...], 1.0, 0.0)
        v_east, u_west = east(v), west(u)
        v_bar = 0.25 * (v + v_east + south(v) + south(v_east))
        u_bar = 0.25 * (u + u_west + north(u) + north(u_west))
        new_u = u + step_duration * (
            coriolis * v_bar - gravity * (east(heat_ext) - heat_ext) + viscosity * laplacian(u)
        )
        new_v = v + step_duration * (
            -coriolis * u_bar - gravity * (north(heat_ext) - heat_ext) + viscosity * laplacian(v)
        )
        vel[0, i] = (wet * east(wet) * new_u)[PAD:PAD + rows]
        vel[1, i] = (wet * north(wet) * new_v)[PAD:PAD + rows]
        warmer = heat_ext + step_duration * spreading_coefficient * laplacian(heat_ext)
        heat[i] = warmer[PAD:PAD + rows]
        return carry

    lax.fori_loop(0, per, momentum, 0)

    tables[0].wait()
    tables[2].wait()

    def invert(s, carry):
        who = jnp.int32(0)
        for t in range(count):
            who = jnp.where(eaten[t] == s, jnp.int32(t), who)
        eater[s] = who
        return carry

    lax.fori_loop(0, count, invert, 0)

    depth = dext[PAD:PAD + rows].astype(jnp.float32)
    aux[2] = depth
    scale = column_optical / nl
    clear = (r * per).astype(jnp.float32) * water_clear

    @pl.when(r == 0)
    def _():
        aux[0] = jnp.zeros((rows, width), jnp.float32)

    @pl.when(r > 0)
    def _():
        above = joined[a]
        for k in range(1, chips):
            over_copy(k).wait_recv()
            above = above + over[k - 1]
        aux[0] = (above + clear) * scale

    def wait_far(c):
        def step(s, carry):
            block_copy(s, c, source(s)).wait_recv()
            return carry
        return step

    def react_chunk(c, carry):
        @pl.when(c < early)
        def _():
            def first_parts(s, carry):
                for i in range(q):
                    inner_copy(s, c, i, source(s)).wait_recv()
                for side in range(2):
                    outer_copy(s, c, side, source(s)).wait_recv()
                return carry

            lax.fori_loop(0, cross, first_parts, 0)
            lax.fori_loop(cross, ranks - 1, wait_far(c), 0)

        @pl.when(c >= early)
        def _():
            lax.fori_loop(0, ranks - 1, wait_far(c), 0)

        def one_level(j, carry):
            i = c * q + j

            def put(t, x):
                cells[t, i] = x

            level = (r * per + i).astype(jnp.float32)
            wet, caught, below = react_level(
                count, level, aux[2], aux[1], aux[0], cells, i,
                eaten, eater, att, rate, scale, sat, pull, put,
            )
            aux[0] = below
            heat[i] = wet * (heat[i] + warming_coefficient * (caught * wet))
            return carry

        lax.fori_loop(0, q, one_level, 0)
        return carry

    lax.fori_loop(0, nc - 1, react_chunk, 0)

    def drain_edges(m, carry):
        for copy in edges(m // nc, lax.rem(m, nc)):
            copy.wait_send()
        return carry

    lax.fori_loop(0, ranks * nc, drain_edges, 0)
    for k in range(1, chips):
        @pl.when(gets_over(k))
        def _():
            over_copy(k).wait_send()

    def drain_first(k, carry):
        s, c = in_cross(k)
        for i in range(q):
            inner_copy(s, c, i, r).wait_send()
        for side in range(2):
            outer_copy(s, c, side, r).wait_send()
        return carry

    lax.fori_loop(0, early * cross, drain_first, 0)

    def drain_far(m, carry):
        s, c = in_cross(m)
        block_copy(s, c, r).wait_send()
        return carry

    lax.fori_loop(early * cross, cross * nc, drain_far, 0)

    def drain_near(m, carry):
        block_copy(cross + m // nc, lax.rem(m, nc), r).wait_send()
        return carry

    lax.fori_loop(0, (cores - 1) * nc, drain_near, 0)
    lax.fori_loop(0, ranks - 1, wait_far(nc - 1), 0)


def finish_kernel(
    levels, q,
    cells, vel, heat, aux, eaten, att, rate,
    out, vel_out, temp_out,
    last, warm, sat, pull, eater, sem, last_sem,
):
    count, per = cells.shape[:2]
    r = lax.axis_index("tracer")
    done = per - q
    scale = column_optical / levels
    copies = [
        pltpu.make_async_copy(cells.at[:, pl.ds(0, done)], out.at[:, pl.ds(0, done)], sem.at[0]),
        pltpu.make_async_copy(vel, vel_out, sem.at[1]),
        pltpu.make_async_copy(heat.at[pl.ds(0, done)], temp_out.at[pl.ds(0, done)], sem.at[2]),
    ]
    for copy in copies:
        copy.start()
    for t in range(count):
        eater[eaten[t]] = t

    def level_copy(j):
        return pltpu.make_async_copy(last.at[j], out.at[:, done + j], last_sem.at[j])

    def one_level(j, tau):
        def put(t, x):
            last[j, t] = x

        level = (r * per + done + j).astype(jnp.float32)
        wet, caught, below = react_level(
            count, level, aux[2], aux[1], tau, cells, done + j,
            eaten, eater, att, rate, scale, sat, pull, put,
        )
        warm[j] = wet * (heat[done + j] + warming_coefficient * (caught * wet))
        level_copy(j).start()
        return below

    lax.fori_loop(0, q, one_level, aux[0])
    warm_copy = pltpu.make_async_copy(warm, temp_out.at[pl.ds(done, q)], sem.at[3])
    warm_copy.start()
    for copy in copies:
        copy.wait()
    for j in range(q):
        level_copy(j).wait()
    warm_copy.wait()


def solution(mesh):
    tiles, ranks = mesh.shape["tile"], mesh.shape["tracer"]
    cores = 2 if ranks % 2 == 0 else 1

    def on_device(
        species_amounts,
        face_currents,
        thermal_anomaly,
        layer_total_per_profile,
        consumed_species,
        attenuation_factor,
        intake_speedup,
        incoming_sunshine,
    ):
        nt, nl, rows, width = species_amounts.shape
        per = nl // ranks
        q = 2 if per % 2 == 0 else 1
        chunks = nl // q
        count = ranks * nt
        cross = ranks - cores
        chips = ranks // cores
        early = min(2, per // q - 1)
        full = rows + 2 * PAD
        f32 = jnp.float32
        any_space = pl.BlockSpec(memory_space=pl.ANY)
        vmem = pl.BlockSpec(memory_space=pltpu.VMEM)
        smem = pl.BlockSpec(memory_space=pltpu.SMEM)
        dma = pltpu.SemaphoreType.DMA
        cells, vel, heat, aux = pl.pallas_call(
            functools.partial(transport_kernel, tiles, ranks, cores, q, early),
            out_shape=(
                pltpu.VMEM((count, per, rows, width), f32),
                pltpu.VMEM((2, per, rows, width), f32),
                pltpu.VMEM((per, rows, width), f32),
                pltpu.VMEM((3, rows, width), f32),
            ),
            in_specs=[any_space] * 8,
            out_specs=(vmem, vmem, vmem, vmem),
            scratch_shapes=[
                pltpu.SMEM((count,), jnp.int32),
                pltpu.SMEM((count,), f32),
                pltpu.SMEM((count,), f32),
                pltpu.VMEM((nt, nl, full, width), f32),
                pltpu.VMEM((2, nl, full, width), f32),
                pltpu.VMEM((per, full, width), f32),
                pltpu.VMEM((full, width), jnp.int32),
                pltpu.VMEM((nt, nl, rows, width), f32),
                pltpu.VMEM((ranks, rows, width), f32),
                pltpu.VMEM((chips, cores, rows, width), f32),
                pltpu.VMEM((chips, rows, width), f32),
                pltpu.VMEM((chips, rows, width), f32),
                pltpu.VMEM((chips, rows, width), f32),
                pltpu.VMEM((count, rows, width), f32),
                pltpu.VMEM((count, rows, width), f32),
                pltpu.SMEM((count,), jnp.int32),
                dma((chunks, 2)), dma((chunks, 2)),
                dma((chunks, 2)), dma((chunks, 2)),
                dma((2, 2)), dma((2, 2)),
                dma((chunks,)), dma((chunks,)),
                dma((early, cross, q)), dma((early, cross, q)),
                dma((early, cross, 2)), dma((early, cross, 2)),
                dma((chips,)), dma((chips,)), dma((1,)), dma((1,)),
                dma((chunks,)), dma((chunks,)), dma((3,)), dma((3,)),
                pltpu.SemaphoreType.REGULAR,
            ],
            compiler_params=pltpu.CompilerParams(
                collective_id=0, has_side_effects=True, vmem_limit_bytes=48 << 20
            ),
            name="transport",
        )(
            *(pltpu.with_memory_space_constraint(x, HBM) for x in (
                species_amounts, face_currents, thermal_anomaly,
                layer_total_per_profile, incoming_sunshine,
                consumed_species, attenuation_factor, intake_speedup,
            ))
        )
        return pl.pallas_call(
            functools.partial(finish_kernel, nl, q),
            out_shape=(
                jax.ShapeDtypeStruct((count, per, rows, width), f32),
                jax.ShapeDtypeStruct((2, per, rows, width), f32),
                jax.ShapeDtypeStruct((per, rows, width), f32),
            ),
            in_specs=[vmem] * 4 + [smem] * 3,
            out_specs=(any_space, any_space, any_space),
            scratch_shapes=[
                pltpu.VMEM((q, count, rows, width), f32),
                pltpu.VMEM((q, rows, width), f32),
                pltpu.VMEM((count, rows, width), f32),
                pltpu.VMEM((count, rows, width), f32),
                pltpu.SMEM((count,), jnp.int32),
                dma((4,)), dma((q,)),
            ],
            compiler_params=pltpu.CompilerParams(vmem_limit_bytes=32 << 20),
            name="finish",
        )(
            cells, vel, heat, aux,
            consumed_species, attenuation_factor, intake_speedup,
        )

    return jax.shard_map(
        on_device,
        mesh=mesh,
        in_specs=(
            P(("groups", "tracer"), None, "tile", None),
            P(None, "groups", "tile", None),
            P(("groups", "tracer"), "tile", None),
            P(("groups", "tile"), None),
            P(),
            P(),
            P(),
            P(("groups", "tile"), None),
        ),
        out_specs=(
            P("groups", "tracer", "tile", None),
            P(None, ("groups", "tracer"), "tile", None),
            P(("groups", "tracer"), "tile", None),
        ),
        check_vma=False,
    )
```

```python
import functools

import jax
import jax.numpy as jnp
from jax import lax
from jax.experimental import pallas as pl
from jax.experimental.pallas import tpu as pltpu
from jax.sharding import PartitionSpec as P

MESH = pl.DeviceIdType.MESH

sub_step = 0.45
step_duration = 0.2
gravity = 0.5
viscosity = 0.2
coriolis_base = 0.5
beta_plane = 0.5
spreading_coefficient = 0.2
water_clear = 0.05
column_optical = 3.0
warming_coefficient = 5.0
light_half = 0.3
nutrient_half = 0.5

PAD = 8
EDGE = 4
TILE = 8
LOW_FLOW, HIGH_FLOW = 3, 2

HBM = pltpu.HBM


def lane_index(shape):
    return lax.broadcasted_iota(jnp.int32, shape, len(shape) - 1)


def east(x):
    return pltpu.roll(x, x.shape[0] - 1, 0)


def west(x):
    return pltpu.roll(x, 1, 0)


def north(x):
    return jnp.where(lane_index(x.shape) == x.shape[1] - 1, 0.0, pltpu.roll(x, x.shape[1] - 1, 1))


def south(x):
    return jnp.where(lane_index(x.shape) == 0, 0.0, pltpu.roll(x, 1, 1))


def minmod(a, b):
    return jnp.maximum(jnp.minimum(a, b), 0.0) + jnp.minimum(jnp.maximum(a, b), 0.0)


def laplacian(x):
    return east(x) + west(x) + north(x) + south(x) - 4.0 * x


def substep(c, es, ns, lane):
    last = c.shape[1] - 1
    d = east(c) - c
    half = 0.5 * minmod(west(d), d)
    flux = es * jnp.where(es > 0.0, c + half, east(c - half))
    spread = flux - west(flux)
    d = jnp.where(lane == last, 0.0, pltpu.roll(c, last, 1)) - c
    half = 0.5 * minmod(jnp.where(lane == 0, c, pltpu.roll(d, 1, 1)), d)
    flux = ns * jnp.where(ns > 0.0, c + half, pltpu.roll(c - half, last, 1))
    return c - (spread + (flux - pltpu.roll(flux, 1, 1)))


def react_level(count, level, depth, sun, tau, cells, c, eaten, eater, att, rate, scale, sat, pull, put):
    total = jnp.full(depth.shape, water_clear, jnp.float32)
    for t in range(count):
        x = cells[t, c]
        size = jnp.abs(x)
        total = total + att[t] * size
        sat[t] = x / (nutrient_half + size)
        pull[t] = rate[t] * x
    optical = total * scale
    wet = jnp.where(level < depth, 1.0, 0.0)
    caught = sun * jnp.exp(-tau) * (1.0 - jnp.exp(-optical))
    mean_light = caught / optical
    gain = wet * (mean_light / (mean_light + light_half))
    for t in range(count):
        change = pull[t] * sat[eaten[t]] - pull[eater[t]] * sat[t]
        put(t, cells[t, c] + gain * change)
    return wet, caught, tau + optical


def transport_kernel(
    tiles, ranks, cores, q, early,
    sp, fc, th, dep, sun, eaten_in, att_in, rate_in,
    cells, vel, heat, aux,
    eaten, att, rate, ext, fext, hext, dext, adv, tot, pre, part, joined, over, sat, pull, eater,
    edge_send, h_recv, f_recv, s_recv, d_send, d_recv, o_send, o_recv,
    l_sem, lf_sem, ls_sem, t_sem, ready,
):
    nt, nl, rows, width = sp.shape
    per = nl // ranks
    nc = per // q
    count = ranks * nt
    chips = ranks // cores
    cross = ranks - cores
    full = rows + 2 * PAD
    r = lax.axis_index("tracer")
    z = lax.axis_index("tile")
    a, b = r // cores, lax.rem(r, cores)
    up, down = lax.rem(z + 1, tiles), lax.rem(z + tiles - 1, tiles)

    def steps(s):
        k = lax.rem(s, cores)
        return lax.rem(1 + s // cores, chips), jnp.where(s < cross, k, cores - 1 - k)

    def target(s):
        ka, kb = steps(s)
        return lax.rem(a + ka, chips) * cores + lax.rem(b + kb, cores)

    def first_level(s, c):
        return target(s) * per + c * q

    mine = pl.ds(r * nt, nt)
    body = pl.ds(PAD, rows)
    inner = pl.ds(EDGE, rows - 2 * EDGE)

    def settle(ref, sem):
        pltpu.make_async_copy(ref, ref, sem).wait()

    def pair(src, dst, lead, send, recv, low=EDGE, high=EDGE):
        return (
            pltpu.make_async_remote_copy(
                src.at[lead + (pl.ds(rows - low, low),)],
                dst.at[lead + (pl.ds(PAD - low, low),)],
                send, recv, device_id={"tile": up}, device_id_type=MESH,
            ),
            pltpu.make_async_remote_copy(
                src.at[lead + (pl.ds(0, high),)],
                dst.at[lead + (pl.ds(PAD + rows, high),)],
                send, recv, device_id={"tile": down}, device_id_type=MESH,
            ),
        )

    def edges(s, c):
        g = jnp.where(s < cross, c, nc + s - cross)
        lead = (slice(None), pl.ds(first_level(s, c), q))
        return (
            pair(fc, fext, lead, edge_send.at[0], f_recv.at[g], LOW_FLOW, HIGH_FLOW)
            + pair(sp, ext, lead, edge_send.at[1], h_recv.at[g])
        )

    def wait_edges(g, levels):
        settle(fext.at[:, pl.ds(0, levels), pl.ds(0, LOW_FLOW + HIGH_FLOW)], f_recv.at[g])
        settle(ext.at[:, pl.ds(0, levels), pl.ds(0, 2 * EDGE)], h_recv.at[g])

    def heat_edges():
        return pair(th, hext, (slice(None),), edge_send.at[2], s_recv.at[0])

    def depth_edges():
        return pair(dep, dext, (), edge_send.at[3], s_recv.at[1])

    def flow_local(s):
        lev = pl.ds(target(s) * per, per)
        sem = lf_sem.at[0] if s == 0 else lf_sem.at[1]
        return pltpu.make_async_copy(fc.at[:, lev], fext.at[:, lev, body], sem)

    def early_local(k):
        lev = pl.ds(first_level(k // early, lax.rem(k, early)), q)
        return pltpu.make_async_copy(sp.at[:, lev], ext.at[:, lev, body], l_sem.at[k])

    def rest_local(s):
        skip = early if s < cross else 0
        lev = pl.ds(first_level(s, skip), per - skip * q)
        return pltpu.make_async_copy(sp.at[:, lev], ext.at[:, lev, body], l_sem.at[early * cross])

    def block_copy(s, c):
        return pltpu.make_async_remote_copy(
            adv.at[:, pl.ds(first_level(s, c), q)],
            cells.at[mine, pl.ds(c * q, q)],
            d_send.at[0], d_recv.at[c],
            device_id={"tracer": target(s)}, device_id_type=MESH,
        )

    def inner_copy(s, c, i):
        return pltpu.make_async_remote_copy(
            adv.at[:, first_level(s, c) + i, inner],
            cells.at[mine, c * q + i, inner],
            d_send.at[0], d_recv.at[c],
            device_id={"tracer": target(s)}, device_id_type=MESH,
        )

    def outer_copy(s, c, side):
        edge = pl.ds(side * (rows - EDGE), EDGE)
        return pltpu.make_async_remote_copy(
            adv.at[:, pl.ds(first_level(s, c), q), edge],
            cells.at[mine, pl.ds(c * q, q), edge],
            d_send.at[0], d_recv.at[c],
            device_id={"tracer": target(s)}, device_id_type=MESH,
        )

    def wait_blocks(c):
        settle(cells.at[pl.ds(0, (ranks - 1) * nt), pl.ds(c * q, q)], d_recv.at[c])

    partner = a * cores + cores - 1 - b

    def part_copy():
        return pltpu.make_async_remote_copy(
            pre.at[:, cores - 1 - b], part, o_send.at[0], o_recv.at[0],
            device_id={"tracer": partner}, device_id_type=MESH,
        )

    def over_copy(k):
        there = lax.rem(a + k, chips)
        return pltpu.make_async_remote_copy(
            joined.at[there], over.at[k - 1], o_send.at[k], o_recv.at[k],
            device_id={"tracer": there * cores + b}, device_id_type=MESH,
        )

    def gets_over(k):
        return lax.rem(a + k, chips) * cores + b > 0

    def in_cross(m):
        return lax.rem(m, cross), m // cross

    def in_near(m):
        return cross + m // nc, lax.rem(m, nc)

    last_core = a * cores + cores - 1
    late = b == cores - 1
    barrier = pltpu.get_barrier_semaphore()
    for s in range(0, cross, cores):
        pl.semaphore_signal(barrier, inc=1, device_id={"tracer": target(s)}, device_id_type=MESH)
    if cores > 1:
        @pl.when(jnp.logical_not(late))
        def _():
            for s in range(1, cross, cores):
                pl.semaphore_signal(
                    barrier, inc=1, device_id={"tracer": target(s)}, device_id_type=MESH
                )
            pl.semaphore_signal(barrier, inc=1, device_id={"tracer": last_core}, device_id_type=MESH)
    for place in (up, down):
        pl.semaphore_signal(
            barrier, inc=1, device_id={"tile": place, "tracer": last_core}, device_id_type=MESH
        )

    dep_local = pltpu.make_async_copy(dep, dext.at[body], ls_sem.at[0])
    th_local = pltpu.make_async_copy(th, hext.at[:, body], ls_sem.at[1])
    sun_local = pltpu.make_async_copy(sun, aux.at[1], ls_sem.at[2])
    tables = [
        pltpu.make_async_copy(src, dst, t_sem.at[k])
        for k, (src, dst) in enumerate(((eaten_in, eaten), (att_in, att), (rate_in, rate)))
    ]
    dep_local.start()
    tables[1].start()

    flow_local(0).start()

    def start_early(k, carry):
        early_local(k).start()
        return carry

    lax.fori_loop(0, early * cross, start_early, 0)
    for s in range(1, ranks):
        flow_local(s).start()

    tot[...] = jnp.zeros_like(tot)
    dep_local.wait()
    tables[1].wait()

    def advect(lev, block, base, size, skip, first, keep, put):
        window = pl.ds(base, size)
        kept = pl.ds(first, keep)
        lane = lane_index((size, width))
        wet = jnp.where(lev < dext[window], 1.0, 0.0)
        es = sub_step * (fext[0, lev, window] * wet * east(wet))
        ns = sub_step * (fext[1, lev, window] * wet * north(wet))

        def one_tracer(t, acc):
            c = substep(ext[t, lev, window], es, ns, lane)
            c = substep(c, es, ns, lane)[skip:skip + keep]
            put(t, lev, kept, c)
            return acc + att[r * nt + t] * jnp.abs(c)

        tot[block, kept] = lax.fori_loop(0, nt, one_tracer, tot[block, kept], unroll=True)

    def put_adv(t, lev, kept, c):
        adv[t, lev, kept] = c

    def put_cells(t, lev, kept, c):
        cells[r * nt + t, lev - r * per, kept] = c

    def advance_inner(s, c, i):
        lev = first_level(s, c) + i
        advect(lev, target(s), PAD, rows, EDGE, EDGE, rows - 2 * EDGE, put_adv)

    def advance_outer(s, c, i, side):
        lev = first_level(s, c) + i
        base = side * (rows - PAD)
        skip, first = (TILE + EDGE, rows - EDGE) if side else (PAD, 0)
        advect(lev, target(s), base, TILE + 2 * PAD, skip, first, EDGE, put_adv)

    def advance(s, c, put):
        block = target(s)
        level_0 = first_level(s, c)

        def one_level(i, carry):
            advect(level_0 + i, block, 0, full, PAD, 0, rows, put)
            return carry

        lax.fori_loop(0, q, one_level, 0)

    def start_edges(order):
        def step(m, carry):
            for copy in edges(*order(m)):
                copy.start()
            return carry
        return step

    turn = jnp.where(late, 0, early * q - 1)

    def inner_step(m, carry):
        k, i = m // q, lax.rem(m, q)
        s, c = k // early, lax.rem(k, early)

        @pl.when(m == 0)
        def _():
            flow_local(0).wait()

        @pl.when(m == early * q)
        def _():
            settle(fext.at[:, pl.ds(0, (ranks - 1) * per), body], lf_sem.at[1])

        @pl.when(i == 0)
        def _():
            early_local(k).wait()

        advance_inner(s, c, i)

        @pl.when(m == 0)
        def _():
            pl.semaphore_wait(barrier, jnp.where(late, cross + cores - 1 + 2 * cores, chips - 1))

        inner_copy(s, c, i).start()

        @pl.when(m == turn)
        def _():
            if cores > 1:
                @pl.when(late)
                def _():
                    pl.semaphore_signal(
                        ready, inc=1, device_id={"tracer": partner}, device_id_type=MESH
                    )

                @pl.when(jnp.logical_not(late))
                def _():
                    pl.semaphore_wait(ready, 1)

            for copy in depth_edges():
                copy.start()
            lax.fori_loop(0, cross, start_edges(in_cross), 0)

        return carry

    lax.fori_loop(0, early * cross * q, inner_step, 0)
    lax.fori_loop(cross, cross * nc, start_edges(in_cross), 0)
    for s in range(ranks):
        rest_local(s).start()
    lax.fori_loop(0, cores * nc, start_edges(in_near), 0)
    for copy in heat_edges():
        copy.start()
    th_local.start()
    sun_local.start()
    tables[0].start()
    tables[2].start()
    settle(dext.at[pl.ds(0, 2 * EDGE)], s_recv.at[1])

    def outer_step(k, carry):
        s, c = in_cross(k)

        @pl.when(s == 0)
        def _():
            wait_edges(c, cross * q)

        def sides(i, carry):
            for side in range(2):
                advance_outer(s, c, i, side)
            return carry

        lax.fori_loop(0, q, sides, 0)
        for side in range(2):
            outer_copy(s, c, side).start()
        return carry

    lax.fori_loop(0, early * cross, outer_step, 0)

    settle(ext.at[:, pl.ds(0, nl - early * cross * q), body], l_sem.at[early * cross])

    def away_step(m, carry):
        far = m < cross * nc
        k = m - cross * nc
        s = jnp.where(far, lax.rem(m, cross), cross + k // nc)
        c = jnp.where(far, m // cross, lax.rem(k, nc))

        @pl.when(jnp.logical_and(far, s == 0))
        def _():
            wait_edges(c, cross * q)

        @pl.when(jnp.logical_and(jnp.logical_not(far), c == 0))
        def _():
            wait_edges(nc + s - cross, per)

        advance(s, c, put_adv)

        @pl.when(m != cross * nc - 1)
        def _():
            block_copy(s, c).start()

        return carry

    lax.fori_loop(early * cross, (ranks - 1) * nc, away_step, 0)

    def own_step(c, carry):
        advance(ranks - 1, c, put_cells)
        return carry

    wait_edges(nc + cores - 1, per)
    lax.fori_loop(0, nc, own_step, 0)

    above = jnp.zeros((rows, width), jnp.float32)
    for place in range(ranks):
        pre[place // cores, place % cores] = above
        above = above + tot[place]
    if cores > 1:
        part_copy().start()
        part_copy().wait()
        for k in range(chips):
            joined[k] = pre[k, b] + part[k]
    else:
        for k in range(chips):
            joined[k] = pre[k, b]
    for k in range(1, chips):
        @pl.when(gets_over(k))
        def _():
            over_copy(k).start()

    block_copy(cross - 1, nc - 1).start()

    th_local.wait()
    sun_local.wait()
    settle(hext.at[:, pl.ds(0, 2 * EDGE)], s_recv.at[0])
    lane = lane_index((full, width))
    coriolis = coriolis_base + beta_plane * lane.astype(jnp.float32) / width

    def momentum(i, carry):
        lev = r * per + i
        u, v, heat_ext = fext[0, lev], fext[1, lev], hext[i]
        wet = jnp.where(lev < dext[...], 1.0, 0.0)
        v_east, u_west = east(v), west(u)
        v_bar = 0.25 * (v + v_east + south(v) + south(v_east))
        u_bar = 0.25 * (u + u_west + north(u) + north(u_west))
        new_u = u + step_duration * (
            coriolis * v_bar - gravity * (east(heat_ext) - heat_ext) + viscosity * laplacian(u)
        )
        new_v = v + step_duration * (
            -coriolis * u_bar - gravity * (north(heat_ext) - heat_ext) + viscosity * laplacian(v)
        )
        vel[0, i] = (wet * east(wet) * new_u)[PAD:PAD + rows]
        vel[1, i] = (wet * north(wet) * new_v)[PAD:PAD + rows]
        warmer = heat_ext + step_duration * spreading_coefficient * laplacian(heat_ext)
        heat[i] = warmer[PAD:PAD + rows]
        return carry

    lax.fori_loop(0, per, momentum, 0)

    tables[0].wait()
    tables[2].wait()

    def invert(s, carry):
        who = jnp.int32(0)
        for t in range(count):
            who = jnp.where(eaten[t] == s, jnp.int32(t), who)
        eater[s] = who
        return carry

    lax.fori_loop(0, count, invert, 0)

    depth = dext[PAD:PAD + rows].astype(jnp.float32)
    aux[2] = depth
    scale = column_optical / nl
    clear = (r * per).astype(jnp.float32) * water_clear

    @pl.when(r == 0)
    def _():
        aux[0] = jnp.zeros((rows, width), jnp.float32)

    @pl.when(r > 0)
    def _():
        above = joined[a]
        for k in range(1, chips):
            over_copy(k).wait_recv()
            above = above + over[k - 1]
        aux[0] = (above + clear) * scale

    def react_chunk(c, carry):
        wait_blocks(c)

        def one_level(j, carry):
            i = c * q + j

            def put(t, x):
                cells[t, i] = x

            level = (r * per + i).astype(jnp.float32)
            wet, caught, below = react_level(
                count, level, aux[2], aux[1], aux[0], cells, i,
                eaten, eater, att, rate, scale, sat, pull, put,
            )
            aux[0] = below
            heat[i] = wet * (heat[i] + warming_coefficient * (caught * wet))
            return carry

        lax.fori_loop(0, q, one_level, 0)
        return carry

    lax.fori_loop(0, nc - 1, react_chunk, 0)

    settle(fc.at[:, :, pl.ds(0, LOW_FLOW + HIGH_FLOW)], edge_send.at[0])
    settle(sp.at[:, :, pl.ds(0, 2 * EDGE)], edge_send.at[1])
    settle(th.at[:, pl.ds(0, 2 * EDGE)], edge_send.at[2])
    settle(dep.at[pl.ds(0, 2 * EDGE)], edge_send.at[3])
    for k in range(1, chips):
        @pl.when(gets_over(k))
        def _():
            over_copy(k).wait_send()

    settle(adv.at[:, pl.ds(0, (ranks - 1) * per)], d_send.at[0])
    wait_blocks(nc - 1)


def finish_kernel(
    levels, q,
    cells, vel, heat, aux, eaten, att, rate,
    out, vel_out, temp_out,
    last, warm, sat, pull, eater, sem,
):
    count, per = cells.shape[:2]
    r = lax.axis_index("tracer")
    done = per - q
    scale = column_optical / levels
    copies = [
        pltpu.make_async_copy(cells.at[:, pl.ds(0, done)], out.at[:, pl.ds(0, done)], sem.at[0]),
        pltpu.make_async_copy(vel, vel_out, sem.at[1]),
        pltpu.make_async_copy(heat.at[pl.ds(0, done)], temp_out.at[pl.ds(0, done)], sem.at[2]),
    ]
    for copy in copies:
        copy.start()
    for t in range(count):
        eater[eaten[t]] = t

    def level_copy(j):
        return pltpu.make_async_copy(last.at[j], out.at[:, done + j], sem.at[4])

    def one_level(j, tau):
        def put(t, x):
            last[j, t] = x

        level = (r * per + done + j).astype(jnp.float32)
        wet, caught, below = react_level(
            count, level, aux[2], aux[1], tau, cells, done + j,
            eaten, eater, att, rate, scale, sat, pull, put,
        )
        warm[j] = wet * (heat[done + j] + warming_coefficient * (caught * wet))
        level_copy(j).start()
        return below

    lax.fori_loop(0, q, one_level, aux[0])
    warm_copy = pltpu.make_async_copy(warm, temp_out.at[pl.ds(done, q)], sem.at[3])
    warm_copy.start()
    for copy in copies:
        copy.wait()
    pltpu.make_async_copy(last, last, sem.at[4]).wait()
    warm_copy.wait()


def solution(mesh):
    tiles, ranks = mesh.shape["tile"], mesh.shape["tracer"]
    cores = 2 if ranks % 2 == 0 else 1

    def on_device(
        species_amounts,
        face_currents,
        thermal_anomaly,
        layer_total_per_profile,
        consumed_species,
        attenuation_factor,
        intake_speedup,
        incoming_sunshine,
    ):
        nt, nl, rows, width = species_amounts.shape
        per = nl // ranks
        q = 2 if per % 2 == 0 else 1
        nc = per // q
        count = ranks * nt
        cross = ranks - cores
        chips = ranks // cores
        early = min(2, nc - 1)
        full = rows + 2 * PAD
        f32 = jnp.float32
        any_space = pl.BlockSpec(memory_space=pl.ANY)
        vmem = pl.BlockSpec(memory_space=pltpu.VMEM)
        smem = pl.BlockSpec(memory_space=pltpu.SMEM)
        dma = pltpu.SemaphoreType.DMA
        cells, vel, heat, aux = pl.pallas_call(
            functools.partial(transport_kernel, tiles, ranks, cores, q, early),
            out_shape=(
                pltpu.VMEM((count, per, rows, width), f32),
                pltpu.VMEM((2, per, rows, width), f32),
                pltpu.VMEM((per, rows, width), f32),
                pltpu.VMEM((3, rows, width), f32),
            ),
            in_specs=[any_space] * 8,
            out_specs=(vmem, vmem, vmem, vmem),
            scratch_shapes=[
                pltpu.SMEM((count,), jnp.int32),
                pltpu.SMEM((count,), f32),
                pltpu.SMEM((count,), f32),
                pltpu.VMEM((nt, nl, full, width), f32),
                pltpu.VMEM((2, nl, full, width), f32),
                pltpu.VMEM((per, full, width), f32),
                pltpu.VMEM((full, width), jnp.int32),
                pltpu.VMEM((nt, nl, rows, width), f32),
                pltpu.VMEM((ranks, rows, width), f32),
                pltpu.VMEM((chips, cores, rows, width), f32),
                pltpu.VMEM((chips, rows, width), f32),
                pltpu.VMEM((chips, rows, width), f32),
                pltpu.VMEM((chips, rows, width), f32),
                pltpu.VMEM((count, rows, width), f32),
                pltpu.VMEM((count, rows, width), f32),
                pltpu.SMEM((count,), jnp.int32),
                dma((4,)), dma((nc + cores,)), dma((nc + cores,)), dma((2,)),
                dma((1,)), dma((nc,)), dma((chips,)), dma((chips,)),
                dma((early * cross + 1,)), dma((2,)), dma((3,)), dma((3,)),
                pltpu.SemaphoreType.REGULAR,
            ],
            compiler_params=pltpu.CompilerParams(
                collective_id=0, has_side_effects=True, vmem_limit_bytes=48 << 20
            ),
            name="transport",
        )(
            *(pltpu.with_memory_space_constraint(x, HBM) for x in (
                species_amounts, face_currents, thermal_anomaly,
                layer_total_per_profile, incoming_sunshine,
                consumed_species, attenuation_factor, intake_speedup,
            ))
        )
        return pl.pallas_call(
            functools.partial(finish_kernel, nl, q),
            out_shape=(
                jax.ShapeDtypeStruct((count, per, rows, width), f32),
                jax.ShapeDtypeStruct((2, per, rows, width), f32),
                jax.ShapeDtypeStruct((per, rows, width), f32),
            ),
            in_specs=[vmem] * 4 + [smem] * 3,
            out_specs=(any_space, any_space, any_space),
            scratch_shapes=[
                pltpu.VMEM((q, count, rows, width), f32),
                pltpu.VMEM((q, rows, width), f32),
                pltpu.VMEM((count, rows, width), f32),
                pltpu.VMEM((count, rows, width), f32),
                pltpu.SMEM((count,), jnp.int32),
                dma((5,)),
            ],
            compiler_params=pltpu.CompilerParams(vmem_limit_bytes=32 << 20),
            name="finish",
        )(
            cells, vel, heat, aux,
            consumed_species, attenuation_factor, intake_speedup,
        )

    return jax.shard_map(
        on_device,
        mesh=mesh,
        in_specs=(
            P(("groups", "tracer"), None, "tile", None),
            P(None, "groups", "tile", None),
            P(("groups", "tracer"), "tile", None),
            P(("groups", "tile"), None),
            P(),
            P(),
            P(),
            P(("groups", "tile"), None),
        ),
        out_specs=(
            P("groups", "tracer", "tile", None),
            P(None, ("groups", "tracer"), "tile", None),
            P(("groups", "tracer"), "tile", None),
        ),
        check_vma=False,
    )
```

```python
import functools

import jax
import jax.numpy as jnp
from jax import lax
from jax.experimental import pallas as pl
from jax.experimental.pallas import tpu as pltpu
from jax.sharding import PartitionSpec as P

MESH = pl.DeviceIdType.MESH

sub_step = 0.45
step_duration = 0.2
gravity = 0.5
viscosity = 0.2
coriolis_base = 0.5
beta_plane = 0.5
spreading_coefficient = 0.2
water_clear = 0.05
column_optical = 3.0
warming_coefficient = 5.0
light_half = 0.3
nutrient_half = 0.5

PAD = 8
EDGE = 4
TILE = 8
LOW_FLOW, HIGH_FLOW = 3, 2

HBM = pltpu.HBM


def lane_index(shape):
    return lax.broadcasted_iota(jnp.int32, shape, len(shape) - 1)


def east(x):
    return pltpu.roll(x, x.shape[0] - 1, 0)


def west(x):
    return pltpu.roll(x, 1, 0)


def north(x):
    return jnp.where(lane_index(x.shape) == x.shape[1] - 1, 0.0, pltpu.roll(x, x.shape[1] - 1, 1))


def south(x):
    return jnp.where(lane_index(x.shape) == 0, 0.0, pltpu.roll(x, 1, 1))


def minmod(a, b):
    return jnp.maximum(jnp.minimum(a, b), jnp.minimum(jnp.maximum(a, b), 0.0))


def laplacian(x):
    return east(x) + west(x) + north(x) + south(x) - 4.0 * x


def substep(c, es, ns, lane):
    last = c.shape[1] - 1
    e = 0.5 * c
    d = east(e) - e
    half = minmod(west(d), d)
    flux = es * jnp.where(es > 0.0, c + half, east(c - half))
    spread = flux - west(flux)
    d = jnp.where(lane == last, 0.0, pltpu.roll(e, last, 1)) - e
    half = minmod(jnp.where(lane == 0, e, pltpu.roll(d, 1, 1)), d)
    flux = ns * jnp.where(ns > 0.0, c + half, pltpu.roll(c - half, last, 1))
    return c - (spread + (flux - pltpu.roll(flux, 1, 1)))


def react_level(count, level, depth, sun, tau, cells, c, eaten, eater, att, rate, scale, sat, pull, put):
    total = jnp.full(depth.shape, water_clear, jnp.float32)
    for t in range(count):
        x = cells[t, c]
        size = jnp.abs(x)
        total = total + att[t] * size
        sat[t] = x / (nutrient_half + size)
        pull[t] = rate[t] * x
    optical = total * scale
    wet = jnp.where(level < depth, 1.0, 0.0)
    caught = sun * jnp.exp(-tau) * (1.0 - jnp.exp(-optical))
    mean_light = caught / optical
    gain = wet * (mean_light / (mean_light + light_half))
    for t in range(count):
        change = pull[t] * sat[eaten[t]] - pull[eater[t]] * sat[t]
        put(t, cells[t, c] + gain * change)
    return wet, caught, tau + optical


def transport_kernel(
    tiles, ranks, cores, q, early,
    sp, fc, th, dep, sun, eaten_in, att_in, rate_in,
    cells, vel, heat, aux,
    eaten, att, rate, ext, fext, hext, dext, adv, tot, pre, part, joined, over, sat, pull, eater,
    edge_send, h_recv, f_recv, s_recv, d_send, d_recv, o_send, o_recv,
    l_sem, lf_sem, ls_sem, t_sem, ready,
):
    nt, nl, rows, width = sp.shape
    per = nl // ranks
    nc = per // q
    count = ranks * nt
    chips = ranks // cores
    cross = ranks - cores
    full = rows + PAD
    r = lax.axis_index("tracer")
    z = lax.axis_index("tile")
    a, b = r // cores, lax.rem(r, cores)
    up, down = lax.rem(z + 1, tiles), lax.rem(z + tiles - 1, tiles)

    def steps(s):
        k = lax.rem(s, cores)
        return lax.rem(1 + s // cores, chips), jnp.where(s < cross, k, cores - 1 - k)

    def target(s):
        ka, kb = steps(s)
        return lax.rem(a + ka, chips) * cores + lax.rem(b + kb, cores)

    def first_level(s, c):
        return target(s) * per + c * q

    mine = pl.ds(r * nt, nt)
    body = pl.ds(PAD, rows)
    inner = pl.ds(EDGE, rows - 2 * EDGE)

    def settle(ref, sem):
        pltpu.make_async_copy(ref, ref, sem).wait()

    def pair(src, dst, lead, send, recv, low=EDGE, high=EDGE):
        return (
            pltpu.make_async_remote_copy(
                src.at[lead + (pl.ds(rows - low, low),)],
                dst.at[lead + (pl.ds(PAD - low, low),)],
                send, recv, device_id={"tile": up}, device_id_type=MESH,
            ),
            pltpu.make_async_remote_copy(
                src.at[lead + (pl.ds(0, high),)],
                dst.at[lead + (pl.ds(0, high),)],
                send, recv, device_id={"tile": down}, device_id_type=MESH,
            ),
        )

    def edges(s, c):
        g = jnp.where(s < cross, c, nc + s - cross)
        lead = (slice(None), pl.ds(first_level(s, c), q))
        return (
            pair(fc, fext, lead, edge_send.at[0], f_recv.at[g], LOW_FLOW, HIGH_FLOW)
            + pair(sp, ext, lead, edge_send.at[1], h_recv.at[g])
        )

    def wait_edges(g, levels):
        settle(fext.at[:, pl.ds(0, levels), pl.ds(0, LOW_FLOW + HIGH_FLOW)], f_recv.at[g])
        settle(ext.at[:, pl.ds(0, levels), pl.ds(0, 2 * EDGE)], h_recv.at[g])

    def heat_edges():
        return pair(th, hext, (slice(None),), edge_send.at[2], s_recv.at[0])

    def depth_edges():
        return pair(dep, dext, (), edge_send.at[3], s_recv.at[1])

    def flow_local(s):
        lev = pl.ds(target(s) * per, per)
        sem = lf_sem.at[0] if s == 0 else lf_sem.at[1]
        return pltpu.make_async_copy(fc.at[:, lev], fext.at[:, lev, body], sem)

    def early_local(k):
        lev = pl.ds(first_level(k // early, lax.rem(k, early)), q)
        return pltpu.make_async_copy(sp.at[:, lev], ext.at[:, lev, body], l_sem.at[k])

    def rest_local(s):
        skip = early if s < cross else 0
        lev = pl.ds(first_level(s, skip), per - skip * q)
        return pltpu.make_async_copy(sp.at[:, lev], ext.at[:, lev, body], l_sem.at[early * cross])

    def block_copy(s, c):
        return pltpu.make_async_remote_copy(
            adv.at[:, pl.ds(first_level(s, c), q)],
            cells.at[mine, pl.ds(c * q, q)],
            d_send.at[0], d_recv.at[c],
            device_id={"tracer": target(s)}, device_id_type=MESH,
        )

    def inner_copy(s, c, i):
        return pltpu.make_async_remote_copy(
            adv.at[:, first_level(s, c) + i, inner],
            cells.at[mine, c * q + i, inner],
            d_send.at[0], d_recv.at[c],
            device_id={"tracer": target(s)}, device_id_type=MESH,
        )

    def outer_copy(s, c, side):
        edge = pl.ds(side * (rows - EDGE), EDGE)
        return pltpu.make_async_remote_copy(
            adv.at[:, pl.ds(first_level(s, c), q), edge],
            cells.at[mine, pl.ds(c * q, q), edge],
            d_send.at[0], d_recv.at[c],
            device_id={"tracer": target(s)}, device_id_type=MESH,
        )

    def wait_blocks(c):
        settle(cells.at[pl.ds(0, (ranks - 1) * nt), pl.ds(c * q, q)], d_recv.at[c])

    partner = a * cores + cores - 1 - b

    def part_copy():
        return pltpu.make_async_remote_copy(
            pre.at[:, cores - 1 - b], part, o_send.at[0], o_recv.at[0],
            device_id={"tracer": partner}, device_id_type=MESH,
        )

    def over_copy(k):
        there = lax.rem(a + k, chips)
        return pltpu.make_async_remote_copy(
            joined.at[there], over.at[k - 1], o_send.at[k], o_recv.at[k],
            device_id={"tracer": there * cores + b}, device_id_type=MESH,
        )

    def gets_over(k):
        return lax.rem(a + k, chips) * cores + b > 0

    def in_cross(m):
        return lax.rem(m, cross), m // cross

    def in_near(m):
        return cross + m // nc, lax.rem(m, nc)

    last_core = a * cores + cores - 1
    late = b == cores - 1
    barrier = pltpu.get_barrier_semaphore()
    for s in range(0, cross, cores):
        pl.semaphore_signal(barrier, inc=1, device_id={"tracer": target(s)}, device_id_type=MESH)
    if cores > 1:
        @pl.when(jnp.logical_not(late))
        def _():
            for s in range(1, cross, cores):
                pl.semaphore_signal(
                    barrier, inc=1, device_id={"tracer": target(s)}, device_id_type=MESH
                )
            pl.semaphore_signal(barrier, inc=1, device_id={"tracer": last_core}, device_id_type=MESH)
    for place in (up, down):
        pl.semaphore_signal(
            barrier, inc=1, device_id={"tile": place, "tracer": last_core}, device_id_type=MESH
        )

    dep_local = pltpu.make_async_copy(dep, dext.at[body], ls_sem.at[0])
    th_local = pltpu.make_async_copy(th, hext.at[:, body], ls_sem.at[1])
    sun_local = pltpu.make_async_copy(sun, aux.at[1], ls_sem.at[2])
    tables = [
        pltpu.make_async_copy(src, dst, t_sem.at[k])
        for k, (src, dst) in enumerate(((eaten_in, eaten), (att_in, att), (rate_in, rate)))
    ]
    dep_local.start()
    tables[1].start()

    flow_local(0).start()

    def start_early(k, carry):
        early_local(k).start()
        return carry

    lax.fori_loop(0, early * cross, start_early, 0)
    for s in range(1, ranks):
        flow_local(s).start()

    tot[...] = jnp.zeros_like(tot)
    dep_local.wait()
    tables[1].wait()

    def advect(lev, block, base, size, skip, first, keep, put):
        window = pl.ds(base, size)
        kept = pl.ds(first, keep)
        lane = lane_index((size, width))
        wet = jnp.where(lev < dext[window], 1.0, 0.0)
        es = sub_step * (fext[0, lev, window] * wet * east(wet))
        ns = sub_step * (fext[1, lev, window] * wet * north(wet))

        def one_tracer(t, acc):
            c = substep(ext[t, lev, window], es, ns, lane)
            c = substep(c, es, ns, lane)[skip:skip + keep]
            put(t, lev, kept, c)
            return acc + att[r * nt + t] * jnp.abs(c)

        tot[block, kept] = lax.fori_loop(0, nt, one_tracer, tot[block, kept], unroll=True)

    def strip(ref, *lead):
        return jnp.concatenate(
            [ref[lead + (pl.ds(full - TILE, TILE),)], ref[lead + (pl.ds(0, PAD + TILE),)]], axis=0
        )

    def put_adv(t, lev, kept, c):
        adv[t, lev, kept] = c

    def put_cells(t, lev, kept, c):
        cells[r * nt + t, lev - r * per, kept] = c

    def advance_inner(s, c, i):
        lev = first_level(s, c) + i
        advect(lev, target(s), PAD, rows, EDGE, EDGE, rows - 2 * EDGE, put_adv)

    def advance_outer(s, c, i):
        lev = first_level(s, c) + i
        block = target(s)
        size = TILE + PAD + TILE
        lane = lane_index((size, width))
        wet = jnp.where(lev < strip(dext), 1.0, 0.0)
        es = sub_step * (strip(fext, 0, lev) * wet * east(wet))
        ns = sub_step * (strip(fext, 1, lev) * wet * north(wet))
        high, low = slice(TILE - EDGE, TILE), slice(TILE + PAD, TILE + PAD + EDGE)
        high_rows, low_rows = pl.ds(rows - EDGE, EDGE), pl.ds(0, EDGE)

        def one_tracer(t, acc):
            c = substep(strip(ext, t, lev), es, ns, lane)
            c = substep(c, es, ns, lane)
            adv[t, lev, high_rows] = c[high]
            adv[t, lev, low_rows] = c[low]
            return acc + att[r * nt + t] * jnp.abs(c)

        acc = lax.fori_loop(0, nt, one_tracer, jnp.zeros((size, width), jnp.float32), unroll=True)
        tot[block, high_rows] += acc[high]
        tot[block, low_rows] += acc[low]

    def advance(s, c, put):
        block = target(s)
        level_0 = first_level(s, c)

        def one_level(i, carry):
            advect(level_0 + i, block, 0, full, PAD, 0, rows, put)
            return carry

        lax.fori_loop(0, q, one_level, 0)

    def start_edges(order):
        def step(m, carry):
            for copy in edges(*order(m)):
                copy.start()
            return carry
        return step

    turn = jnp.where(late, 0, early * q - 1)

    def inner_step(m, carry):
        k, i = m // q, lax.rem(m, q)
        s, c = k // early, lax.rem(k, early)

        @pl.when(m == 0)
        def _():
            flow_local(0).wait()

        @pl.when(m == early * q)
        def _():
            settle(fext.at[:, pl.ds(0, (ranks - 1) * per), body], lf_sem.at[1])

        @pl.when(i == 0)
        def _():
            early_local(k).wait()

        advance_inner(s, c, i)

        @pl.when(m == 0)
        def _():
            pl.semaphore_wait(barrier, jnp.where(late, cross + cores - 1 + 2 * cores, chips - 1))

        inner_copy(s, c, i).start()

        @pl.when(m == turn)
        def _():
            if cores > 1:
                @pl.when(late)
                def _():
                    pl.semaphore_signal(
                        ready, inc=1, device_id={"tracer": partner}, device_id_type=MESH
                    )

                @pl.when(jnp.logical_not(late))
                def _():
                    pl.semaphore_wait(ready, 1)

            for copy in depth_edges():
                copy.start()
            lax.fori_loop(0, cross, start_edges(in_cross), 0)

        return carry

    lax.fori_loop(0, early * cross * q, inner_step, 0)
    lax.fori_loop(cross, cross * nc, start_edges(in_cross), 0)
    for s in range(ranks):
        rest_local(s).start()
    lax.fori_loop(0, cores * nc, start_edges(in_near), 0)
    for copy in heat_edges():
        copy.start()
    th_local.start()
    sun_local.start()
    tables[0].start()
    tables[2].start()
    settle(dext.at[pl.ds(0, 2 * EDGE)], s_recv.at[1])

    def outer_step(k, carry):
        s, c = in_cross(k)

        @pl.when(s == 0)
        def _():
            wait_edges(c, cross * q)

        def sides(i, carry):
            advance_outer(s, c, i)
            return carry

        lax.fori_loop(0, q, sides, 0)
        for side in range(2):
            outer_copy(s, c, side).start()
        return carry

    lax.fori_loop(0, early * cross, outer_step, 0)

    settle(ext.at[:, pl.ds(0, nl - early * cross * q), body], l_sem.at[early * cross])

    def away_step(m, carry):
        far = m < cross * nc
        k = m - cross * nc
        s = jnp.where(far, lax.rem(m, cross), cross + k // nc)
        c = jnp.where(far, m // cross, lax.rem(k, nc))

        @pl.when(jnp.logical_and(far, s == 0))
        def _():
            wait_edges(c, cross * q)

        @pl.when(jnp.logical_and(jnp.logical_not(far), c == 0))
        def _():
            wait_edges(nc + s - cross, per)

        advance(s, c, put_adv)

        @pl.when(m != cross * nc - 1)
        def _():
            block_copy(s, c).start()

        return carry

    lax.fori_loop(early * cross, (ranks - 1) * nc, away_step, 0)

    def own_step(c, carry):
        advance(ranks - 1, c, put_cells)
        return carry

    wait_edges(nc + cores - 1, per)
    lax.fori_loop(0, nc, own_step, 0)

    above = jnp.zeros((rows, width), jnp.float32)
    for place in range(ranks):
        pre[place // cores, place % cores] = above
        above = above + tot[place]
    if cores > 1:
        part_copy().start()
        part_copy().wait()
        for k in range(chips):
            joined[k] = pre[k, b] + part[k]
    else:
        for k in range(chips):
            joined[k] = pre[k, b]
    for k in range(1, chips):
        @pl.when(gets_over(k))
        def _():
            over_copy(k).start()

    block_copy(cross - 1, nc - 1).start()

    th_local.wait()
    sun_local.wait()
    settle(hext.at[:, pl.ds(0, 2 * EDGE)], s_recv.at[0])
    lane = lane_index((full, width))
    coriolis = coriolis_base + beta_plane * lane.astype(jnp.float32) / width

    def momentum(i, carry):
        lev = r * per + i
        u, v, heat_ext = fext[0, lev], fext[1, lev], hext[i]
        wet = jnp.where(lev < dext[...], 1.0, 0.0)
        v_east, u_west = east(v), west(u)
        v_bar = 0.25 * (v + v_east + south(v) + south(v_east))
        u_bar = 0.25 * (u + u_west + north(u) + north(u_west))
        new_u = u + step_duration * (
            coriolis * v_bar - gravity * (east(heat_ext) - heat_ext) + viscosity * laplacian(u)
        )
        new_v = v + step_duration * (
            -coriolis * u_bar - gravity * (north(heat_ext) - heat_ext) + viscosity * laplacian(v)
        )
        vel[0, i] = (wet * east(wet) * new_u)[PAD:PAD + rows]
        vel[1, i] = (wet * north(wet) * new_v)[PAD:PAD + rows]
        warmer = heat_ext + step_duration * spreading_coefficient * laplacian(heat_ext)
        heat[i] = warmer[PAD:PAD + rows]
        return carry

    lax.fori_loop(0, per, momentum, 0)

    tables[0].wait()
    tables[2].wait()

    def invert(s, carry):
        who = jnp.int32(0)
        for t in range(count):
            who = jnp.where(eaten[t] == s, jnp.int32(t), who)
        eater[s] = who
        return carry

    lax.fori_loop(0, count, invert, 0)

    depth = dext[PAD:PAD + rows].astype(jnp.float32)
    aux[2] = depth
    scale = column_optical / nl
    clear = (r * per).astype(jnp.float32) * water_clear

    @pl.when(r == 0)
    def _():
        aux[0] = jnp.zeros((rows, width), jnp.float32)

    @pl.when(r > 0)
    def _():
        above = joined[a]
        for k in range(1, chips):
            over_copy(k).wait_recv()
            above = above + over[k - 1]
        aux[0] = (above + clear) * scale

    def react_chunk(c, carry):
        wait_blocks(c)

        def one_level(j, carry):
            i = c * q + j

            def put(t, x):
                cells[t, i] = x

            level = (r * per + i).astype(jnp.float32)
            wet, caught, below = react_level(
                count, level, aux[2], aux[1], aux[0], cells, i,
                eaten, eater, att, rate, scale, sat, pull, put,
            )
            aux[0] = below
            heat[i] = wet * (heat[i] + warming_coefficient * (caught * wet))
            return carry

        lax.fori_loop(0, q, one_level, 0)
        return carry

    lax.fori_loop(0, nc - 1, react_chunk, 0)

    settle(fc.at[:, :, pl.ds(0, LOW_FLOW + HIGH_FLOW)], edge_send.at[0])
    settle(sp.at[:, :, pl.ds(0, 2 * EDGE)], edge_send.at[1])
    settle(th.at[:, pl.ds(0, 2 * EDGE)], edge_send.at[2])
    settle(dep.at[pl.ds(0, 2 * EDGE)], edge_send.at[3])
    for k in range(1, chips):
        @pl.when(gets_over(k))
        def _():
            over_copy(k).wait_send()

    settle(adv.at[:, pl.ds(0, (ranks - 1) * per)], d_send.at[0])
    wait_blocks(nc - 1)


def finish_kernel(
    levels, q,
    cells, vel, heat, aux, eaten, att, rate,
    out, vel_out, temp_out,
    last, warm, sat, pull, eater, sem,
):
    count, per = cells.shape[:2]
    r = lax.axis_index("tracer")
    done = per - q
    scale = column_optical / levels
    copies = [
        pltpu.make_async_copy(cells.at[:, pl.ds(0, done)], out.at[:, pl.ds(0, done)], sem.at[0]),
        pltpu.make_async_copy(vel, vel_out, sem.at[1]),
        pltpu.make_async_copy(heat.at[pl.ds(0, done)], temp_out.at[pl.ds(0, done)], sem.at[2]),
    ]
    for copy in copies:
        copy.start()
    for t in range(count):
        eater[eaten[t]] = t

    def level_copy(j):
        return pltpu.make_async_copy(last.at[j], out.at[:, done + j], sem.at[4])

    def one_level(j, tau):
        def put(t, x):
            last[j, t] = x

        level = (r * per + done + j).astype(jnp.float32)
        wet, caught, below = react_level(
            count, level, aux[2], aux[1], tau, cells, done + j,
            eaten, eater, att, rate, scale, sat, pull, put,
        )
        warm[j] = wet * (heat[done + j] + warming_coefficient * (caught * wet))
        level_copy(j).start()
        return below

    lax.fori_loop(0, q, one_level, aux[0])
    warm_copy = pltpu.make_async_copy(warm, temp_out.at[pl.ds(done, q)], sem.at[3])
    warm_copy.start()
    for copy in copies:
        copy.wait()
    pltpu.make_async_copy(last, last, sem.at[4]).wait()
    warm_copy.wait()


def solution(mesh):
    tiles, ranks = mesh.shape["tile"], mesh.shape["tracer"]
    cores = 2 if ranks % 2 == 0 else 1

    def on_device(
        species_amounts,
        face_currents,
        thermal_anomaly,
        layer_total_per_profile,
        consumed_species,
        attenuation_factor,
        intake_speedup,
        incoming_sunshine,
    ):
        nt, nl, rows, width = species_amounts.shape
        per = nl // ranks
        q = 2 if per % 2 == 0 else 1
        nc = per // q
        count = ranks * nt
        cross = ranks - cores
        chips = ranks // cores
        early = min(2, nc - 1)
        full = rows + PAD
        f32 = jnp.float32
        any_space = pl.BlockSpec(memory_space=pl.ANY)
        vmem = pl.BlockSpec(memory_space=pltpu.VMEM)
        smem = pl.BlockSpec(memory_space=pltpu.SMEM)
        dma = pltpu.SemaphoreType.DMA
        cells, vel, heat, aux = pl.pallas_call(
            functools.partial(transport_kernel, tiles, ranks, cores, q, early),
            out_shape=(
                pltpu.VMEM((count, per, rows, width), f32),
                pltpu.VMEM((2, per, rows, width), f32),
                pltpu.VMEM((per, rows, width), f32),
                pltpu.VMEM((3, rows, width), f32),
            ),
            in_specs=[any_space] * 8,
            out_specs=(vmem, vmem, vmem, vmem),
            scratch_shapes=[
                pltpu.SMEM((count,), jnp.int32),
                pltpu.SMEM((count,), f32),
                pltpu.SMEM((count,), f32),
                pltpu.VMEM((nt, nl, full, width), f32),
                pltpu.VMEM((2, nl, full, width), f32),
                pltpu.VMEM((per, full, width), f32),
                pltpu.VMEM((full, width), jnp.int32),
                pltpu.VMEM((nt, nl, rows, width), f32),
                pltpu.VMEM((ranks, rows, width), f32),
                pltpu.VMEM((chips, cores, rows, width), f32),
                pltpu.VMEM((chips, rows, width), f32),
                pltpu.VMEM((chips, rows, width), f32),
                pltpu.VMEM((chips, rows, width), f32),
                pltpu.VMEM((count, rows, width), f32),
                pltpu.VMEM((count, rows, width), f32),
                pltpu.SMEM((count,), jnp.int32),
                dma((4,)), dma((nc + cores,)), dma((nc + cores,)), dma((2,)),
                dma((1,)), dma((nc,)), dma((chips,)), dma((chips,)),
                dma((early * cross + 1,)), dma((2,)), dma((3,)), dma((3,)),
                pltpu.SemaphoreType.REGULAR,
            ],
            compiler_params=pltpu.CompilerParams(
                collective_id=0, has_side_effects=True, vmem_limit_bytes=48 << 20
            ),
            name="transport",
        )(
            *(pltpu.with_memory_space_constraint(x, HBM) for x in (
                species_amounts, face_currents, thermal_anomaly,
                layer_total_per_profile, incoming_sunshine,
                consumed_species, attenuation_factor, intake_speedup,
            ))
        )
        return pl.pallas_call(
            functools.partial(finish_kernel, nl, q),
            out_shape=(
                jax.ShapeDtypeStruct((count, per, rows, width), f32),
                jax.ShapeDtypeStruct((2, per, rows, width), f32),
                jax.ShapeDtypeStruct((per, rows, width), f32),
            ),
            in_specs=[vmem] * 4 + [smem] * 3,
            out_specs=(any_space, any_space, any_space),
            scratch_shapes=[
                pltpu.VMEM((q, count, rows, width), f32),
                pltpu.VMEM((q, rows, width), f32),
                pltpu.VMEM((count, rows, width), f32),
                pltpu.VMEM((count, rows, width), f32),
                pltpu.SMEM((count,), jnp.int32),
                dma((5,)),
            ],
            compiler_params=pltpu.CompilerParams(vmem_limit_bytes=32 << 20),
            name="finish",
        )(
            cells, vel, heat, aux,
            consumed_species, attenuation_factor, intake_speedup,
        )

    return jax.shard_map(
        on_device,
        mesh=mesh,
        in_specs=(
            P(("groups", "tracer"), None, "tile", None),
            P(None, "groups", "tile", None),
            P(("groups", "tracer"), "tile", None),
            P(("groups", "tile"), None),
            P(),
            P(),
            P(),
            P(("groups", "tile"), None),
        ),
        out_specs=(
            P("groups", "tracer", "tile", None),
            P(None, ("groups", "tracer"), "tile", None),
            P(("groups", "tracer"), "tile", None),
        ),
        check_vma=False,
    )
```

```python
import functools

import jax
import jax.numpy as jnp
from jax import lax
from jax.experimental import pallas as pl
from jax.experimental.pallas import tpu as pltpu
from jax.sharding import PartitionSpec as P

MESH = pl.DeviceIdType.MESH

sub_step = 0.45
step_duration = 0.2
gravity = 0.5
viscosity = 0.2
coriolis_base = 0.5
beta_plane = 0.5
spreading_coefficient = 0.2
water_clear = 0.05
column_optical = 3.0
warming_coefficient = 5.0
light_half = 0.3
nutrient_half = 0.5

PAD = 8
EDGE = 4
TILE = 8
LOW_FLOW, HIGH_FLOW = 3, 2

HBM = pltpu.HBM


def lane_index(shape):
    return lax.broadcasted_iota(jnp.int32, shape, len(shape) - 1)


def east(x):
    return pltpu.roll(x, x.shape[0] - 1, 0)


def west(x):
    return pltpu.roll(x, 1, 0)


def north(x):
    return jnp.where(lane_index(x.shape) == x.shape[1] - 1, 0.0, pltpu.roll(x, x.shape[1] - 1, 1))


def south(x):
    return jnp.where(lane_index(x.shape) == 0, 0.0, pltpu.roll(x, 1, 1))


def minmod(a, b):
    return jnp.maximum(jnp.minimum(a, b), jnp.minimum(jnp.maximum(a, b), 0.0))


def laplacian(x):
    return east(x) + west(x) + north(x) + south(x) - 4.0 * x


def substep(c, es, ns, lane):
    last = c.shape[1] - 1
    e = 0.5 * c
    d = east(e) - e
    half = minmod(west(d), d)
    flux = es * jnp.where(es > 0.0, c + half, east(c - half))
    spread = flux - west(flux)
    d = jnp.where(lane == last, 0.0, pltpu.roll(e, last, 1)) - e
    half = minmod(jnp.where(lane == 0, e, pltpu.roll(d, 1, 1)), d)
    flux = ns * jnp.where(ns > 0.0, c + half, pltpu.roll(c - half, last, 1))
    return c - (spread + (flux - pltpu.roll(flux, 1, 1)))


def react_level(count, level, depth, sun, tau, cells, c, eaten, eater, att, rate, scale, sat, pull, put):
    total = jnp.full(depth.shape, water_clear, jnp.float32)
    for t in range(count):
        x = cells[t, c]
        size = jnp.abs(x)
        total = total + att[t] * size
        sat[t] = x / (nutrient_half + size)
        pull[t] = rate[t] * x
    optical = total * scale
    wet = jnp.where(level < depth, 1.0, 0.0)
    caught = sun * jnp.exp(-tau) * (1.0 - jnp.exp(-optical))
    mean_light = caught / optical
    gain = wet * (mean_light / (mean_light + light_half))
    for t in range(count):
        change = pull[t] * sat[eaten[t]] - pull[eater[t]] * sat[t]
        put(t, cells[t, c] + gain * change)
    return wet, caught, tau + optical


def transport_kernel(
    tiles, ranks, cores, q, early,
    sp, fc, th, dep, sun, eaten_in, att_in, rate_in,
    cells, vel, heat, aux,
    eaten, att, rate, ext, fext, hext, dext, adv, tot, pre, part, joined, over, sat, pull, eater,
    edge_send, h_recv, f_recv, s_recv, d_send, d_recv, o_send, o_recv,
    l_sem, lf_sem, ls_sem, t_sem, ready,
):
    nt, nl, rows, width = sp.shape
    per = nl // ranks
    nc = per // q
    count = ranks * nt
    chips = ranks // cores
    cross = ranks - cores
    full = rows + PAD
    parts = 2 if nt % 2 == 0 else 1
    some = nt // parts
    r = lax.axis_index("tracer")
    z = lax.axis_index("tile")
    a, b = r // cores, lax.rem(r, cores)
    up, down = lax.rem(z + 1, tiles), lax.rem(z + tiles - 1, tiles)

    def target(s):
        k = lax.rem(s, cores)
        chip = lax.rem(a + 1 + s // cores, chips)
        core = jnp.where(s < cross, k, lax.rem(b + cores - 1 - k, cores))
        return chip * cores + core

    def first_level(s, c):
        return target(s) * per + c * q

    mine = pl.ds(r * nt, nt)
    body = pl.ds(PAD, rows)
    inner = pl.ds(EDGE, rows - 2 * EDGE)

    def settle(ref, sem):
        pltpu.make_async_copy(ref, ref, sem).wait()

    def pair(src, dst, lead, send, recv, low=EDGE, high=EDGE):
        return (
            pltpu.make_async_remote_copy(
                src.at[lead + (pl.ds(rows - low, low),)],
                dst.at[lead + (pl.ds(PAD - low, low),)],
                send, recv, device_id={"tile": up}, device_id_type=MESH,
            ),
            pltpu.make_async_remote_copy(
                src.at[lead + (pl.ds(0, high),)],
                dst.at[lead + (pl.ds(0, high),)],
                send, recv, device_id={"tile": down}, device_id_type=MESH,
            ),
        )

    def edges(s, c):
        g = jnp.where(s < cross, c, nc + s - cross)
        lead = (slice(None), pl.ds(first_level(s, c), q))
        return (
            pair(fc, fext, lead, edge_send.at[0], f_recv.at[g], LOW_FLOW, HIGH_FLOW)
            + pair(sp, ext, lead, edge_send.at[1], h_recv.at[g])
        )

    def wait_edges(g, levels):
        settle(fext.at[:, pl.ds(0, levels), pl.ds(0, LOW_FLOW + HIGH_FLOW)], f_recv.at[g])
        settle(ext.at[:, pl.ds(0, levels), pl.ds(0, 2 * EDGE)], h_recv.at[g])

    def heat_edges():
        return pair(th, hext, (slice(None),), edge_send.at[2], s_recv.at[0])

    def depth_edges():
        return pair(dep, dext, (), edge_send.at[3], s_recv.at[1])

    def flow_local(s):
        lev = pl.ds(target(s) * per, per)
        sem = lf_sem.at[0] if s == 0 else lf_sem.at[1]
        return pltpu.make_async_copy(fc.at[:, lev], fext.at[:, lev, body], sem)

    def early_local(k):
        lev = pl.ds(first_level(k // early, lax.rem(k, early)), q)
        return pltpu.make_async_copy(sp.at[:, lev], ext.at[:, lev, body], l_sem.at[k])

    def rest_local(s):
        skip = early if s < cross else 0
        lev = pl.ds(first_level(s, skip), per - skip * q)
        return pltpu.make_async_copy(sp.at[:, lev], ext.at[:, lev, body], l_sem.at[early * cross])

    def block_copy(s, c):
        return pltpu.make_async_remote_copy(
            adv.at[:, pl.ds(first_level(s, c), q)],
            cells.at[mine, pl.ds(c * q, q)],
            d_send.at[0], d_recv.at[c],
            device_id={"tracer": target(s)}, device_id_type=MESH,
        )

    def inner_copy(s, c, i, h):
        return pltpu.make_async_remote_copy(
            adv.at[pl.ds(h * some, some), first_level(s, c) + i, inner],
            cells.at[pl.ds(r * nt + h * some, some), c * q + i, inner],
            d_send.at[0], d_recv.at[c],
            device_id={"tracer": target(s)}, device_id_type=MESH,
        )

    def outer_copy(s, c, side):
        edge = pl.ds(side * (rows - EDGE), EDGE)
        return pltpu.make_async_remote_copy(
            adv.at[:, pl.ds(first_level(s, c), q), edge],
            cells.at[mine, pl.ds(c * q, q), edge],
            d_send.at[0], d_recv.at[c],
            device_id={"tracer": target(s)}, device_id_type=MESH,
        )

    def wait_blocks(c):
        settle(cells.at[pl.ds(0, (ranks - 1) * nt), pl.ds(c * q, q)], d_recv.at[c])

    partner = a * cores + cores - 1 - b

    def part_copy():
        return pltpu.make_async_remote_copy(
            pre.at[:, cores - 1 - b], part, o_send.at[0], o_recv.at[0],
            device_id={"tracer": partner}, device_id_type=MESH,
        )

    def over_copy(k):
        there = lax.rem(a + k, chips)
        return pltpu.make_async_remote_copy(
            joined.at[there], over.at[k - 1], o_send.at[k], o_recv.at[k],
            device_id={"tracer": there * cores + b}, device_id_type=MESH,
        )

    def gets_over(k):
        return lax.rem(a + k, chips) * cores + b > 0

    def in_cross(m):
        return lax.rem(m, cross), m // cross

    def in_near(m):
        return cross + m // nc, lax.rem(m, nc)

    last_core = a * cores + cores - 1
    late = b == cores - 1
    barrier = pltpu.get_barrier_semaphore()
    for s in range(cores - 1, cross, cores):
        pl.semaphore_signal(barrier, inc=1, device_id={"tracer": target(s)}, device_id_type=MESH)
    if cores > 1:
        @pl.when(jnp.logical_not(late))
        def _():
            for s in range(0, cross, cores):
                pl.semaphore_signal(
                    barrier, inc=1, device_id={"tracer": target(s)}, device_id_type=MESH
                )
            pl.semaphore_signal(barrier, inc=1, device_id={"tracer": last_core}, device_id_type=MESH)
    for place in (up, down):
        pl.semaphore_signal(
            barrier, inc=1, device_id={"tile": place, "tracer": last_core}, device_id_type=MESH
        )

    dep_local = pltpu.make_async_copy(dep, dext.at[body], ls_sem.at[0])
    th_local = pltpu.make_async_copy(th, hext.at[:, body], ls_sem.at[1])
    sun_local = pltpu.make_async_copy(sun, aux.at[1], ls_sem.at[2])
    tables = [
        pltpu.make_async_copy(src, dst, t_sem.at[k])
        for k, (src, dst) in enumerate(((eaten_in, eaten), (att_in, att), (rate_in, rate)))
    ]
    dep_local.start()
    tables[1].start()

    flow_local(0).start()

    def start_early(k, carry):
        early_local(k).start()
        return carry

    lax.fori_loop(0, early * cross, start_early, 0)
    for s in range(1, ranks):
        flow_local(s).start()

    tot[...] = jnp.zeros_like(tot)
    dep_local.wait()
    tables[1].wait()

    def advect(lev, block, base, size, skip, first, keep, put, t_0=0, some=nt):
        window = pl.ds(base, size)
        kept = pl.ds(first, keep)
        lane = lane_index((size, width))
        wet = jnp.where(lev < dext[window], 1.0, 0.0)
        es = sub_step * (fext[0, lev, window] * wet * east(wet))
        ns = sub_step * (fext[1, lev, window] * wet * north(wet))

        def one_tracer(k, acc):
            t = t_0 + k
            c = substep(ext[t, lev, window], es, ns, lane)
            c = substep(c, es, ns, lane)[skip:skip + keep]
            put(t, lev, kept, c)
            return acc + att[r * nt + t] * jnp.abs(c)

        tot[block, kept] = lax.fori_loop(0, some, one_tracer, tot[block, kept], unroll=True)

    def strip(ref, *lead):
        return jnp.concatenate(
            [ref[lead + (pl.ds(full - TILE, TILE),)], ref[lead + (pl.ds(0, PAD + TILE),)]], axis=0
        )

    def put_adv(t, lev, kept, c):
        adv[t, lev, kept] = c

    def put_cells(t, lev, kept, c):
        cells[r * nt + t, lev - r * per, kept] = c

    def advance_inner(s, c, i, h):
        lev = first_level(s, c) + i
        advect(lev, target(s), PAD, rows, EDGE, EDGE, rows - 2 * EDGE, put_adv, h * some, some)

    def advance_outer(s, c, i):
        lev = first_level(s, c) + i
        block = target(s)
        size = TILE + PAD + TILE
        lane = lane_index((size, width))
        wet = jnp.where(lev < strip(dext), 1.0, 0.0)
        es = sub_step * (strip(fext, 0, lev) * wet * east(wet))
        ns = sub_step * (strip(fext, 1, lev) * wet * north(wet))
        high, low = slice(TILE - EDGE, TILE), slice(TILE + PAD, TILE + PAD + EDGE)
        high_rows, low_rows = pl.ds(rows - EDGE, EDGE), pl.ds(0, EDGE)

        def one_tracer(t, acc):
            c = substep(strip(ext, t, lev), es, ns, lane)
            c = substep(c, es, ns, lane)
            adv[t, lev, high_rows] = c[high]
            adv[t, lev, low_rows] = c[low]
            return acc + att[r * nt + t] * jnp.abs(c)

        acc = lax.fori_loop(0, nt, one_tracer, jnp.zeros((size, width), jnp.float32), unroll=True)
        tot[block, high_rows] += acc[high]
        tot[block, low_rows] += acc[low]

    def advance(s, c, put):
        block = target(s)
        level_0 = first_level(s, c)

        def one_level(i, carry):
            advect(level_0 + i, block, 0, full, PAD, 0, rows, put)
            return carry

        lax.fori_loop(0, q, one_level, 0)

    def start_edges(order):
        def step(m, carry):
            for copy in edges(*order(m)):
                copy.start()
            return carry
        return step

    turn = jnp.where(late, 0, early * q * parts - 1)

    def inner_step(m, carry):
        h = lax.rem(m, parts)
        k, i = m // (q * parts), lax.rem(m // parts, q)
        s, c = k // early, lax.rem(k, early)

        @pl.when(m == 0)
        def _():
            flow_local(0).wait()

        @pl.when(m == early * q * parts)
        def _():
            settle(fext.at[:, pl.ds(0, (ranks - 1) * per), body], lf_sem.at[1])

        @pl.when(jnp.logical_and(i == 0, h == 0))
        def _():
            early_local(k).wait()

        advance_inner(s, c, i, h)

        @pl.when(m == 0)
        def _():
            pl.semaphore_wait(barrier, jnp.where(late, cross + cores - 1 + 2 * cores, chips - 1))

        inner_copy(s, c, i, h).start()

        @pl.when(m == turn)
        def _():
            if cores > 1:
                @pl.when(late)
                def _():
                    pl.semaphore_signal(
                        ready, inc=1, device_id={"tracer": partner}, device_id_type=MESH
                    )

                @pl.when(jnp.logical_not(late))
                def _():
                    pl.semaphore_wait(ready, 1)

            for copy in depth_edges():
                copy.start()
            lax.fori_loop(0, cross, start_edges(in_cross), 0)

        return carry

    lax.fori_loop(0, early * cross * q * parts, inner_step, 0)
    lax.fori_loop(cross, cross * nc, start_edges(in_cross), 0)
    for s in range(ranks):
        rest_local(s).start()
    lax.fori_loop(0, cores * nc, start_edges(in_near), 0)
    for copy in heat_edges():
        copy.start()
    th_local.start()
    sun_local.start()
    tables[0].start()
    tables[2].start()
    settle(dext.at[pl.ds(0, 2 * EDGE)], s_recv.at[1])

    def outer_step(k, carry):
        s, c = in_cross(k)

        @pl.when(s == 0)
        def _():
            wait_edges(c, cross * q)

        def sides(i, carry):
            advance_outer(s, c, i)
            return carry

        lax.fori_loop(0, q, sides, 0)
        for side in range(2):
            outer_copy(s, c, side).start()
        return carry

    lax.fori_loop(0, early * cross, outer_step, 0)

    settle(ext.at[:, pl.ds(0, nl - early * cross * q), body], l_sem.at[early * cross])

    def away_step(m, carry):
        far = m < cross * nc
        k = m - cross * nc
        s = jnp.where(far, lax.rem(m, cross), cross + k // nc)
        c = jnp.where(far, m // cross, lax.rem(k, nc))

        @pl.when(jnp.logical_and(far, s == 0))
        def _():
            wait_edges(c, cross * q)

        @pl.when(jnp.logical_and(jnp.logical_not(far), c == 0))
        def _():
            wait_edges(nc + s - cross, per)

        advance(s, c, put_adv)

        @pl.when(m != cross * nc - 1)
        def _():
            block_copy(s, c).start()

        return carry

    lax.fori_loop(early * cross, (ranks - 1) * nc, away_step, 0)

    def own_step(c, carry):
        advance(ranks - 1, c, put_cells)
        return carry

    wait_edges(nc + cores - 1, per)
    lax.fori_loop(0, nc, own_step, 0)

    above = jnp.zeros((rows, width), jnp.float32)
    for place in range(ranks):
        pre[place // cores, place % cores] = above
        above = above + tot[place]
    if cores > 1:
        part_copy().start()
        part_copy().wait()
        for k in range(chips):
            joined[k] = pre[k, b] + part[k]
    else:
        for k in range(chips):
            joined[k] = pre[k, b]
    for k in range(1, chips):
        @pl.when(gets_over(k))
        def _():
            over_copy(k).start()

    block_copy(cross - 1, nc - 1).start()

    th_local.wait()
    sun_local.wait()
    settle(hext.at[:, pl.ds(0, 2 * EDGE)], s_recv.at[0])
    lane = lane_index((full, width))
    coriolis = coriolis_base + beta_plane * lane.astype(jnp.float32) / width

    def momentum(i, carry):
        lev = r * per + i
        u, v, heat_ext = fext[0, lev], fext[1, lev], hext[i]
        wet = jnp.where(lev < dext[...], 1.0, 0.0)
        v_east, u_west = east(v), west(u)
        v_bar = 0.25 * (v + v_east + south(v) + south(v_east))
        u_bar = 0.25 * (u + u_west + north(u) + north(u_west))
        new_u = u + step_duration * (
            coriolis * v_bar - gravity * (east(heat_ext) - heat_ext) + viscosity * laplacian(u)
        )
        new_v = v + step_duration * (
            -coriolis * u_bar - gravity * (north(heat_ext) - heat_ext) + viscosity * laplacian(v)
        )
        vel[0, i] = (wet * east(wet) * new_u)[PAD:PAD + rows]
        vel[1, i] = (wet * north(wet) * new_v)[PAD:PAD + rows]
        warmer = heat_ext + step_duration * spreading_coefficient * laplacian(heat_ext)
        heat[i] = warmer[PAD:PAD + rows]
        return carry

    lax.fori_loop(0, per, momentum, 0)

    tables[0].wait()
    tables[2].wait()

    def invert(s, carry):
        who = jnp.int32(0)
        for t in range(count):
            who = jnp.where(eaten[t] == s, jnp.int32(t), who)
        eater[s] = who
        return carry

    lax.fori_loop(0, count, invert, 0)

    depth = dext[PAD:PAD + rows].astype(jnp.float32)
    aux[2] = depth
    scale = column_optical / nl
    clear = (r * per).astype(jnp.float32) * water_clear

    @pl.when(r == 0)
    def _():
        aux[0] = jnp.zeros((rows, width), jnp.float32)

    @pl.when(r > 0)
    def _():
        above = joined[a]
        for k in range(1, chips):
            over_copy(k).wait_recv()
            above = above + over[k - 1]
        aux[0] = (above + clear) * scale

    def react_chunk(c, carry):
        wait_blocks(c)

        def one_level(j, carry):
            i = c * q + j

            def put(t, x):
                cells[t, i] = x

            level = (r * per + i).astype(jnp.float32)
            wet, caught, below = react_level(
                count, level, aux[2], aux[1], aux[0], cells, i,
                eaten, eater, att, rate, scale, sat, pull, put,
            )
            aux[0] = below
            heat[i] = wet * (heat[i] + warming_coefficient * (caught * wet))
            return carry

        lax.fori_loop(0, q, one_level, 0)
        return carry

    lax.fori_loop(0, nc - 1, react_chunk, 0)

    settle(fc.at[:, :, pl.ds(0, LOW_FLOW + HIGH_FLOW)], edge_send.at[0])
    settle(sp.at[:, :, pl.ds(0, 2 * EDGE)], edge_send.at[1])
    settle(th.at[:, pl.ds(0, 2 * EDGE)], edge_send.at[2])
    settle(dep.at[pl.ds(0, 2 * EDGE)], edge_send.at[3])
    for k in range(1, chips):
        @pl.when(gets_over(k))
        def _():
            over_copy(k).wait_send()

    settle(adv.at[:, pl.ds(0, (ranks - 1) * per)], d_send.at[0])
    wait_blocks(nc - 1)


def finish_kernel(
    levels, q,
    cells, vel, heat, aux, eaten_in, att_in, rate_in,
    out, vel_out, temp_out,
    eaten, att, rate, last, warm, sat, pull, eater, sem, t_sem,
):
    count, per = cells.shape[:2]
    r = lax.axis_index("tracer")
    done = per - q
    scale = column_optical / levels
    copies = [
        pltpu.make_async_copy(cells.at[:, pl.ds(0, done)], out.at[:, pl.ds(0, done)], sem.at[0]),
        pltpu.make_async_copy(vel, vel_out, sem.at[1]),
        pltpu.make_async_copy(heat.at[pl.ds(0, done)], temp_out.at[pl.ds(0, done)], sem.at[2]),
    ]
    tables = [
        pltpu.make_async_copy(src, dst, t_sem.at[k])
        for k, (src, dst) in enumerate(((eaten_in, eaten), (att_in, att), (rate_in, rate)))
    ]
    for copy in tables + copies:
        copy.start()
    for copy in tables:
        copy.wait()
    for t in range(count):
        eater[eaten[t]] = t

    def level_copy(j):
        return pltpu.make_async_copy(last.at[j], out.at[:, done + j], sem.at[4])

    def one_level(j, tau):
        def put(t, x):
            last[j, t] = x

        level = (r * per + done + j).astype(jnp.float32)
        wet, caught, below = react_level(
            count, level, aux[2], aux[1], tau, cells, done + j,
            eaten, eater, att, rate, scale, sat, pull, put,
        )
        warm[j] = wet * (heat[done + j] + warming_coefficient * (caught * wet))
        level_copy(j).start()
        return below

    lax.fori_loop(0, q, one_level, aux[0])
    warm_copy = pltpu.make_async_copy(warm, temp_out.at[pl.ds(done, q)], sem.at[3])
    warm_copy.start()
    for copy in copies:
        copy.wait()
    pltpu.make_async_copy(last, last, sem.at[4]).wait()
    warm_copy.wait()


def solution(mesh):
    tiles, ranks = mesh.shape["tile"], mesh.shape["tracer"]
    cores = 2 if ranks % 2 == 0 else 1

    def on_device(
        species_amounts,
        face_currents,
        thermal_anomaly,
        layer_total_per_profile,
        consumed_species,
        attenuation_factor,
        intake_speedup,
        incoming_sunshine,
    ):
        nt, nl, rows, width = species_amounts.shape
        per = nl // ranks
        q = 2 if per % 2 == 0 else 1
        nc = per // q
        count = ranks * nt
        cross = ranks - cores
        chips = ranks // cores
        early = min(2, nc - 1)
        full = rows + PAD
        f32 = jnp.float32
        any_space = pl.BlockSpec(memory_space=pl.ANY)
        vmem = pl.BlockSpec(memory_space=pltpu.VMEM)
        dma = pltpu.SemaphoreType.DMA
        cells, vel, heat, aux = pl.pallas_call(
            functools.partial(transport_kernel, tiles, ranks, cores, q, early),
            out_shape=(
                pltpu.VMEM((count, per, rows, width), f32),
                pltpu.VMEM((2, per, rows, width), f32),
                pltpu.VMEM((per, rows, width), f32),
                pltpu.VMEM((3, rows, width), f32),
            ),
            in_specs=[any_space] * 8,
            out_specs=(vmem, vmem, vmem, vmem),
            scratch_shapes=[
                pltpu.SMEM((count,), jnp.int32),
                pltpu.SMEM((count,), f32),
                pltpu.SMEM((count,), f32),
                pltpu.VMEM((nt, nl, full, width), f32),
                pltpu.VMEM((2, nl, full, width), f32),
                pltpu.VMEM((per, full, width), f32),
                pltpu.VMEM((full, width), jnp.int32),
                pltpu.VMEM((nt, nl, rows, width), f32),
                pltpu.VMEM((ranks, rows, width), f32),
                pltpu.VMEM((chips, cores, rows, width), f32),
                pltpu.VMEM((chips, rows, width), f32),
                pltpu.VMEM((chips, rows, width), f32),
                pltpu.VMEM((chips, rows, width), f32),
                pltpu.VMEM((count, rows, width), f32),
                pltpu.VMEM((count, rows, width), f32),
                pltpu.SMEM((count,), jnp.int32),
                dma((4,)), dma((nc + cores,)), dma((nc + cores,)), dma((2,)),
                dma((1,)), dma((nc,)), dma((chips,)), dma((chips,)),
                dma((early * cross + 1,)), dma((2,)), dma((3,)), dma((3,)),
                pltpu.SemaphoreType.REGULAR,
            ],
            compiler_params=pltpu.CompilerParams(
                collective_id=0, has_side_effects=True, vmem_limit_bytes=48 << 20
            ),
            name="transport",
        )(
            *(pltpu.with_memory_space_constraint(x, HBM) for x in (
                species_amounts, face_currents, thermal_anomaly,
                layer_total_per_profile, incoming_sunshine,
                consumed_species, attenuation_factor, intake_speedup,
            ))
        )
        return pl.pallas_call(
            functools.partial(finish_kernel, nl, q),
            out_shape=(
                jax.ShapeDtypeStruct((count, per, rows, width), f32),
                jax.ShapeDtypeStruct((2, per, rows, width), f32),
                jax.ShapeDtypeStruct((per, rows, width), f32),
            ),
            in_specs=[vmem] * 4 + [any_space] * 3,
            out_specs=(any_space, any_space, any_space),
            scratch_shapes=[
                pltpu.SMEM((count,), jnp.int32),
                pltpu.SMEM((count,), f32),
                pltpu.SMEM((count,), f32),
                pltpu.VMEM((q, count, rows, width), f32),
                pltpu.VMEM((q, rows, width), f32),
                pltpu.VMEM((count, rows, width), f32),
                pltpu.VMEM((count, rows, width), f32),
                pltpu.SMEM((count,), jnp.int32),
                dma((5,)), dma((3,)),
            ],
            compiler_params=pltpu.CompilerParams(vmem_limit_bytes=32 << 20),
            name="finish",
        )(
            cells, vel, heat, aux,
            consumed_species, attenuation_factor, intake_speedup,
        )

    return jax.shard_map(
        on_device,
        mesh=mesh,
        in_specs=(
            P(("groups", "tracer"), None, "tile", None),
            P(None, "groups", "tile", None),
            P(("groups", "tracer"), "tile", None),
            P(("groups", "tile"), None),
            P(),
            P(),
            P(),
            P(("groups", "tile"), None),
        ),
        out_specs=(
            P("groups", "tracer", "tile", None),
            P(None, ("groups", "tracer"), "tile", None),
            P(("groups", "tracer"), "tile", None),
        ),
        check_vma=False,
    )
```

```python
import functools

import jax
import jax.numpy as jnp
from jax import lax
from jax.experimental import pallas as pl
from jax.experimental.pallas import tpu as pltpu
from jax.sharding import PartitionSpec as P

MESH = pl.DeviceIdType.MESH

sub_step = 0.45
step_duration = 0.2
gravity = 0.5
viscosity = 0.2
coriolis_base = 0.5
beta_plane = 0.5
spreading_coefficient = 0.2
water_clear = 0.05
column_optical = 3.0
warming_coefficient = 5.0
light_half = 0.3
nutrient_half = 0.5

PAD = 8
EDGE = 4
TILE = 8
LOW_FLOW, HIGH_FLOW = 3, 2

HBM = pltpu.HBM


def lane_index(shape):
    return lax.broadcasted_iota(jnp.int32, shape, len(shape) - 1)


def east(x):
    return pltpu.roll(x, x.shape[0] - 1, 0)


def west(x):
    return pltpu.roll(x, 1, 0)


def north(x):
    return jnp.where(lane_index(x.shape) == x.shape[1] - 1, 0.0, pltpu.roll(x, x.shape[1] - 1, 1))


def south(x):
    return jnp.where(lane_index(x.shape) == 0, 0.0, pltpu.roll(x, 1, 1))


def minmod(a, b):
    return jnp.maximum(jnp.minimum(a, b), jnp.minimum(jnp.maximum(a, b), 0.0))


def laplacian(x):
    return east(x) + west(x) + north(x) + south(x) - 4.0 * x


def substep(c, es, ns, lane):
    last = c.shape[1] - 1
    e = 0.5 * c
    d = east(e) - e
    half = minmod(west(d), d)
    flux = es * jnp.where(es > 0.0, c + half, east(c - half))
    spread = flux - west(flux)
    d = jnp.where(lane == last, 0.0, pltpu.roll(e, last, 1)) - e
    half = minmod(jnp.where(lane == 0, e, pltpu.roll(d, 1, 1)), d)
    flux = ns * jnp.where(ns > 0.0, c + half, pltpu.roll(c - half, last, 1))
    return c - (spread + (flux - pltpu.roll(flux, 1, 1)))


def react_level(count, level, depth, sun, tau, cells, c, eaten, eater, att, rate, scale, sat, pull, put):
    total = jnp.full(depth.shape, water_clear, jnp.float32)
    for t in range(count):
        x = cells[t, c]
        size = jnp.abs(x)
        total = total + att[t] * size
        sat[t] = x / (nutrient_half + size)
        pull[t] = rate[t] * x
    optical = total * scale
    wet = jnp.where(level < depth, 1.0, 0.0)
    caught = sun * jnp.exp(-tau) * (1.0 - jnp.exp(-optical))
    mean_light = caught / optical
    gain = wet * (mean_light / (mean_light + light_half))
    for t in range(count):
        change = pull[t] * sat[eaten[t]] - pull[eater[t]] * sat[t]
        put(t, cells[t, c] + gain * change)
    return wet, caught, tau + optical


def transport_kernel(
    tiles, ranks, cores, q, early,
    sp, fc, th, dep, sun, eaten_in, att_in, rate_in,
    cells, vel, heat, aux,
    eaten, att, rate, ext, fext, hext, dext, adv, tot, pre, part, joined, over, sat, pull, eater,
    edge_send, h_recv, f_recv, s_recv, d_send, d_recv, o_send, o_recv,
    l_sem, lf_sem, ls_sem, t_sem, ready,
):
    nt, nl, rows, width = sp.shape
    per = nl // ranks
    nc = per // q
    count = ranks * nt
    chips = ranks // cores
    cross = ranks - cores
    full = rows + PAD
    r = lax.axis_index("tracer")
    z = lax.axis_index("tile")
    a, b = r // cores, lax.rem(r, cores)
    up, down = lax.rem(z + 1, tiles), lax.rem(z + tiles - 1, tiles)

    def target(s):
        k = lax.rem(s, cores)
        chip = lax.rem(a + 1 + s // cores, chips)
        core = jnp.where(s < cross, k, lax.rem(b + cores - 1 - k, cores))
        return chip * cores + core

    def first_level(s, c):
        return target(s) * per + c * q

    mine = pl.ds(r * nt, nt)
    body = pl.ds(PAD, rows)
    inner = pl.ds(EDGE, rows - 2 * EDGE)

    def settle(ref, sem):
        pltpu.make_async_copy(ref, ref, sem).wait()

    def pair(src, dst, lead, send, recv, low=EDGE, high=EDGE):
        return (
            pltpu.make_async_remote_copy(
                src.at[lead + (pl.ds(rows - low, low),)],
                dst.at[lead + (pl.ds(PAD - low, low),)],
                send, recv, device_id={"tile": up}, device_id_type=MESH,
            ),
            pltpu.make_async_remote_copy(
                src.at[lead + (pl.ds(0, high),)],
                dst.at[lead + (pl.ds(0, high),)],
                send, recv, device_id={"tile": down}, device_id_type=MESH,
            ),
        )

    def edges(s, c):
        g = jnp.where(s < cross, c, nc + s - cross)
        lead = (slice(None), pl.ds(first_level(s, c), q))
        return (
            pair(fc, fext, lead, edge_send.at[0], f_recv.at[g], LOW_FLOW, HIGH_FLOW)
            + pair(sp, ext, lead, edge_send.at[1], h_recv.at[g])
        )

    def wait_edges(g, levels):
        settle(fext.at[:, pl.ds(0, levels), pl.ds(0, LOW_FLOW + HIGH_FLOW)], f_recv.at[g])
        settle(ext.at[:, pl.ds(0, levels), pl.ds(0, 2 * EDGE)], h_recv.at[g])

    def heat_edges():
        return pair(th, hext, (slice(None),), edge_send.at[2], s_recv.at[0])

    def depth_edges():
        return pair(dep, dext, (), edge_send.at[3], s_recv.at[1])

    def flow_local(s):
        lev = pl.ds(target(s) * per, per)
        sem = lf_sem.at[0] if s == 0 else lf_sem.at[1]
        return pltpu.make_async_copy(fc.at[:, lev], fext.at[:, lev, body], sem)

    def early_local(k):
        lev = pl.ds(first_level(k // early, lax.rem(k, early)), q)
        return pltpu.make_async_copy(sp.at[:, lev], ext.at[:, lev, body], l_sem.at[k])

    def rest_local(s):
        skip = early if s < cross else 0
        lev = pl.ds(first_level(s, skip), per - skip * q)
        return pltpu.make_async_copy(sp.at[:, lev], ext.at[:, lev, body], l_sem.at[early * cross])

    def block_copy(s, c):
        return pltpu.make_async_remote_copy(
            adv.at[:, pl.ds(first_level(s, c), q)],
            cells.at[mine, pl.ds(c * q, q)],
            d_send.at[0], d_recv.at[c],
            device_id={"tracer": target(s)}, device_id_type=MESH,
        )

    def inner_copy(s, c, i):
        return pltpu.make_async_remote_copy(
            adv.at[:, first_level(s, c) + i, inner],
            cells.at[mine, c * q + i, inner],
            d_send.at[0], d_recv.at[c],
            device_id={"tracer": target(s)}, device_id_type=MESH,
        )

    def outer_copy(s, c, side):
        edge = pl.ds(side * (rows - EDGE), EDGE)
        return pltpu.make_async_remote_copy(
            adv.at[:, pl.ds(first_level(s, c), q), edge],
            cells.at[mine, pl.ds(c * q, q), edge],
            d_send.at[0], d_recv.at[c],
            device_id={"tracer": target(s)}, device_id_type=MESH,
        )

    def wait_blocks(c):
        settle(cells.at[pl.ds(0, (ranks - 1) * nt), pl.ds(c * q, q)], d_recv.at[c])

    partner = a * cores + cores - 1 - b

    def part_copy():
        return pltpu.make_async_remote_copy(
            pre.at[:, cores - 1 - b], part, o_send.at[0], o_recv.at[0],
            device_id={"tracer": partner}, device_id_type=MESH,
        )

    def over_copy(k):
        there = lax.rem(a + k, chips)
        return pltpu.make_async_remote_copy(
            joined.at[there], over.at[k - 1], o_send.at[k], o_recv.at[k],
            device_id={"tracer": there * cores + b}, device_id_type=MESH,
        )

    def gets_over(k):
        return lax.rem(a + k, chips) * cores + b > 0

    def in_cross(m):
        return lax.rem(m, cross), m // cross

    def in_near(m):
        return cross + m // nc, lax.rem(m, nc)

    last_core = a * cores + cores - 1
    late = b == cores - 1
    barrier = pltpu.get_barrier_semaphore()
    for s in range(cores - 1, cross, cores):
        pl.semaphore_signal(barrier, inc=1, device_id={"tracer": target(s)}, device_id_type=MESH)
    if cores > 1:
        @pl.when(jnp.logical_not(late))
        def _():
            for s in range(0, cross, cores):
                pl.semaphore_signal(
                    barrier, inc=1, device_id={"tracer": target(s)}, device_id_type=MESH
                )
            pl.semaphore_signal(barrier, inc=1, device_id={"tracer": last_core}, device_id_type=MESH)
    for place in (up, down):
        pl.semaphore_signal(
            barrier, inc=1, device_id={"tile": place, "tracer": last_core}, device_id_type=MESH
        )

    dep_local = pltpu.make_async_copy(dep, dext.at[body], ls_sem.at[0])
    th_local = pltpu.make_async_copy(th, hext.at[:, body], ls_sem.at[1])
    sun_local = pltpu.make_async_copy(sun, aux.at[1], ls_sem.at[2])
    tables = [
        pltpu.make_async_copy(src, dst, t_sem.at[k])
        for k, (src, dst) in enumerate(((eaten_in, eaten), (att_in, att), (rate_in, rate)))
    ]
    dep_local.start()
    tables[1].start()

    flow_local(0).start()

    def start_early(k, carry):
        early_local(k).start()
        return carry

    lax.fori_loop(0, early * cross, start_early, 0)
    for s in range(1, ranks):
        flow_local(s).start()

    tot[...] = jnp.zeros_like(tot)
    dep_local.wait()
    tables[1].wait()

    def advect(lev, block, base, size, skip, first, keep, put):
        window = pl.ds(base, size)
        kept = pl.ds(first, keep)
        lane = lane_index((size, width))
        wet = jnp.where(lev < dext[window], 1.0, 0.0)
        es = sub_step * (fext[0, lev, window] * wet * east(wet))
        ns = sub_step * (fext[1, lev, window] * wet * north(wet))

        def one_tracer(t, acc):
            c = substep(ext[t, lev, window], es, ns, lane)
            c = substep(c, es, ns, lane)[skip:skip + keep]
            put(t, lev, kept, c)
            return acc + att[r * nt + t] * jnp.abs(c)

        tot[block, kept] = lax.fori_loop(0, nt, one_tracer, tot[block, kept], unroll=True)

    def strip(ref, *lead):
        return jnp.concatenate(
            [ref[lead + (pl.ds(full - TILE, TILE),)], ref[lead + (pl.ds(0, PAD + TILE),)]], axis=0
        )

    def put_adv(t, lev, kept, c):
        adv[t, lev, kept] = c

    def put_cells(t, lev, kept, c):
        cells[r * nt + t, lev - r * per, kept] = c

    def advance_inner(s, c, i):
        lev = first_level(s, c) + i
        advect(lev, target(s), PAD, rows, EDGE, EDGE, rows - 2 * EDGE, put_adv)

    def advance_outer(s, c, i):
        lev = first_level(s, c) + i
        block = target(s)
        size = TILE + PAD + TILE
        lane = lane_index((size, width))
        wet = jnp.where(lev < strip(dext), 1.0, 0.0)
        es = sub_step * (strip(fext, 0, lev) * wet * east(wet))
        ns = sub_step * (strip(fext, 1, lev) * wet * north(wet))
        high, low = slice(TILE - EDGE, TILE), slice(TILE + PAD, TILE + PAD + EDGE)
        high_rows, low_rows = pl.ds(rows - EDGE, EDGE), pl.ds(0, EDGE)

        def one_tracer(t, acc):
            c = substep(strip(ext, t, lev), es, ns, lane)
            c = substep(c, es, ns, lane)
            adv[t, lev, high_rows] = c[high]
            adv[t, lev, low_rows] = c[low]
            return acc + att[r * nt + t] * jnp.abs(c)

        acc = lax.fori_loop(0, nt, one_tracer, jnp.zeros((size, width), jnp.float32), unroll=True)
        tot[block, high_rows] += acc[high]
        tot[block, low_rows] += acc[low]

    def advance(s, c, put):
        block = target(s)
        level_0 = first_level(s, c)

        def one_level(i, carry):
            advect(level_0 + i, block, 0, full, PAD, 0, rows, put)
            return carry

        lax.fori_loop(0, q, one_level, 0)

    def start_edges(order):
        def step(m, carry):
            for copy in edges(*order(m)):
                copy.start()
            return carry
        return step

    turn = jnp.where(late, 0, early * q - 1)

    def inner_step(m, carry):
        k, i = m // q, lax.rem(m, q)
        s, c = k // early, lax.rem(k, early)

        @pl.when(m == 0)
        def _():
            flow_local(0).wait()

        @pl.when(m == early * q)
        def _():
            settle(fext.at[:, pl.ds(0, (ranks - 1) * per), body], lf_sem.at[1])

        @pl.when(i == 0)
        def _():
            early_local(k).wait()

        advance_inner(s, c, i)

        @pl.when(m == 0)
        def _():
            pl.semaphore_wait(barrier, jnp.where(late, cross + cores - 1 + 2 * cores, chips - 1))

        inner_copy(s, c, i).start()

        @pl.when(m == turn)
        def _():
            if cores > 1:
                @pl.when(late)
                def _():
                    pl.semaphore_signal(
                        ready, inc=1, device_id={"tracer": partner}, device_id_type=MESH
                    )

                @pl.when(jnp.logical_not(late))
                def _():
                    pl.semaphore_wait(ready, 1)

            for copy in depth_edges():
                copy.start()
            lax.fori_loop(0, cross, start_edges(in_cross), 0)

        return carry

    lax.fori_loop(0, early * cross * q, inner_step, 0)
    lax.fori_loop(cross, cross * nc, start_edges(in_cross), 0)
    for s in range(ranks):
        rest_local(s).start()
    lax.fori_loop(0, cores * nc, start_edges(in_near), 0)
    for copy in heat_edges():
        copy.start()
    th_local.start()
    sun_local.start()
    tables[0].start()
    tables[2].start()
    settle(dext.at[pl.ds(0, 2 * EDGE)], s_recv.at[1])

    def outer_step(k, carry):
        s, c = in_cross(k)

        @pl.when(s == 0)
        def _():
            wait_edges(c, cross * q)

        def sides(i, carry):
            advance_outer(s, c, i)
            return carry

        lax.fori_loop(0, q, sides, 0)
        for side in range(2):
            outer_copy(s, c, side).start()
        return carry

    lax.fori_loop(0, early * cross, outer_step, 0)

    settle(ext.at[:, pl.ds(0, nl - early * cross * q), body], l_sem.at[early * cross])

    def away_step(m, carry):
        far = m < cross * nc
        k = m - cross * nc
        s = jnp.where(far, lax.rem(m, cross), cross + k // nc)
        c = jnp.where(far, m // cross, lax.rem(k, nc))

        @pl.when(jnp.logical_and(far, s == 0))
        def _():
            wait_edges(c, cross * q)

        @pl.when(jnp.logical_and(jnp.logical_not(far), c == 0))
        def _():
            wait_edges(nc + s - cross, per)

        advance(s, c, put_adv)

        @pl.when(m != cross * nc - 1)
        def _():
            block_copy(s, c).start()

        return carry

    lax.fori_loop(early * cross, (ranks - 1) * nc, away_step, 0)

    def own_step(c, carry):
        advance(ranks - 1, c, put_cells)
        return carry

    wait_edges(nc + cores - 1, per)
    lax.fori_loop(0, nc, own_step, 0)

    above = jnp.zeros((rows, width), jnp.float32)
    for place in range(ranks):
        pre[place // cores, place % cores] = above
        above = above + tot[place]
    if cores > 1:
        part_copy().start()
        part_copy().wait()
        for k in range(chips):
            joined[k] = pre[k, b] + part[k]
    else:
        for k in range(chips):
            joined[k] = pre[k, b]
    for k in range(1, chips):
        @pl.when(gets_over(k))
        def _():
            over_copy(k).start()

    block_copy(cross - 1, nc - 1).start()

    th_local.wait()
    sun_local.wait()
    settle(hext.at[:, pl.ds(0, 2 * EDGE)], s_recv.at[0])
    lane = lane_index((full, width))
    coriolis = coriolis_base + beta_plane * lane.astype(jnp.float32) / width

    def momentum(i, carry):
        lev = r * per + i
        u, v, heat_ext = fext[0, lev], fext[1, lev], hext[i]
        wet = jnp.where(lev < dext[...], 1.0, 0.0)
        v_east, u_west = east(v), west(u)
        v_bar = 0.25 * (v + v_east + south(v) + south(v_east))
        u_bar = 0.25 * (u + u_west + north(u) + north(u_west))
        new_u = u + step_duration * (
            coriolis * v_bar - gravity * (east(heat_ext) - heat_ext) + viscosity * laplacian(u)
        )
        new_v = v + step_duration * (
            -coriolis * u_bar - gravity * (north(heat_ext) - heat_ext) + viscosity * laplacian(v)
        )
        vel[0, i] = (wet * east(wet) * new_u)[PAD:PAD + rows]
        vel[1, i] = (wet * north(wet) * new_v)[PAD:PAD + rows]
        warmer = heat_ext + step_duration * spreading_coefficient * laplacian(heat_ext)
        heat[i] = warmer[PAD:PAD + rows]
        return carry

    lax.fori_loop(0, per, momentum, 0)

    tables[0].wait()
    tables[2].wait()

    def invert(s, carry):
        who = jnp.int32(0)
        for t in range(count):
            who = jnp.where(eaten[t] == s, jnp.int32(t), who)
        eater[s] = who
        return carry

    lax.fori_loop(0, count, invert, 0)

    depth = dext[PAD:PAD + rows].astype(jnp.float32)
    aux[2] = depth
    scale = column_optical / nl
    clear = (r * per).astype(jnp.float32) * water_clear

    @pl.when(r == 0)
    def _():
        aux[0] = jnp.zeros((rows, width), jnp.float32)

    @pl.when(r > 0)
    def _():
        above = joined[a]
        for k in range(1, chips):
            over_copy(k).wait_recv()
            above = above + over[k - 1]
        aux[0] = (above + clear) * scale

    def react_chunk(c, carry):
        wait_blocks(c)

        def one_level(j, carry):
            i = c * q + j

            def put(t, x):
                cells[t, i] = x

            level = (r * per + i).astype(jnp.float32)
            wet, caught, below = react_level(
                count, level, aux[2], aux[1], aux[0], cells, i,
                eaten, eater, att, rate, scale, sat, pull, put,
            )
            aux[0] = below
            heat[i] = wet * (heat[i] + warming_coefficient * (caught * wet))
            return carry

        lax.fori_loop(0, q, one_level, 0)
        return carry

    lax.fori_loop(0, nc - 1, react_chunk, 0)

    settle(fc.at[:, :, pl.ds(0, LOW_FLOW + HIGH_FLOW)], edge_send.at[0])
    settle(sp.at[:, :, pl.ds(0, 2 * EDGE)], edge_send.at[1])
    settle(th.at[:, pl.ds(0, 2 * EDGE)], edge_send.at[2])
    settle(dep.at[pl.ds(0, 2 * EDGE)], edge_send.at[3])
    for k in range(1, chips):
        @pl.when(gets_over(k))
        def _():
            over_copy(k).wait_send()

    settle(adv.at[:, pl.ds(0, (ranks - 1) * per)], d_send.at[0])
    wait_blocks(nc - 1)


def finish_kernel(
    levels, q,
    cells, vel, heat, aux, eaten_in, att_in, rate_in,
    out, vel_out, temp_out,
    eaten, att, rate, last, warm, sat, pull, eater, sem, t_sem,
):
    count, per = cells.shape[:2]
    r = lax.axis_index("tracer")
    done = per - q
    scale = column_optical / levels
    copies = [
        pltpu.make_async_copy(cells.at[:, pl.ds(0, done)], out.at[:, pl.ds(0, done)], sem.at[0]),
        pltpu.make_async_copy(vel, vel_out, sem.at[1]),
        pltpu.make_async_copy(heat.at[pl.ds(0, done)], temp_out.at[pl.ds(0, done)], sem.at[2]),
    ]
    tables = [
        pltpu.make_async_copy(src, dst, t_sem.at[k])
        for k, (src, dst) in enumerate(((eaten_in, eaten), (att_in, att), (rate_in, rate)))
    ]
    for copy in tables + copies:
        copy.start()
    for copy in tables:
        copy.wait()
    for t in range(count):
        eater[eaten[t]] = t

    def level_copy(j):
        return pltpu.make_async_copy(last.at[j], out.at[:, done + j], sem.at[4])

    def one_level(j, tau):
        def put(t, x):
            last[j, t] = x

        level = (r * per + done + j).astype(jnp.float32)
        wet, caught, below = react_level(
            count, level, aux[2], aux[1], tau, cells, done + j,
            eaten, eater, att, rate, scale, sat, pull, put,
        )
        warm[j] = wet * (heat[done + j] + warming_coefficient * (caught * wet))
        level_copy(j).start()
        return below

    lax.fori_loop(0, q, one_level, aux[0])
    warm_copy = pltpu.make_async_copy(warm, temp_out.at[pl.ds(done, q)], sem.at[3])
    warm_copy.start()
    for copy in copies:
        copy.wait()
    pltpu.make_async_copy(last, last, sem.at[4]).wait()
    warm_copy.wait()


def solution(mesh):
    tiles, ranks = mesh.shape["tile"], mesh.shape["tracer"]
    cores = 2 if ranks % 2 == 0 else 1

    def on_device(
        species_amounts,
        face_currents,
        thermal_anomaly,
        layer_total_per_profile,
        consumed_species,
        attenuation_factor,
        intake_speedup,
        incoming_sunshine,
    ):
        nt, nl, rows, width = species_amounts.shape
        per = nl // ranks
        q = 2 if per % 2 == 0 else 1
        nc = per // q
        count = ranks * nt
        cross = ranks - cores
        chips = ranks // cores
        early = min(2, nc - 1)
        full = rows + PAD
        f32 = jnp.float32
        any_space = pl.BlockSpec(memory_space=pl.ANY)
        vmem = pl.BlockSpec(memory_space=pltpu.VMEM)
        dma = pltpu.SemaphoreType.DMA
        cells, vel, heat, aux = pl.pallas_call(
            functools.partial(transport_kernel, tiles, ranks, cores, q, early),
            out_shape=(
                pltpu.VMEM((count, per, rows, width), f32),
                pltpu.VMEM((2, per, rows, width), f32),
                pltpu.VMEM((per, rows, width), f32),
                pltpu.VMEM((3, rows, width), f32),
            ),
            in_specs=[any_space] * 8,
            out_specs=(vmem, vmem, vmem, vmem),
            scratch_shapes=[
                pltpu.SMEM((count,), jnp.int32),
                pltpu.SMEM((count,), f32),
                pltpu.SMEM((count,), f32),
                pltpu.VMEM((nt, nl, full, width), f32),
                pltpu.VMEM((2, nl, full, width), f32),
                pltpu.VMEM((per, full, width), f32),
                pltpu.VMEM((full, width), jnp.int32),
                pltpu.VMEM((nt, nl, rows, width), f32),
                pltpu.VMEM((ranks, rows, width), f32),
                pltpu.VMEM((chips, cores, rows, width), f32),
                pltpu.VMEM((chips, rows, width), f32),
                pltpu.VMEM((chips, rows, width), f32),
                pltpu.VMEM((chips, rows, width), f32),
                pltpu.VMEM((count, rows, width), f32),
                pltpu.VMEM((count, rows, width), f32),
                pltpu.SMEM((count,), jnp.int32),
                dma((4,)), dma((nc + cores,)), dma((nc + cores,)), dma((2,)),
                dma((1,)), dma((nc,)), dma((chips,)), dma((chips,)),
                dma((early * cross + 1,)), dma((2,)), dma((3,)), dma((3,)),
                pltpu.SemaphoreType.REGULAR,
            ],
            compiler_params=pltpu.CompilerParams(
                collective_id=0, has_side_effects=True, vmem_limit_bytes=48 << 20
            ),
            name="transport",
        )(
            *(pltpu.with_memory_space_constraint(x, HBM) for x in (
                species_amounts, face_currents, thermal_anomaly,
                layer_total_per_profile, incoming_sunshine,
                consumed_species, attenuation_factor, intake_speedup,
            ))
        )
        return pl.pallas_call(
            functools.partial(finish_kernel, nl, q),
            out_shape=(
                jax.ShapeDtypeStruct((count, per, rows, width), f32),
                jax.ShapeDtypeStruct((2, per, rows, width), f32),
                jax.ShapeDtypeStruct((per, rows, width), f32),
            ),
            in_specs=[vmem] * 4 + [any_space] * 3,
            out_specs=(any_space, any_space, any_space),
            scratch_shapes=[
                pltpu.SMEM((count,), jnp.int32),
                pltpu.SMEM((count,), f32),
                pltpu.SMEM((count,), f32),
                pltpu.VMEM((q, count, rows, width), f32),
                pltpu.VMEM((q, rows, width), f32),
                pltpu.VMEM((count, rows, width), f32),
                pltpu.VMEM((count, rows, width), f32),
                pltpu.SMEM((count,), jnp.int32),
                dma((5,)), dma((3,)),
            ],
            compiler_params=pltpu.CompilerParams(vmem_limit_bytes=32 << 20),
            name="finish",
        )(
            cells, vel, heat, aux,
            consumed_species, attenuation_factor, intake_speedup,
        )

    return jax.shard_map(
        on_device,
        mesh=mesh,
        in_specs=(
            P(("groups", "tracer"), None, "tile", None),
            P(None, "groups", "tile", None),
            P(("groups", "tracer"), "tile", None),
            P(("groups", "tile"), None),
            P(),
            P(),
            P(),
            P(("groups", "tile"), None),
        ),
        out_specs=(
            P("groups", "tracer", "tile", None),
            P(None, ("groups", "tracer"), "tile", None),
            P(("groups", "tracer"), "tile", None),
        ),
        check_vma=False,
    )
```

```python
import functools

import jax
import jax.numpy as jnp
from jax import lax
from jax.experimental import pallas as pl
from jax.experimental.pallas import tpu as pltpu
from jax.sharding import PartitionSpec as P

MESH = pl.DeviceIdType.MESH

sub_step = 0.45
step_duration = 0.2
gravity = 0.5
viscosity = 0.2
coriolis_base = 0.5
beta_plane = 0.5
spreading_coefficient = 0.2
water_clear = 0.05
column_optical = 3.0
warming_coefficient = 5.0
light_half = 0.3
nutrient_half = 0.5

PAD = 8
EDGE = 4
TILE = 8
LOW_FLOW, HIGH_FLOW = 3, 2
DEEP = 3

HBM = pltpu.HBM


def lane_index(shape):
    return lax.broadcasted_iota(jnp.int32, shape, len(shape) - 1)


def east(x):
    return pltpu.roll(x, x.shape[0] - 1, 0)


def west(x):
    return pltpu.roll(x, 1, 0)


def north(x):
    return jnp.where(lane_index(x.shape) == x.shape[1] - 1, 0.0, pltpu.roll(x, x.shape[1] - 1, 1))


def south(x):
    return jnp.where(lane_index(x.shape) == 0, 0.0, pltpu.roll(x, 1, 1))


def minmod(a, b):
    return jnp.maximum(jnp.minimum(a, b), jnp.minimum(jnp.maximum(a, b), 0.0))


def laplacian(x):
    return east(x) + west(x) + north(x) + south(x) - 4.0 * x


def substep(c, es, ns, lane):
    last = c.shape[1] - 1
    e = 0.5 * c
    d = east(e) - e
    half = minmod(west(d), d)
    flux = es * jnp.where(es > 0.0, c + half, east(c - half))
    spread = flux - west(flux)
    d = jnp.where(lane == last, 0.0, pltpu.roll(e, last, 1)) - e
    half = minmod(jnp.where(lane == 0, e, pltpu.roll(d, 1, 1)), d)
    flux = ns * jnp.where(ns > 0.0, c + half, pltpu.roll(c - half, last, 1))
    return c - (spread + (flux - pltpu.roll(flux, 1, 1)))


def react_level(count, level, depth, sun, tau, cells, c, eaten, eater, att, rate, scale, sat, pull, put):
    total = jnp.full(depth.shape, water_clear, jnp.float32)
    for t in range(count):
        x = cells[t, c]
        size = jnp.abs(x)
        total = total + att[t] * size
        sat[t] = x / (nutrient_half + size)
        pull[t] = rate[t] * x
    optical = total * scale
    wet = jnp.where(level < depth, 1.0, 0.0)
    caught = sun * jnp.exp(-tau) * (1.0 - jnp.exp(-optical))
    mean_light = caught / optical
    gain = wet * (mean_light / (mean_light + light_half))
    for t in range(count):
        change = pull[t] * sat[eaten[t]] - pull[eater[t]] * sat[t]
        put(t, cells[t, c] + gain * change)
    return wet, caught, tau + optical


def transport_kernel(
    tiles, ranks, cores, q, deep,
    sp, fc, th, dep, sun, eaten_in, att_in, rate_in,
    cells, vel, heat, aux,
    eaten, att, rate, ext, fext, hext, dext, adv, tot, pre, part, joined, over, sat, pull, eater, raw,
    edge_send, h_recv, f_recv, s_recv, d_send, d_recv, o_send, o_recv,
    l_sem, lf_sem, ls_sem, t_sem, r_send, r_recv, ready,
):
    nt, nl, rows, width = sp.shape
    per = nl // ranks
    nc = per // q
    count = ranks * nt
    chips = ranks // cores
    cross = ranks - cores
    full = rows + PAD
    early = deep + cross - 1
    r = lax.axis_index("tracer")
    z = lax.axis_index("tile")
    a, b = r // cores, lax.rem(r, cores)
    up, down = lax.rem(z + 1, tiles), lax.rem(z + tiles - 1, tiles)

    def target(s):
        k = lax.rem(s, cores)
        chip = lax.rem(a + 1 + s // cores, chips)
        core = jnp.where(s < cross, k, lax.rem(b + cores - 1 - k, cores))
        return chip * cores + core

    def first_level(s, c):
        return target(s) * per + c * q

    mine = pl.ds(r * nt, nt)
    body = pl.ds(PAD, rows)
    inner = pl.ds(EDGE, rows - 2 * EDGE)

    def settle(ref, sem):
        pltpu.make_async_copy(ref, ref, sem).wait()

    def pair(src, dst, lead, send, recv, low=EDGE, high=EDGE):
        return (
            pltpu.make_async_remote_copy(
                src.at[lead + (pl.ds(rows - low, low),)],
                dst.at[lead + (pl.ds(PAD - low, low),)],
                send, recv, device_id={"tile": up}, device_id_type=MESH,
            ),
            pltpu.make_async_remote_copy(
                src.at[lead + (pl.ds(0, high),)],
                dst.at[lead + (pl.ds(0, high),)],
                send, recv, device_id={"tile": down}, device_id_type=MESH,
            ),
        )

    def edges(s, c):
        g = jnp.where(s < cross, c, nc + (s - cross) * nc + c)
        lead = (slice(None), pl.ds(first_level(s, c), q))
        return (
            pair(fc, fext, lead, edge_send.at[0], f_recv.at[g], LOW_FLOW, HIGH_FLOW)
            + pair(sp, ext, lead, edge_send.at[1], h_recv.at[g])
        )

    def wait_edges(g, levels):
        settle(fext.at[:, pl.ds(0, levels), pl.ds(0, LOW_FLOW + HIGH_FLOW)], f_recv.at[g])
        settle(ext.at[:, pl.ds(0, levels), pl.ds(0, 2 * EDGE)], h_recv.at[g])

    def heat_edges():
        return pair(th, hext, (slice(None),), edge_send.at[2], s_recv.at[0])

    def depth_edges():
        return pair(dep, dext, (), edge_send.at[3], s_recv.at[1])

    def flow_local(s):
        lev = pl.ds(target(s) * per, per)
        sem = lf_sem.at[0] if s == 0 else lf_sem.at[1]
        return pltpu.make_async_copy(fc.at[:, lev], fext.at[:, lev, body], sem)

    def early_chunk(k):
        return jnp.where(k < deep, 0, k - deep + 1), jnp.where(k < deep, k, 0)

    def edge_chunk(k):
        return jnp.where(k < cross, k, 0), jnp.where(k < cross, 0, k - cross + 1)

    def early_local(k):
        lev = pl.ds(first_level(*early_chunk(k)), q)
        return pltpu.make_async_copy(sp.at[:, lev], ext.at[:, lev, body], l_sem.at[k])

    def rest_local(s):
        skip = deep if s == 0 else 1 if s < cross else 0
        lev = pl.ds(first_level(s, skip), per - skip * q)
        return pltpu.make_async_copy(sp.at[:, lev], ext.at[:, lev, body], l_sem.at[early])

    def block_copy(s, c):
        return pltpu.make_async_remote_copy(
            adv.at[:, pl.ds(first_level(s, c), q)],
            cells.at[mine, pl.ds(c * q, q)],
            d_send.at[0], d_recv.at[c],
            device_id={"tracer": target(s)}, device_id_type=MESH,
        )

    def inner_copy(s, c, i):
        return pltpu.make_async_remote_copy(
            adv.at[:, first_level(s, c) + i, inner],
            cells.at[mine, c * q + i, inner],
            d_send.at[1], d_recv.at[jnp.where(c == 0, nc, c)],
            device_id={"tracer": target(s)}, device_id_type=MESH,
        )

    def outer_copy(s, c, side):
        edge = pl.ds(side * (rows - EDGE), EDGE)
        return pltpu.make_async_remote_copy(
            adv.at[:, pl.ds(first_level(s, c), q), edge],
            cells.at[mine, pl.ds(c * q, q), edge],
            d_send.at[2], d_recv.at[c],
            device_id={"tracer": target(s)}, device_id_type=MESH,
        )

    def raw_copy():
        return pltpu.make_async_remote_copy(
            sp.at[:, first_level(0, 0)], raw, r_send.at[0], r_recv.at[0],
            device_id={"tracer": target(0)}, device_id_type=MESH,
        )

    def wait_first():
        settle(ext.at[:, pl.ds(0, q * (cross + rows // TILE)), pl.ds(0, TILE)], d_recv.at[0])
        for pieces, mask in ((cross * q, late), (cross * q - 1, jnp.logical_not(late))):
            @pl.when(mask)
            def _():
                settle(ext.at[:, pl.ds(0, pieces), inner], d_recv.at[nc])

    def wait_blocks(c):
        settle(cells.at[pl.ds(0, (ranks - 1) * nt), pl.ds(c * q, q)], d_recv.at[c])

    partner = a * cores + cores - 1 - b

    def part_copy():
        return pltpu.make_async_remote_copy(
            pre.at[:, cores - 1 - b], part, o_send.at[0], o_recv.at[0],
            device_id={"tracer": partner}, device_id_type=MESH,
        )

    def over_copy(k):
        there = lax.rem(a + k, chips)
        return pltpu.make_async_remote_copy(
            joined.at[there], over.at[k - 1], o_send.at[k], o_recv.at[k],
            device_id={"tracer": there * cores + b}, device_id_type=MESH,
        )

    def gets_over(k):
        return lax.rem(a + k, chips) * cores + b > 0

    def in_cross(m):
        return lax.rem(m, cross), m // cross

    def in_near(m):
        return cross + m // nc, lax.rem(m, nc)

    last_core = a * cores + cores - 1
    late = b == cores - 1
    barrier = pltpu.get_barrier_semaphore()
    for s in range(cores - 1, cross, cores):
        pl.semaphore_signal(barrier, inc=1, device_id={"tracer": target(s)}, device_id_type=MESH)
    if cores > 1:
        @pl.when(jnp.logical_not(late))
        def _():
            for s in range(0, cross, cores):
                pl.semaphore_signal(
                    barrier, inc=1, device_id={"tracer": target(s)}, device_id_type=MESH
                )
            pl.semaphore_signal(barrier, inc=1, device_id={"tracer": last_core}, device_id_type=MESH)
    for place in (up, down):
        pl.semaphore_signal(
            barrier, inc=1, device_id={"tile": place, "tracer": last_core}, device_id_type=MESH
        )

    dep_local = pltpu.make_async_copy(dep, dext.at[body], ls_sem.at[0])
    th_local = pltpu.make_async_copy(th, hext.at[:, body], ls_sem.at[1])
    sun_local = pltpu.make_async_copy(sun, aux.at[1], ls_sem.at[2])
    tables = [
        pltpu.make_async_copy(src, dst, t_sem.at[k])
        for k, (src, dst) in enumerate(((eaten_in, eaten), (att_in, att), (rate_in, rate)))
    ]
    dep_local.start()
    tables[1].start()

    flow_local(0).start()

    def start_early(k, carry):
        early_local(k).start()
        return carry

    lax.fori_loop(0, early, start_early, 0)
    for s in range(1, ranks):
        flow_local(s).start()

    @pl.when(jnp.logical_not(late))
    def _():
        pl.semaphore_wait(barrier, chips - 1)
        raw_copy().start()

    tot[...] = jnp.zeros_like(tot)
    dep_local.wait()
    tables[1].wait()

    def advect(lev, block, base, size, skip, first, keep, put, take=None, owner=r):
        window = pl.ds(base, size)
        kept = pl.ds(first, keep)
        lane = lane_index((size, width))
        wet = jnp.where(lev < dext[window], 1.0, 0.0)
        es = sub_step * (fext[0, lev, window] * wet * east(wet))
        ns = sub_step * (fext[1, lev, window] * wet * north(wet))

        def one_tracer(t, acc):
            c = substep(take(t) if take else ext[t, lev, window], es, ns, lane)
            c = substep(c, es, ns, lane)[skip:skip + keep]
            put(t, lev, kept, c)
            return acc + att[owner * nt + t] * jnp.abs(c)

        tot[block, kept] = lax.fori_loop(0, nt, one_tracer, tot[block, kept], unroll=True)

    def strip(ref, *lead):
        return jnp.concatenate(
            [ref[lead + (pl.ds(full - TILE, TILE),)], ref[lead + (pl.ds(0, PAD + TILE),)]], axis=0
        )

    def put_adv(t, lev, kept, c):
        adv[t, lev, kept] = c

    def put_cells(t, lev, kept, c):
        cells[r * nt + t, lev - r * per, kept] = c

    def advance_inner(s, c, i):
        lev = first_level(s, c) + i
        advect(lev, target(s), PAD, rows, EDGE, EDGE, rows - 2 * EDGE, put_adv)

    def advance_outer(s, c, i):
        lev = first_level(s, c) + i
        block = target(s)
        size = TILE + PAD + TILE
        lane = lane_index((size, width))
        wet = jnp.where(lev < strip(dext), 1.0, 0.0)
        es = sub_step * (strip(fext, 0, lev) * wet * east(wet))
        ns = sub_step * (strip(fext, 1, lev) * wet * north(wet))
        high, low = slice(TILE - EDGE, TILE), slice(TILE + PAD, TILE + PAD + EDGE)
        high_rows, low_rows = pl.ds(rows - EDGE, EDGE), pl.ds(0, EDGE)

        def one_tracer(t, acc):
            c = substep(strip(ext, t, lev), es, ns, lane)
            c = substep(c, es, ns, lane)
            adv[t, lev, high_rows] = c[high]
            adv[t, lev, low_rows] = c[low]
            return acc + att[r * nt + t] * jnp.abs(c)

        acc = lax.fori_loop(0, nt, one_tracer, jnp.zeros((size, width), jnp.float32), unroll=True)
        tot[block, high_rows] += acc[high]
        tot[block, low_rows] += acc[low]

    def advance(s, c, put):
        block = target(s)
        level_0 = first_level(s, c)

        def one_level(i, carry):
            advect(level_0 + i, block, 0, full, PAD, 0, rows, put)
            return carry

        lax.fori_loop(0, q, one_level, 0)

    def start_edges(order):
        def step(m, carry):
            for copy in edges(*order(m)):
                copy.start()
            return carry
        return step

    turn = jnp.where(late, 0, deep * q - 1)

    def inner_step(m, carry):
        k, i = m // q, lax.rem(m, q)
        s, c = early_chunk(k)

        @pl.when(m == 0)
        def _():
            flow_local(0).wait()

        @pl.when(m == deep * q)
        def _():
            settle(fext.at[:, pl.ds(0, (ranks - 1) * per), body], lf_sem.at[1])

        @pl.when(i == 0)
        def _():
            early_local(k).wait()

        @pl.when(jnp.logical_or(late, m > 0))
        def _():
            advance_inner(s, c, i)

            @pl.when(m == 0)
            def _():
                pl.semaphore_wait(barrier, cross + cores - 1 + 2 * cores)

            inner_copy(s, c, i).start()

        @pl.when(m == turn)
        def _():
            if cores > 1:
                @pl.when(late)
                def _():
                    pl.semaphore_signal(
                        ready, inc=1, device_id={"tracer": partner}, device_id_type=MESH
                    )

                @pl.when(jnp.logical_not(late))
                def _():
                    pl.semaphore_wait(ready, 1)

            for copy in depth_edges():
                copy.start()
            lax.fori_loop(0, cross, start_edges(in_cross), 0)

        return carry

    lax.fori_loop(0, early * q, inner_step, 0)
    lax.fori_loop(cross, cross * nc, start_edges(in_cross), 0)
    for s in range(ranks):
        rest_local(s).start()
    lax.fori_loop(0, cores * nc, start_edges(in_near), 0)
    for copy in heat_edges():
        copy.start()
    th_local.start()
    sun_local.start()
    tables[0].start()
    tables[2].start()
    settle(dext.at[pl.ds(0, 2 * EDGE)], s_recv.at[1])

    def outer_step(k, carry):
        s, c = edge_chunk(k)

        @pl.when(s == 0)
        def _():
            wait_edges(c, cross * q)

        def sides(i, carry):
            advance_outer(s, c, i)
            return carry

        lax.fori_loop(0, q, sides, 0)
        for side in range(2):
            outer_copy(s, c, side).start()
        return carry

    lax.fori_loop(0, early, outer_step, 0)

    settle(ext.at[:, pl.ds(0, nl - early * q), body], l_sem.at[early])

    def away_step(m, carry):
        far = m < cross * nc
        k = m - cross * nc
        s = jnp.where(far, lax.rem(m, cross), cross + k // nc)
        c = jnp.where(far, m // cross, lax.rem(k, nc))

        @pl.when(jnp.logical_and(far, jnp.logical_and(s == 0, c >= deep)))
        def _():
            wait_edges(c, cross * q)

        @pl.when(jnp.logical_not(far))
        def _():
            wait_edges(nc + k, q)

        @pl.when(jnp.logical_or(s > 0, c >= deep))
        def _():
            advance(s, c, put_adv)

            @pl.when(m != cross * nc - 1)
            def _():
                block_copy(s, c).start()

        return carry

    lax.fori_loop(cross, (ranks - 1) * nc, away_step, 0)

    @pl.when(jnp.logical_not(late))
    def _():
        giver = lax.rem(a + chips - 1, chips) * cores

        def put_given(t, lev, kept, c):
            cells[giver * nt + t, 0, kept] = c

        pltpu.make_async_copy(raw, raw, r_recv.at[0]).wait()
        advect(
            r * per, r, PAD, rows, EDGE, EDGE, rows - 2 * EDGE, put_given,
            lambda t: raw[t], giver,
        )

    def own_step(c, carry):
        wait_edges(cores * nc + c, q)
        advance(ranks - 1, c, put_cells)
        return carry

    lax.fori_loop(0, nc, own_step, 0)

    above = jnp.zeros((rows, width), jnp.float32)
    for place in range(ranks):
        pre[place // cores, place % cores] = above
        above = above + tot[place]
    if cores > 1:
        part_copy().start()
        part_copy().wait()
        for k in range(chips):
            joined[k] = pre[k, b] + part[k]
    else:
        for k in range(chips):
            joined[k] = pre[k, b]
    for k in range(1, chips):
        @pl.when(gets_over(k))
        def _():
            over_copy(k).start()

    block_copy(cross - 1, nc - 1).start()

    th_local.wait()
    sun_local.wait()
    settle(hext.at[:, pl.ds(0, 2 * EDGE)], s_recv.at[0])
    lane = lane_index((full, width))
    coriolis = coriolis_base + beta_plane * lane.astype(jnp.float32) / width

    def momentum(i, carry):
        lev = r * per + i
        u, v, heat_ext = fext[0, lev], fext[1, lev], hext[i]
        wet = jnp.where(lev < dext[...], 1.0, 0.0)
        v_east, u_west = east(v), west(u)
        v_bar = 0.25 * (v + v_east + south(v) + south(v_east))
        u_bar = 0.25 * (u + u_west + north(u) + north(u_west))
        new_u = u + step_duration * (
            coriolis * v_bar - gravity * (east(heat_ext) - heat_ext) + viscosity * laplacian(u)
        )
        new_v = v + step_duration * (
            -coriolis * u_bar - gravity * (north(heat_ext) - heat_ext) + viscosity * laplacian(v)
        )
        vel[0, i] = (wet * east(wet) * new_u)[PAD:PAD + rows]
        vel[1, i] = (wet * north(wet) * new_v)[PAD:PAD + rows]
        warmer = heat_ext + step_duration * spreading_coefficient * laplacian(heat_ext)
        heat[i] = warmer[PAD:PAD + rows]
        return carry

    lax.fori_loop(0, per, momentum, 0)

    tables[0].wait()
    tables[2].wait()

    def invert(s, carry):
        who = jnp.int32(0)
        for t in range(count):
            who = jnp.where(eaten[t] == s, jnp.int32(t), who)
        eater[s] = who
        return carry

    lax.fori_loop(0, count, invert, 0)

    depth = dext[PAD:PAD + rows].astype(jnp.float32)
    aux[2] = depth
    scale = column_optical / nl
    clear = (r * per).astype(jnp.float32) * water_clear

    @pl.when(r == 0)
    def _():
        aux[0] = jnp.zeros((rows, width), jnp.float32)

    @pl.when(r > 0)
    def _():
        above = joined[a]
        for k in range(1, chips):
            over_copy(k).wait_recv()
            above = above + over[k - 1]
        aux[0] = (above + clear) * scale

    def react_chunk(c, carry):
        @pl.when(c == 0)
        def _():
            wait_first()

        @pl.when(c > 0)
        def _():
            wait_blocks(c)

        def one_level(j, carry):
            i = c * q + j

            def put(t, x):
                cells[t, i] = x

            level = (r * per + i).astype(jnp.float32)
            wet, caught, below = react_level(
                count, level, aux[2], aux[1], aux[0], cells, i,
                eaten, eater, att, rate, scale, sat, pull, put,
            )
            aux[0] = below
            heat[i] = wet * (heat[i] + warming_coefficient * (caught * wet))
            return carry

        lax.fori_loop(0, q, one_level, 0)
        return carry

    lax.fori_loop(0, nc - 1, react_chunk, 0)

    settle(fc.at[:, :, pl.ds(0, LOW_FLOW + HIGH_FLOW)], edge_send.at[0])
    settle(sp.at[:, :, pl.ds(0, 2 * EDGE)], edge_send.at[1])
    settle(th.at[:, pl.ds(0, 2 * EDGE)], edge_send.at[2])
    settle(dep.at[pl.ds(0, 2 * EDGE)], edge_send.at[3])
    for k in range(1, chips):
        @pl.when(gets_over(k))
        def _():
            over_copy(k).wait_send()

    settle(adv.at[:, pl.ds(0, (ranks - 1) * per - early * q)], d_send.at[0])
    settle(ext.at[:, pl.ds(0, early * q), pl.ds(0, 2 * EDGE)], d_send.at[2])
    for pieces, mask in ((early * q, late), (early * q - 1, jnp.logical_not(late))):
        @pl.when(mask)
        def _():
            settle(ext.at[:, pl.ds(0, pieces), inner], d_send.at[1])

    @pl.when(jnp.logical_not(late))
    def _():
        raw_copy().wait_send()

    wait_blocks(nc - 1)


def finish_kernel(
    levels, q,
    cells, vel, heat, aux, eaten_in, att_in, rate_in,
    out, vel_out, temp_out,
    eaten, att, rate, last, warm, sat, pull, eater, sem, t_sem,
):
    count, per = cells.shape[:2]
    r = lax.axis_index("tracer")
    done = per - q
    scale = column_optical / levels
    copies = [
        pltpu.make_async_copy(cells.at[:, pl.ds(0, done)], out.at[:, pl.ds(0, done)], sem.at[0]),
        pltpu.make_async_copy(vel, vel_out, sem.at[1]),
        pltpu.make_async_copy(heat.at[pl.ds(0, done)], temp_out.at[pl.ds(0, done)], sem.at[2]),
    ]
    tables = [
        pltpu.make_async_copy(src, dst, t_sem.at[k])
        for k, (src, dst) in enumerate(((eaten_in, eaten), (att_in, att), (rate_in, rate)))
    ]
    for copy in tables + copies:
        copy.start()
    for copy in tables:
        copy.wait()
    for t in range(count):
        eater[eaten[t]] = t

    def level_copy(j):
        return pltpu.make_async_copy(last.at[j], out.at[:, done + j], sem.at[4])

    def one_level(j, tau):
        def put(t, x):
            last[j, t] = x

        level = (r * per + done + j).astype(jnp.float32)
        wet, caught, below = react_level(
            count, level, aux[2], aux[1], tau, cells, done + j,
            eaten, eater, att, rate, scale, sat, pull, put,
        )
        warm[j] = wet * (heat[done + j] + warming_coefficient * (caught * wet))
        level_copy(j).start()
        return below

    lax.fori_loop(0, q, one_level, aux[0])
    warm_copy = pltpu.make_async_copy(warm, temp_out.at[pl.ds(done, q)], sem.at[3])
    warm_copy.start()
    for copy in copies:
        copy.wait()
    pltpu.make_async_copy(last, last, sem.at[4]).wait()
    warm_copy.wait()


def solution(mesh):
    tiles, ranks = mesh.shape["tile"], mesh.shape["tracer"]
    cores = 2 if ranks % 2 == 0 else 1

    def on_device(
        species_amounts,
        face_currents,
        thermal_anomaly,
        layer_total_per_profile,
        consumed_species,
        attenuation_factor,
        intake_speedup,
        incoming_sunshine,
    ):
        nt, nl, rows, width = species_amounts.shape
        per = nl // ranks
        q = 2 if per % 2 == 0 else 1
        nc = per // q
        count = ranks * nt
        cross = ranks - cores
        chips = ranks // cores
        deep = min(DEEP, nc - 1)
        full = rows + PAD
        f32 = jnp.float32
        any_space = pl.BlockSpec(memory_space=pl.ANY)
        vmem = pl.BlockSpec(memory_space=pltpu.VMEM)
        dma = pltpu.SemaphoreType.DMA
        cells, vel, heat, aux = pl.pallas_call(
            functools.partial(transport_kernel, tiles, ranks, cores, q, deep),
            out_shape=(
                pltpu.VMEM((count, per, rows, width), f32),
                pltpu.VMEM((2, per, rows, width), f32),
                pltpu.VMEM((per, rows, width), f32),
                pltpu.VMEM((3, rows, width), f32),
            ),
            in_specs=[any_space] * 8,
            out_specs=(vmem, vmem, vmem, vmem),
            scratch_shapes=[
                pltpu.SMEM((count,), jnp.int32),
                pltpu.SMEM((count,), f32),
                pltpu.SMEM((count,), f32),
                pltpu.VMEM((nt, nl, full, width), f32),
                pltpu.VMEM((2, nl, full, width), f32),
                pltpu.VMEM((per, full, width), f32),
                pltpu.VMEM((full, width), jnp.int32),
                pltpu.VMEM((nt, nl, rows, width), f32),
                pltpu.VMEM((ranks, rows, width), f32),
                pltpu.VMEM((chips, cores, rows, width), f32),
                pltpu.VMEM((chips, rows, width), f32),
                pltpu.VMEM((chips, rows, width), f32),
                pltpu.VMEM((chips, rows, width), f32),
                pltpu.VMEM((count, rows, width), f32),
                pltpu.VMEM((count, rows, width), f32),
                pltpu.SMEM((count,), jnp.int32),
                pltpu.VMEM((nt, rows, width), f32),
                dma((4,)), dma((nc + cores * nc,)), dma((nc + cores * nc,)), dma((2,)),
                dma((3,)), dma((nc + 1,)), dma((chips,)), dma((chips,)),
                dma((deep + cross,)), dma((2,)), dma((3,)), dma((3,)),
                dma((1,)), dma((1,)), pltpu.SemaphoreType.REGULAR,
            ],
            compiler_params=pltpu.CompilerParams(
                collective_id=0, has_side_effects=True, vmem_limit_bytes=48 << 20
            ),
            name="transport",
        )(
            *(pltpu.with_memory_space_constraint(x, HBM) for x in (
                species_amounts, face_currents, thermal_anomaly,
                layer_total_per_profile, incoming_sunshine,
                consumed_species, attenuation_factor, intake_speedup,
            ))
        )
        return pl.pallas_call(
            functools.partial(finish_kernel, nl, q),
            out_shape=(
                jax.ShapeDtypeStruct((count, per, rows, width), f32),
                jax.ShapeDtypeStruct((2, per, rows, width), f32),
                jax.ShapeDtypeStruct((per, rows, width), f32),
            ),
            in_specs=[vmem] * 4 + [any_space] * 3,
            out_specs=(any_space, any_space, any_space),
            scratch_shapes=[
                pltpu.SMEM((count,), jnp.int32),
                pltpu.SMEM((count,), f32),
                pltpu.SMEM((count,), f32),
                pltpu.VMEM((q, count, rows, width), f32),
                pltpu.VMEM((q, rows, width), f32),
                pltpu.VMEM((count, rows, width), f32),
                pltpu.VMEM((count, rows, width), f32),
                pltpu.SMEM((count,), jnp.int32),
                dma((5,)), dma((3,)),
            ],
            compiler_params=pltpu.CompilerParams(vmem_limit_bytes=32 << 20),
            name="finish",
        )(
            cells, vel, heat, aux,
            consumed_species, attenuation_factor, intake_speedup,
        )

    return jax.shard_map(
        on_device,
        mesh=mesh,
        in_specs=(
            P(("groups", "tracer"), None, "tile", None),
            P(None, "groups", "tile", None),
            P(("groups", "tracer"), "tile", None),
            P(("groups", "tile"), None),
            P(),
            P(),
            P(),
            P(("groups", "tile"), None),
        ),
        out_specs=(
            P("groups", "tracer", "tile", None),
            P(None, ("groups", "tracer"), "tile", None),
            P(("groups", "tracer"), "tile", None),
        ),
        check_vma=False,
    )
```

```python
import functools

import jax
import jax.numpy as jnp
from jax import lax
from jax.experimental import pallas as pl
from jax.experimental.pallas import tpu as pltpu
from jax.sharding import PartitionSpec as P

MESH = pl.DeviceIdType.MESH

sub_step = 0.45
step_duration = 0.2
gravity = 0.5
viscosity = 0.2
coriolis_base = 0.5
beta_plane = 0.5
spreading_coefficient = 0.2
water_clear = 0.05
column_optical = 3.0
warming_coefficient = 5.0
light_half = 0.3
nutrient_half = 0.5

PAD = 8
EDGE = 4
TILE = 8
LOW_FLOW, HIGH_FLOW = 3, 2
DEEP = 2

HBM = pltpu.HBM


def lane_index(shape):
    return lax.broadcasted_iota(jnp.int32, shape, len(shape) - 1)


def east(x):
    return pltpu.roll(x, x.shape[0] - 1, 0)


def west(x):
    return pltpu.roll(x, 1, 0)


def north(x):
    return jnp.where(lane_index(x.shape) == x.shape[1] - 1, 0.0, pltpu.roll(x, x.shape[1] - 1, 1))


def south(x):
    return jnp.where(lane_index(x.shape) == 0, 0.0, pltpu.roll(x, 1, 1))


def minmod(a, b):
    return jnp.maximum(jnp.minimum(a, b), jnp.minimum(jnp.maximum(a, b), 0.0))


def laplacian(x):
    return east(x) + west(x) + north(x) + south(x) - 4.0 * x


def substep(c, es, ns, lane):
    last = c.shape[1] - 1
    e = 0.5 * c
    d = east(e) - e
    half = minmod(west(d), d)
    flux = es * jnp.where(es > 0.0, c + half, east(c - half))
    spread = flux - west(flux)
    d = jnp.where(lane == last, 0.0, pltpu.roll(e, last, 1)) - e
    half = minmod(jnp.where(lane == 0, e, pltpu.roll(d, 1, 1)), d)
    flux = ns * jnp.where(ns > 0.0, c + half, pltpu.roll(c - half, last, 1))
    return c - (spread + (flux - pltpu.roll(flux, 1, 1)))


def react_level(count, level, depth, sun, tau, cells, c, eaten, eater, att, rate, scale, sat, pull, put):
    total = jnp.full(depth.shape, water_clear, jnp.float32)
    for t in range(count):
        x = cells[t, c]
        size = jnp.abs(x)
        total = total + att[t] * size
        sat[t] = x / (nutrient_half + size)
        pull[t] = rate[t] * x
    optical = total * scale
    wet = jnp.where(level < depth, 1.0, 0.0)
    caught = sun * jnp.exp(-tau) * (1.0 - jnp.exp(-optical))
    mean_light = caught / optical
    gain = wet * (mean_light / (mean_light + light_half))
    for t in range(count):
        change = pull[t] * sat[eaten[t]] - pull[eater[t]] * sat[t]
        put(t, cells[t, c] + gain * change)
    return wet, caught, tau + optical


def transport_kernel(
    tiles, ranks, cores, q, deep,
    sp, fc, th, dep, sun, eaten_in, att_in, rate_in,
    cells, vel, heat, aux,
    eaten, att, rate, ext, fext, hext, dext, adv, tot, pre, part, joined, over, sat, pull, eater, raw,
    edge_send, g_recv, s_recv, d_send, d_recv, o_send, o_recv,
    l_sem, lf_sem, ls_sem, t_sem, r_send, r_recv, ready,
):
    nt, nl, rows, width = sp.shape
    per = nl // ranks
    nc = per // q
    count = ranks * nt
    chips = ranks // cores
    cross = ranks - cores
    full = rows + PAD
    early = deep + cross - 1
    r = lax.axis_index("tracer")
    z = lax.axis_index("tile")
    a, b = r // cores, lax.rem(r, cores)
    up, down = lax.rem(z + 1, tiles), lax.rem(z + tiles - 1, tiles)

    def target(s):
        k = lax.rem(s, cores)
        chip = lax.rem(a + 1 + s // cores, chips)
        core = jnp.where(s < cross, k, lax.rem(b + cores - 1 - k, cores))
        return chip * cores + core

    def first_level(s, c):
        return target(s) * per + c * q

    mine = pl.ds(r * nt, nt)
    body = pl.ds(PAD, rows)
    inner = pl.ds(EDGE, rows - 2 * EDGE)

    def settle(ref, sem):
        pltpu.make_async_copy(ref, ref, sem).wait()

    def pair(src, dst, lead, send, recv, low=EDGE, high=EDGE):
        return (
            pltpu.make_async_remote_copy(
                src.at[lead + (pl.ds(rows - low, low),)],
                dst.at[lead + (pl.ds(PAD - low, low),)],
                send, recv, device_id={"tile": up}, device_id_type=MESH,
            ),
            pltpu.make_async_remote_copy(
                src.at[lead + (pl.ds(0, high),)],
                dst.at[lead + (pl.ds(0, high),)],
                send, recv, device_id={"tile": down}, device_id_type=MESH,
            ),
        )

    def edges(s, c):
        g = jnp.where(s < cross, c, jnp.where(s < ranks - 1, nc + s - cross, own_group + c))
        lead = (slice(None), pl.ds(first_level(s, c), q))
        return (
            pair(fc, fext, lead, edge_send.at[0], g_recv.at[g], LOW_FLOW, HIGH_FLOW)
            + pair(sp, ext, lead, edge_send.at[0], g_recv.at[g])
        )

    own_group = nc + cores - 1

    def edge_rows(levels):
        return fext.at[:, pl.ds(0, levels), pl.ds(0, nt * EDGE + LOW_FLOW + HIGH_FLOW)]

    def wait_edges(g, levels):
        settle(edge_rows(levels), g_recv.at[g])

    def heat_edges():
        return pair(th, hext, (slice(None),), edge_send.at[1], s_recv.at[0])

    def depth_edges():
        return pair(dep, dext, (), edge_send.at[2], s_recv.at[1])

    def flow_local(s):
        lev = pl.ds(target(s) * per, per)
        sem = lf_sem.at[0] if s == 0 else lf_sem.at[1]
        return pltpu.make_async_copy(fc.at[:, lev], fext.at[:, lev, body], sem)

    def early_chunk(k):
        return jnp.where(k < deep, 0, k - deep + 1), jnp.where(k < deep, k, 0)

    def edge_chunk(k):
        return jnp.where(k < cross, k, 0), jnp.where(k < cross, 0, k - cross + 1)

    def early_local(k):
        lev = pl.ds(first_level(*early_chunk(k)), q)
        return pltpu.make_async_copy(sp.at[:, lev], ext.at[:, lev, body], l_sem.at[k])

    def rest_local(s):
        skip = deep if s == 0 else 1 if s < cross else 0
        lev = pl.ds(first_level(s, skip), per - skip * q)
        return pltpu.make_async_copy(sp.at[:, lev], ext.at[:, lev, body], l_sem.at[early])

    def block_copy(s, c):
        return pltpu.make_async_remote_copy(
            adv.at[:, pl.ds(first_level(s, c), q)],
            cells.at[mine, pl.ds(c * q, q)],
            d_send.at[0], d_recv.at[c],
            device_id={"tracer": target(s)}, device_id_type=MESH,
        )

    def inner_copy(s, c, i):
        return pltpu.make_async_remote_copy(
            adv.at[:, first_level(s, c) + i, inner],
            cells.at[mine, c * q + i, inner],
            d_send.at[1], d_recv.at[jnp.where(c == 0, nc, c)],
            device_id={"tracer": target(s)}, device_id_type=MESH,
        )

    def outer_copy(s, c, side, skip=0):
        edge = pl.ds(side * (rows - EDGE), EDGE)
        return pltpu.make_async_remote_copy(
            adv.at[:, pl.ds(first_level(s, c) + skip, q - skip), edge],
            cells.at[mine, pl.ds(c * q + skip, q - skip), edge],
            d_send.at[2], d_recv.at[c],
            device_id={"tracer": target(s)}, device_id_type=MESH,
        )

    def raw_copy():
        return pltpu.make_async_remote_copy(
            sp.at[:, first_level(0, 0)], raw.at[:, body], r_send.at[0], r_recv.at[0],
            device_id={"tracer": target(0)}, device_id_type=MESH,
        )

    def raw_edges():
        return pair(raw.at[:, body], raw, (slice(None),), r_send.at[1], r_recv.at[1])

    def wait_first():
        for pieces, mask in ((cross * q, late), (cross * q - 1, jnp.logical_not(late))):
            @pl.when(mask)
            def _():
                strips = pl.ds(0, pieces + q * (rows // TILE))
                settle(ext.at[:, strips, pl.ds(0, TILE)], d_recv.at[0])
                settle(ext.at[:, pl.ds(0, pieces), inner], d_recv.at[nc])

    def wait_blocks(c):
        settle(cells.at[pl.ds(0, (ranks - 1) * nt), pl.ds(c * q, q)], d_recv.at[c])

    partner = a * cores + cores - 1 - b

    def part_copy():
        return pltpu.make_async_remote_copy(
            pre.at[:, cores - 1 - b], part, o_send.at[0], o_recv.at[0],
            device_id={"tracer": partner}, device_id_type=MESH,
        )

    def over_copy(k):
        there = lax.rem(a + k, chips)
        return pltpu.make_async_remote_copy(
            joined.at[there], over.at[k - 1], o_send.at[k], o_recv.at[k],
            device_id={"tracer": there * cores + b}, device_id_type=MESH,
        )

    def gets_over(k):
        return lax.rem(a + k, chips) * cores + b > 0

    def in_cross(m):
        return lax.rem(m, cross), m // cross

    def in_near(m):
        return cross + m // nc, lax.rem(m, nc)

    last_core = a * cores + cores - 1
    late = b == cores - 1
    barrier = pltpu.get_barrier_semaphore()
    if cores > 1:
        @pl.when(jnp.logical_not(late))
        def _():
            for s in range(0, cross, cores):
                pl.semaphore_signal(
                    barrier, inc=1, device_id={"tracer": target(s)}, device_id_type=MESH
                )
            pl.semaphore_signal(barrier, inc=1, device_id={"tracer": last_core}, device_id_type=MESH)
    for place in (up, down):
        pl.semaphore_signal(
            barrier, inc=1, device_id={"tile": place, "tracer": last_core}, device_id_type=MESH
        )
    for s in range(cores - 1, cross, cores):
        pl.semaphore_signal(barrier, inc=1, device_id={"tracer": target(s)}, device_id_type=MESH)

    dep_local = pltpu.make_async_copy(dep, dext.at[body], ls_sem.at[0])
    th_local = pltpu.make_async_copy(th, hext.at[:, body], ls_sem.at[1])
    sun_local = pltpu.make_async_copy(sun, aux.at[1], ls_sem.at[2])
    tables = [
        pltpu.make_async_copy(src, dst, t_sem.at[k])
        for k, (src, dst) in enumerate(((eaten_in, eaten), (att_in, att), (rate_in, rate)))
    ]
    dep_local.start()
    tables[1].start()

    flow_local(0).start()

    def start_early(k, carry):
        early_local(k).start()
        return carry

    early_local(0).start()
    @pl.when(jnp.logical_not(late))
    def _():
        pl.semaphore_wait(barrier, chips - 1)
        raw_copy().start()

    lax.fori_loop(1, early, start_early, 0)
    for s in range(1, ranks):
        flow_local(s).start()

    tot[...] = jnp.zeros_like(tot)
    dep_local.wait()
    tables[1].wait()

    def advect(lev, block, base, size, skip, first, keep, put, take=None, owner=r):
        window = pl.ds(base, size)
        kept = pl.ds(first, keep)
        lane = lane_index((size, width))
        wet = jnp.where(lev < dext[window], 1.0, 0.0)
        es = sub_step * (fext[0, lev, window] * wet * east(wet))
        ns = sub_step * (fext[1, lev, window] * wet * north(wet))

        def one_tracer(t, acc):
            c = substep(take(t) if take else ext[t, lev, window], es, ns, lane)
            c = substep(c, es, ns, lane)[skip:skip + keep]
            put(t, lev, kept, c)
            return acc + att[owner * nt + t] * jnp.abs(c)

        tot[block, kept] = lax.fori_loop(0, nt, one_tracer, tot[block, kept], unroll=True)

    def strip(ref, *lead):
        return jnp.concatenate(
            [ref[lead + (pl.ds(full - TILE, TILE),)], ref[lead + (pl.ds(0, PAD + TILE),)]], axis=0
        )

    def put_adv(t, lev, kept, c):
        adv[t, lev, kept] = c

    def put_cells(t, lev, kept, c):
        cells[r * nt + t, lev - r * per, kept] = c

    def advance_inner(s, c, i):
        lev = first_level(s, c) + i
        advect(lev, target(s), PAD, rows, EDGE, EDGE, rows - 2 * EDGE, put_adv)

    def advance_outer(s, c, i):
        lev = first_level(s, c) + i
        block = target(s)
        size = TILE + PAD + TILE
        lane = lane_index((size, width))
        wet = jnp.where(lev < strip(dext), 1.0, 0.0)
        es = sub_step * (strip(fext, 0, lev) * wet * east(wet))
        ns = sub_step * (strip(fext, 1, lev) * wet * north(wet))
        high, low = slice(TILE - EDGE, TILE), slice(TILE + PAD, TILE + PAD + EDGE)
        high_rows, low_rows = pl.ds(rows - EDGE, EDGE), pl.ds(0, EDGE)

        def one_tracer(t, acc):
            c = substep(strip(ext, t, lev), es, ns, lane)
            c = substep(c, es, ns, lane)
            adv[t, lev, high_rows] = c[high]
            adv[t, lev, low_rows] = c[low]
            return acc + att[r * nt + t] * jnp.abs(c)

        acc = lax.fori_loop(0, nt, one_tracer, jnp.zeros((size, width), jnp.float32), unroll=True)
        tot[block, high_rows] += acc[high]
        tot[block, low_rows] += acc[low]

    def advance(s, c, put):
        block = target(s)
        level_0 = first_level(s, c)

        def one_level(i, carry):
            advect(level_0 + i, block, 0, full, PAD, 0, rows, put)
            return carry

        lax.fori_loop(0, q, one_level, 0)

    def start_edges(order):
        def step(m, carry):
            for copy in edges(*order(m)):
                copy.start()
            return carry
        return step

    turn = jnp.where(late, 0, deep * q - 1)

    def inner_step(m, carry):
        k, i = m // q, lax.rem(m, q)
        s, c = early_chunk(k)

        @pl.when(m == 0)
        def _():
            flow_local(0).wait()

        @pl.when(m == deep * q)
        def _():
            settle(fext.at[:, pl.ds(0, (ranks - 1) * per), body], lf_sem.at[1])

        @pl.when(i == 0)
        def _():
            early_local(k).wait()

        @pl.when(jnp.logical_or(late, m > 0))
        def _():
            advance_inner(s, c, i)

            @pl.when(m == 0)
            def _():
                pl.semaphore_wait(barrier, cross + cores - 1 + 2 * cores)

            inner_copy(s, c, i).start()

        @pl.when(m == turn)
        def _():
            if cores > 1:
                @pl.when(late)
                def _():
                    pl.semaphore_signal(
                        ready, inc=1, device_id={"tracer": partner}, device_id_type=MESH
                    )

                @pl.when(jnp.logical_not(late))
                def _():
                    pl.semaphore_wait(ready, 1)

            for copy in depth_edges():
                copy.start()
            lax.fori_loop(0, cross, start_edges(in_cross), 0)

        return carry

    lax.fori_loop(0, early * q, inner_step, 0)
    lax.fori_loop(cross, cross * nc, start_edges(in_cross), 0)
    for s in range(ranks):
        rest_local(s).start()

    @pl.when(jnp.logical_not(late))
    def _():
        raw_copy().wait_recv()
        for copy in raw_edges():
            copy.start()

    lax.fori_loop(0, cores * nc, start_edges(in_near), 0)
    for copy in heat_edges():
        copy.start()
    th_local.start()
    sun_local.start()
    tables[0].start()
    tables[2].start()
    tables[0].wait()
    tables[2].wait()

    def invert(s, carry):
        who = jnp.int32(0)
        for t in range(count):
            who = jnp.where(eaten[t] == s, jnp.int32(t), who)
        eater[s] = who
        return carry

    lax.fori_loop(0, count, invert, 0)

    settle(dext.at[pl.ds(0, 2 * EDGE)], s_recv.at[1])

    def outer_step(k, carry):
        s, c = edge_chunk(k)

        @pl.when(s == 0)
        def _():
            wait_edges(c, cross * q)

        def sides(i, carry):
            advance_outer(s, c, i)
            return carry

        given = jnp.logical_and(jnp.logical_not(late), k == 0)
        lax.fori_loop(jnp.where(given, 1, 0), q, sides, 0)

        @pl.when(jnp.logical_not(given))
        def _():
            for side in range(2):
                outer_copy(s, c, side).start()

        if q > 1:
            @pl.when(given)
            def _():
                for side in range(2):
                    outer_copy(s, c, side, 1).start()

        return carry

    lax.fori_loop(0, early, outer_step, 0)

    settle(ext.at[:, pl.ds(0, nl - early * q), body], l_sem.at[early])

    def away_step(m, carry):
        far = m < cross * nc
        k = m - cross * nc
        s = jnp.where(far, lax.rem(m, cross), cross + k // nc)
        c = jnp.where(far, m // cross, lax.rem(k, nc))

        @pl.when(jnp.logical_and(far, jnp.logical_and(s == 0, c >= deep)))
        def _():
            wait_edges(c, cross * q)

        @pl.when(jnp.logical_and(jnp.logical_not(far), c == 0))
        def _():
            wait_edges(nc + s - cross, per)

        @pl.when(jnp.logical_or(s > 0, c >= deep))
        def _():
            advance(s, c, put_adv)

            @pl.when(m != cross * nc - 1)
            def _():
                block_copy(s, c).start()

        return carry

    lax.fori_loop(cross, (ranks - 1) * nc, away_step, 0)

    wait_edges(own_group, q)

    @pl.when(jnp.logical_not(late))
    def _():
        giver = lax.rem(a + chips - 1, chips) * cores

        def put_given(t, lev, kept, c):
            cells[giver * nt + t, 0, kept] = c

        settle(raw.at[:, pl.ds(0, 2 * EDGE)], r_recv.at[1])
        advect(r * per, r, 0, full, PAD, 0, rows, put_given, lambda t: raw[t], giver)

    def own_step(c, carry):
        @pl.when(c > 0)
        def _():
            wait_edges(own_group + c, q)

        advance(ranks - 1, c, put_cells)
        return carry

    lax.fori_loop(0, nc, own_step, 0)

    above = jnp.zeros((rows, width), jnp.float32)
    for place in range(ranks):
        pre[place // cores, place % cores] = above
        above = above + tot[place]
    if cores > 1:
        part_copy().start()
        part_copy().wait()
        for k in range(chips):
            joined[k] = pre[k, b] + part[k]
    else:
        for k in range(chips):
            joined[k] = pre[k, b]
    for k in range(1, chips):
        @pl.when(gets_over(k))
        def _():
            over_copy(k).start()

    block_copy(cross - 1, nc - 1).start()

    th_local.wait()
    sun_local.wait()
    settle(hext.at[:, pl.ds(0, 2 * EDGE)], s_recv.at[0])
    lane = lane_index((full, width))
    coriolis = coriolis_base + beta_plane * lane.astype(jnp.float32) / width

    def momentum(i, carry):
        lev = r * per + i
        u, v, heat_ext = fext[0, lev], fext[1, lev], hext[i]
        wet = jnp.where(lev < dext[...], 1.0, 0.0)
        v_east, u_west = east(v), west(u)
        v_bar = 0.25 * (v + v_east + south(v) + south(v_east))
        u_bar = 0.25 * (u + u_west + north(u) + north(u_west))
        new_u = u + step_duration * (
            coriolis * v_bar - gravity * (east(heat_ext) - heat_ext) + viscosity * laplacian(u)
        )
        new_v = v + step_duration * (
            -coriolis * u_bar - gravity * (north(heat_ext) - heat_ext) + viscosity * laplacian(v)
        )
        vel[0, i] = (wet * east(wet) * new_u)[PAD:PAD + rows]
        vel[1, i] = (wet * north(wet) * new_v)[PAD:PAD + rows]
        warmer = heat_ext + step_duration * spreading_coefficient * laplacian(heat_ext)
        heat[i] = warmer[PAD:PAD + rows]
        return carry

    lax.fori_loop(0, per, momentum, 0)

    depth = dext[PAD:PAD + rows].astype(jnp.float32)
    aux[2] = depth
    scale = column_optical / nl
    clear = (r * per).astype(jnp.float32) * water_clear

    @pl.when(r == 0)
    def _():
        aux[0] = jnp.zeros((rows, width), jnp.float32)

    @pl.when(r > 0)
    def _():
        above = joined[a]
        for k in range(1, chips):
            over_copy(k).wait_recv()
            above = above + over[k - 1]
        aux[0] = (above + clear) * scale

    def react_chunk(c, carry):
        @pl.when(c == 0)
        def _():
            wait_first()

        @pl.when(c > 0)
        def _():
            wait_blocks(c)

        def one_level(j, carry):
            i = c * q + j

            def put(t, x):
                cells[t, i] = x

            level = (r * per + i).astype(jnp.float32)
            wet, caught, below = react_level(
                count, level, aux[2], aux[1], aux[0], cells, i,
                eaten, eater, att, rate, scale, sat, pull, put,
            )
            aux[0] = below
            heat[i] = wet * (heat[i] + warming_coefficient * (caught * wet))
            return carry

        lax.fori_loop(0, q, one_level, 0)
        return carry

    lax.fori_loop(0, nc - 1, react_chunk, 0)

    settle(edge_rows(nl), edge_send.at[0])
    settle(th.at[:, pl.ds(0, 2 * EDGE)], edge_send.at[1])
    settle(dep.at[pl.ds(0, 2 * EDGE)], edge_send.at[2])
    for k in range(1, chips):
        @pl.when(gets_over(k))
        def _():
            over_copy(k).wait_send()

    settle(adv.at[:, pl.ds(0, (ranks - 1) * per - early * q)], d_send.at[0])
    for pieces, mask in ((early * q, late), (early * q - 1, jnp.logical_not(late))):
        @pl.when(mask)
        def _():
            settle(ext.at[:, pl.ds(0, pieces), pl.ds(0, 2 * EDGE)], d_send.at[2])
            settle(ext.at[:, pl.ds(0, pieces), inner], d_send.at[1])

    @pl.when(jnp.logical_not(late))
    def _():
        raw_copy().wait_send()
        settle(raw.at[:, pl.ds(0, 2 * EDGE)], r_send.at[1])

    wait_blocks(nc - 1)


def finish_kernel(
    levels, q,
    cells, vel, heat, aux, eaten_in, att_in, rate_in,
    out, vel_out, temp_out,
    eaten, att, rate, last, warm, sat, pull, eater, sem, t_sem,
):
    count, per = cells.shape[:2]
    r = lax.axis_index("tracer")
    done = per - q
    scale = column_optical / levels
    copies = [
        pltpu.make_async_copy(cells.at[:, pl.ds(0, done)], out.at[:, pl.ds(0, done)], sem.at[0]),
        pltpu.make_async_copy(vel, vel_out, sem.at[1]),
        pltpu.make_async_copy(heat.at[pl.ds(0, done)], temp_out.at[pl.ds(0, done)], sem.at[2]),
    ]
    tables = [
        pltpu.make_async_copy(src, dst, t_sem.at[k])
        for k, (src, dst) in enumerate(((eaten_in, eaten), (att_in, att), (rate_in, rate)))
    ]
    for copy in tables + copies:
        copy.start()
    for copy in tables:
        copy.wait()
    for t in range(count):
        eater[eaten[t]] = t

    def level_copy(j):
        return pltpu.make_async_copy(last.at[j], out.at[:, done + j], sem.at[4])

    def one_level(j, tau):
        def put(t, x):
            last[j, t] = x

        level = (r * per + done + j).astype(jnp.float32)
        wet, caught, below = react_level(
            count, level, aux[2], aux[1], tau, cells, done + j,
            eaten, eater, att, rate, scale, sat, pull, put,
        )
        warm[j] = wet * (heat[done + j] + warming_coefficient * (caught * wet))
        level_copy(j).start()
        return below

    lax.fori_loop(0, q, one_level, aux[0])
    warm_copy = pltpu.make_async_copy(warm, temp_out.at[pl.ds(done, q)], sem.at[3])
    warm_copy.start()
    for copy in copies:
        copy.wait()
    pltpu.make_async_copy(last, last, sem.at[4]).wait()
    warm_copy.wait()


def solution(mesh):
    tiles, ranks = mesh.shape["tile"], mesh.shape["tracer"]
    cores = 2 if ranks % 2 == 0 else 1

    def on_device(
        species_amounts,
        face_currents,
        thermal_anomaly,
        layer_total_per_profile,
        consumed_species,
        attenuation_factor,
        intake_speedup,
        incoming_sunshine,
    ):
        nt, nl, rows, width = species_amounts.shape
        per = nl // ranks
        q = 2 if per % 2 == 0 else 1
        nc = per // q
        count = ranks * nt
        cross = ranks - cores
        chips = ranks // cores
        deep = min(DEEP, nc - 1)
        full = rows + PAD
        f32 = jnp.float32
        any_space = pl.BlockSpec(memory_space=pl.ANY)
        vmem = pl.BlockSpec(memory_space=pltpu.VMEM)
        dma = pltpu.SemaphoreType.DMA
        cells, vel, heat, aux = pl.pallas_call(
            functools.partial(transport_kernel, tiles, ranks, cores, q, deep),
            out_shape=(
                pltpu.VMEM((count, per, rows, width), f32),
                pltpu.VMEM((2, per, rows, width), f32),
                pltpu.VMEM((per, rows, width), f32),
                pltpu.VMEM((3, rows, width), f32),
            ),
            in_specs=[any_space] * 8,
            out_specs=(vmem, vmem, vmem, vmem),
            scratch_shapes=[
                pltpu.SMEM((count,), jnp.int32),
                pltpu.SMEM((count,), f32),
                pltpu.SMEM((count,), f32),
                pltpu.VMEM((nt, nl, full, width), f32),
                pltpu.VMEM((2, nl, full, width), f32),
                pltpu.VMEM((per, full, width), f32),
                pltpu.VMEM((full, width), jnp.int32),
                pltpu.VMEM((nt, nl, rows, width), f32),
                pltpu.VMEM((ranks, rows, width), f32),
                pltpu.VMEM((chips, cores, rows, width), f32),
                pltpu.VMEM((chips, rows, width), f32),
                pltpu.VMEM((chips, rows, width), f32),
                pltpu.VMEM((chips, rows, width), f32),
                pltpu.VMEM((count, rows, width), f32),
                pltpu.VMEM((count, rows, width), f32),
                pltpu.SMEM((count,), jnp.int32),
                pltpu.VMEM((nt, full, width), f32),
                dma((3,)), dma((2 * nc + cores - 1,)), dma((2,)),
                dma((3,)), dma((nc + 1,)), dma((chips,)), dma((chips,)),
                dma((deep + cross,)), dma((2,)), dma((3,)), dma((3,)),
                dma((2,)), dma((2,)), pltpu.SemaphoreType.REGULAR,
            ],
            compiler_params=pltpu.CompilerParams(
                collective_id=0, has_side_effects=True, vmem_limit_bytes=48 << 20
            ),
            name="transport",
        )(
            *(pltpu.with_memory_space_constraint(x, HBM) for x in (
                species_amounts, face_currents, thermal_anomaly,
                layer_total_per_profile, incoming_sunshine,
                consumed_species, attenuation_factor, intake_speedup,
            ))
        )
        return pl.pallas_call(
            functools.partial(finish_kernel, nl, q),
            out_shape=(
                jax.ShapeDtypeStruct((count, per, rows, width), f32),
                jax.ShapeDtypeStruct((2, per, rows, width), f32),
                jax.ShapeDtypeStruct((per, rows, width), f32),
            ),
            in_specs=[vmem] * 4 + [any_space] * 3,
            out_specs=(any_space, any_space, any_space),
            scratch_shapes=[
                pltpu.SMEM((count,), jnp.int32),
                pltpu.SMEM((count,), f32),
                pltpu.SMEM((count,), f32),
                pltpu.VMEM((q, count, rows, width), f32),
                pltpu.VMEM((q, rows, width), f32),
                pltpu.VMEM((count, rows, width), f32),
                pltpu.VMEM((count, rows, width), f32),
                pltpu.SMEM((count,), jnp.int32),
                dma((5,)), dma((3,)),
            ],
            compiler_params=pltpu.CompilerParams(vmem_limit_bytes=32 << 20),
            name="finish",
        )(
            cells, vel, heat, aux,
            consumed_species, attenuation_factor, intake_speedup,
        )

    return jax.shard_map(
        on_device,
        mesh=mesh,
        in_specs=(
            P(("groups", "tracer"), None, "tile", None),
            P(None, "groups", "tile", None),
            P(("groups", "tracer"), "tile", None),
            P(("groups", "tile"), None),
            P(),
            P(),
            P(),
            P(("groups", "tile"), None),
        ),
        out_specs=(
            P("groups", "tracer", "tile", None),
            P(None, ("groups", "tracer"), "tile", None),
            P(("groups", "tracer"), "tile", None),
        ),
        check_vma=False,
    )
```

```python
import functools

import jax
import jax.numpy as jnp
from jax import lax
from jax.experimental import pallas as pl
from jax.experimental.pallas import tpu as pltpu
from jax.sharding import PartitionSpec as P

MESH = pl.DeviceIdType.MESH

sub_step = 0.45
step_duration = 0.2
gravity = 0.5
viscosity = 0.2
coriolis_base = 0.5
beta_plane = 0.5
spreading_coefficient = 0.2
water_clear = 0.05
column_optical = 3.0
warming_coefficient = 5.0
light_half = 0.3
nutrient_half = 0.5

PAD = 8
EDGE = 4
TILE = 8
LOW_FLOW, HIGH_FLOW = 3, 2
DEEP = 2

HBM = pltpu.HBM


def lane_index(shape):
    return lax.broadcasted_iota(jnp.int32, shape, len(shape) - 1)


def east(x):
    return pltpu.roll(x, x.shape[0] - 1, 0)


def west(x):
    return pltpu.roll(x, 1, 0)


def north(x):
    return jnp.where(lane_index(x.shape) == x.shape[1] - 1, 0.0, pltpu.roll(x, x.shape[1] - 1, 1))


def south(x):
    return jnp.where(lane_index(x.shape) == 0, 0.0, pltpu.roll(x, 1, 1))


def minmod(a, b):
    return jnp.maximum(jnp.minimum(a, b), jnp.minimum(jnp.maximum(a, b), 0.0))


def laplacian(x):
    return east(x) + west(x) + north(x) + south(x) - 4.0 * x


def substep(c, es, ns, lane):
    last = c.shape[1] - 1
    e = 0.5 * c
    d = east(e) - e
    half = minmod(west(d), d)
    flux = es * jnp.where(es > 0.0, c + half, east(c - half))
    spread = flux - west(flux)
    d = jnp.where(lane == last, 0.0, pltpu.roll(e, last, 1)) - e
    half = minmod(jnp.where(lane == 0, e, pltpu.roll(d, 1, 1)), d)
    flux = ns * jnp.where(ns > 0.0, c + half, pltpu.roll(c - half, last, 1))
    return c - (spread + (flux - pltpu.roll(flux, 1, 1)))


def react_level(count, level, depth, sun, tau, cells, c, eaten, eater, att, rate, scale, sat, pull, put):
    total = jnp.full(depth.shape, water_clear, jnp.float32)
    for t in range(count):
        x = cells[t, c]
        size = jnp.abs(x)
        total = total + att[t] * size
        sat[t] = x / (nutrient_half + size)
        pull[t] = rate[t] * x
    optical = total * scale
    wet = jnp.where(level < depth, 1.0, 0.0)
    caught = sun * jnp.exp(-tau) * (1.0 - jnp.exp(-optical))
    mean_light = caught / optical
    gain = wet * (mean_light / (mean_light + light_half))
    for t in range(count):
        change = pull[t] * sat[eaten[t]] - pull[eater[t]] * sat[t]
        put(t, cells[t, c] + gain * change)
    return wet, caught, tau + optical


def transport_kernel(
    tiles, ranks, cores, q, deep,
    sp, fc, th, dep, sun, eaten_in, att_in, rate_in,
    cells, vel, heat, aux,
    eaten, att, rate, ext, fext, hext, dext, adv, tot, pre, part, joined, over, sat, pull, eater, raw,
    edge_send, g_recv, s_recv, d_send, d_recv, o_send, o_recv,
    l_sem, lf_sem, ls_sem, t_sem, r_send, r_recv, ready,
):
    nt, nl, rows, width = sp.shape
    per = nl // ranks
    nc = per // q
    count = ranks * nt
    chips = ranks // cores
    cross = ranks - cores
    full = rows + PAD
    early = deep + cross - 1
    r = lax.axis_index("tracer")
    z = lax.axis_index("tile")
    a, b = r // cores, lax.rem(r, cores)
    up, down = lax.rem(z + 1, tiles), lax.rem(z + tiles - 1, tiles)

    def target(s):
        k = lax.rem(s, cores)
        chip = lax.rem(a + 1 + s // cores, chips)
        core = jnp.where(s < cross, k, lax.rem(b + cores - 1 - k, cores))
        return chip * cores + core

    def first_level(s, c):
        return target(s) * per + c * q

    mine = pl.ds(r * nt, nt)
    body = pl.ds(PAD, rows)
    inner = pl.ds(EDGE, rows - 2 * EDGE)

    def settle(ref, sem):
        pltpu.make_async_copy(ref, ref, sem).wait()

    def pair(src, dst, lead, send, recv, low=EDGE, high=EDGE):
        return (
            pltpu.make_async_remote_copy(
                src.at[lead + (pl.ds(rows - low, low),)],
                dst.at[lead + (pl.ds(PAD - low, low),)],
                send, recv, device_id={"tile": up}, device_id_type=MESH,
            ),
            pltpu.make_async_remote_copy(
                src.at[lead + (pl.ds(0, high),)],
                dst.at[lead + (pl.ds(0, high),)],
                send, recv, device_id={"tile": down}, device_id_type=MESH,
            ),
        )

    def edges(s, c):
        g = jnp.where(s < cross, c, jnp.where(s < ranks - 1, nc + s - cross, own_group + c))
        lead = (slice(None), pl.ds(first_level(s, c), q))
        return (
            pair(fc, fext, lead, edge_send.at[0], g_recv.at[g], LOW_FLOW, HIGH_FLOW)
            + pair(sp, ext, lead, edge_send.at[0], g_recv.at[g])
        )

    own_group = nc + cores - 1

    def edge_rows(levels):
        return fext.at[:, pl.ds(0, levels), pl.ds(0, nt * EDGE + LOW_FLOW + HIGH_FLOW)]

    def wait_edges(g, levels):
        settle(edge_rows(levels), g_recv.at[g])

    def heat_edges():
        return pair(th, hext, (slice(None),), edge_send.at[1], s_recv.at[0])

    def depth_edges():
        return pair(dep, dext, (), edge_send.at[2], s_recv.at[1])

    def flow_local(s):
        lev = pl.ds(target(s) * per, per)
        sem = lf_sem.at[0] if s == 0 else lf_sem.at[1]
        return pltpu.make_async_copy(fc.at[:, lev], fext.at[:, lev, body], sem)

    def early_chunk(k):
        return jnp.where(k < deep, 0, k - deep + 1), jnp.where(k < deep, k, 0)

    def edge_chunk(k):
        return jnp.where(k < cross, k, 0), jnp.where(k < cross, 0, k - cross + 1)

    def early_local(k):
        lev = pl.ds(first_level(*early_chunk(k)), q)
        return pltpu.make_async_copy(sp.at[:, lev], ext.at[:, lev, body], l_sem.at[k])

    def rest_local(s):
        skip = deep if s == 0 else 1 if s < cross else 0
        lev = pl.ds(first_level(s, skip), per - skip * q)
        return pltpu.make_async_copy(sp.at[:, lev], ext.at[:, lev, body], l_sem.at[early])

    def block_copy(s, c):
        return pltpu.make_async_remote_copy(
            adv.at[:, pl.ds(first_level(s, c), q)],
            cells.at[mine, pl.ds(c * q, q)],
            d_send.at[0], d_recv.at[c],
            device_id={"tracer": target(s)}, device_id_type=MESH,
        )

    def inner_copy(s, c, i):
        return pltpu.make_async_remote_copy(
            adv.at[:, first_level(s, c) + i, inner],
            cells.at[mine, c * q + i, inner],
            d_send.at[0], d_recv.at[c],
            device_id={"tracer": target(s)}, device_id_type=MESH,
        )

    def outer_copy(s, c, side, skip=0):
        edge = pl.ds(side * (rows - EDGE), EDGE)
        return pltpu.make_async_remote_copy(
            adv.at[:, pl.ds(first_level(s, c) + skip, q - skip), edge],
            cells.at[mine, pl.ds(c * q + skip, q - skip), edge],
            d_send.at[0], d_recv.at[c],
            device_id={"tracer": target(s)}, device_id_type=MESH,
        )

    def raw_copy():
        return pltpu.make_async_remote_copy(
            sp.at[:, first_level(0, 0)], raw.at[:, body], r_send.at[0], r_recv.at[0],
            device_id={"tracer": target(0)}, device_id_type=MESH,
        )

    def raw_edges():
        return pair(raw.at[:, body], raw, (slice(None),), r_send.at[0], r_recv.at[1])

    def wait_first():
        for given, mask in ((0, late), (1, jnp.logical_not(late))):
            @pl.when(mask)
            def _():
                settle(adv.at[:, pl.ds(0, (ranks - 1) * q - given)], d_recv.at[0])

    def wait_blocks(c):
        settle(cells.at[pl.ds(0, (ranks - 1) * nt), pl.ds(c * q, q)], d_recv.at[c])

    partner = a * cores + cores - 1 - b

    def part_copy():
        return pltpu.make_async_remote_copy(
            pre.at[:, cores - 1 - b], part, o_send.at[0], o_recv.at[0],
            device_id={"tracer": partner}, device_id_type=MESH,
        )

    def over_copy(k):
        there = lax.rem(a + k, chips)
        return pltpu.make_async_remote_copy(
            joined.at[there], over.at[k - 1], o_send.at[k], o_recv.at[k],
            device_id={"tracer": there * cores + b}, device_id_type=MESH,
        )

    def gets_over(k):
        return lax.rem(a + k, chips) * cores + b > 0

    def in_cross(m):
        return lax.rem(m, cross), m // cross

    def in_near(m):
        return cross + m // nc, lax.rem(m, nc)

    last_core = a * cores + cores - 1
    late = b == cores - 1
    barrier = pltpu.get_barrier_semaphore()
    if cores > 1:
        @pl.when(jnp.logical_not(late))
        def _():
            for s in range(0, cross, cores):
                pl.semaphore_signal(
                    barrier, inc=1, device_id={"tracer": target(s)}, device_id_type=MESH
                )
            pl.semaphore_signal(barrier, inc=1, device_id={"tracer": last_core}, device_id_type=MESH)
    for place in (up, down):
        pl.semaphore_signal(
            barrier, inc=1, device_id={"tile": place, "tracer": last_core}, device_id_type=MESH
        )
    for s in range(cores - 1, cross, cores):
        pl.semaphore_signal(barrier, inc=1, device_id={"tracer": target(s)}, device_id_type=MESH)

    dep_local = pltpu.make_async_copy(dep, dext.at[body], ls_sem.at[0])
    th_local = pltpu.make_async_copy(th, hext.at[:, body], ls_sem.at[1])
    sun_local = pltpu.make_async_copy(sun, aux.at[1], ls_sem.at[2])
    tables = [
        pltpu.make_async_copy(src, dst, t_sem.at[k])
        for k, (src, dst) in enumerate(((eaten_in, eaten), (att_in, att), (rate_in, rate)))
    ]
    dep_local.start()
    tables[1].start()

    flow_local(0).start()

    def start_early(k, carry):
        early_local(k).start()
        return carry

    early_local(0).start()
    @pl.when(jnp.logical_not(late))
    def _():
        pl.semaphore_wait(barrier, chips - 1)
        raw_copy().start()

    lax.fori_loop(1, early, start_early, 0)
    for s in range(1, ranks):
        flow_local(s).start()

    tot[...] = jnp.zeros_like(tot)
    dep_local.wait()
    tables[1].wait()

    def advect(lev, block, base, size, skip, first, keep, put, take=None, owner=r):
        window = pl.ds(base, size)
        kept = pl.ds(first, keep)
        lane = lane_index((size, width))
        wet = jnp.where(lev < dext[window], 1.0, 0.0)
        es = sub_step * (fext[0, lev, window] * wet * east(wet))
        ns = sub_step * (fext[1, lev, window] * wet * north(wet))

        def one_tracer(t, acc):
            c = substep(take(t) if take else ext[t, lev, window], es, ns, lane)
            c = substep(c, es, ns, lane)[skip:skip + keep]
            put(t, lev, kept, c)
            return acc + att[owner * nt + t] * jnp.abs(c)

        tot[block, kept] = lax.fori_loop(0, nt, one_tracer, tot[block, kept], unroll=True)

    def strip(ref, *lead):
        return jnp.concatenate(
            [ref[lead + (pl.ds(full - TILE, TILE),)], ref[lead + (pl.ds(0, PAD + TILE),)]], axis=0
        )

    def put_adv(t, lev, kept, c):
        adv[t, lev, kept] = c

    def put_cells(t, lev, kept, c):
        cells[r * nt + t, lev - r * per, kept] = c

    def advance_inner(s, c, i):
        lev = first_level(s, c) + i
        advect(lev, target(s), PAD, rows, EDGE, EDGE, rows - 2 * EDGE, put_adv)

    def advance_outer(s, c, i):
        lev = first_level(s, c) + i
        block = target(s)
        size = TILE + PAD + TILE
        lane = lane_index((size, width))
        wet = jnp.where(lev < strip(dext), 1.0, 0.0)
        es = sub_step * (strip(fext, 0, lev) * wet * east(wet))
        ns = sub_step * (strip(fext, 1, lev) * wet * north(wet))
        high, low = slice(TILE - EDGE, TILE), slice(TILE + PAD, TILE + PAD + EDGE)
        high_rows, low_rows = pl.ds(rows - EDGE, EDGE), pl.ds(0, EDGE)

        def one_tracer(t, acc):
            c = substep(strip(ext, t, lev), es, ns, lane)
            c = substep(c, es, ns, lane)
            adv[t, lev, high_rows] = c[high]
            adv[t, lev, low_rows] = c[low]
            return acc + att[r * nt + t] * jnp.abs(c)

        acc = lax.fori_loop(0, nt, one_tracer, jnp.zeros((size, width), jnp.float32), unroll=True)
        tot[block, high_rows] += acc[high]
        tot[block, low_rows] += acc[low]

    def advance(s, c, put):
        block = target(s)
        level_0 = first_level(s, c)

        def one_level(i, carry):
            advect(level_0 + i, block, 0, full, PAD, 0, rows, put)
            return carry

        lax.fori_loop(0, q, one_level, 0)

    def start_edges(order):
        def step(m, carry):
            for copy in edges(*order(m)):
                copy.start()
            return carry
        return step

    turn = jnp.where(late, 0, deep * q - 1)

    def inner_step(m, carry):
        k, i = m // q, lax.rem(m, q)
        s, c = early_chunk(k)

        @pl.when(m == 0)
        def _():
            flow_local(0).wait()

        @pl.when(m == deep * q)
        def _():
            settle(fext.at[:, pl.ds(0, (ranks - 1) * per), body], lf_sem.at[1])

        @pl.when(i == 0)
        def _():
            early_local(k).wait()

        @pl.when(jnp.logical_or(late, m > 0))
        def _():
            advance_inner(s, c, i)

            @pl.when(m == 0)
            def _():
                pl.semaphore_wait(barrier, cross + cores - 1 + 2 * cores)

            inner_copy(s, c, i).start()

        @pl.when(m == turn)
        def _():
            if cores > 1:
                @pl.when(late)
                def _():
                    pl.semaphore_signal(
                        ready, inc=1, device_id={"tracer": partner}, device_id_type=MESH
                    )

                @pl.when(jnp.logical_not(late))
                def _():
                    pl.semaphore_wait(ready, 1)

            for copy in depth_edges():
                copy.start()
            lax.fori_loop(0, cross, start_edges(in_cross), 0)

        return carry

    lax.fori_loop(0, early * q, inner_step, 0)
    lax.fori_loop(cross, cross * nc, start_edges(in_cross), 0)
    for s in range(ranks):
        rest_local(s).start()

    @pl.when(jnp.logical_not(late))
    def _():
        raw_copy().wait_recv()
        for copy in raw_edges():
            copy.start()

    lax.fori_loop(0, cores * nc, start_edges(in_near), 0)
    for copy in heat_edges():
        copy.start()
    th_local.start()
    sun_local.start()
    tables[0].start()
    tables[2].start()
    tables[0].wait()
    tables[2].wait()

    def invert(s, carry):
        who = jnp.int32(0)
        for t in range(count):
            who = jnp.where(eaten[t] == s, jnp.int32(t), who)
        eater[s] = who
        return carry

    lax.fori_loop(0, count, invert, 0)

    settle(dext.at[pl.ds(0, 2 * EDGE)], s_recv.at[1])

    def outer_step(k, carry):
        s, c = edge_chunk(k)

        @pl.when(s == 0)
        def _():
            wait_edges(c, cross * q)

        def sides(i, carry):
            advance_outer(s, c, i)
            return carry

        given = jnp.logical_and(jnp.logical_not(late), k == 0)
        lax.fori_loop(jnp.where(given, 1, 0), q, sides, 0)

        @pl.when(jnp.logical_not(given))
        def _():
            for side in range(2):
                outer_copy(s, c, side).start()

        if q > 1:
            @pl.when(given)
            def _():
                for side in range(2):
                    outer_copy(s, c, side, 1).start()

        return carry

    lax.fori_loop(0, early, outer_step, 0)

    settle(ext.at[:, pl.ds(0, nl - early * q), body], l_sem.at[early])

    def away_step(m, carry):
        far = m < cross * nc
        k = m - cross * nc
        s = jnp.where(far, lax.rem(m, cross), cross + k // nc)
        c = jnp.where(far, m // cross, lax.rem(k, nc))

        @pl.when(jnp.logical_and(far, jnp.logical_and(s == 0, c >= deep)))
        def _():
            wait_edges(c, cross * q)

        @pl.when(jnp.logical_and(jnp.logical_not(far), c == 0))
        def _():
            wait_edges(nc + s - cross, per)

        @pl.when(jnp.logical_or(s > 0, c >= deep))
        def _():
            advance(s, c, put_adv)

            @pl.when(m != cross * nc - 1)
            def _():
                block_copy(s, c).start()

        return carry

    lax.fori_loop(cross, (ranks - 1) * nc, away_step, 0)

    wait_edges(own_group, q)

    @pl.when(jnp.logical_not(late))
    def _():
        giver = lax.rem(a + chips - 1, chips) * cores

        def put_given(t, lev, kept, c):
            cells[giver * nt + t, 0, kept] = c

        settle(raw.at[:, pl.ds(0, 2 * EDGE)], r_recv.at[1])
        advect(r * per, r, 0, full, PAD, 0, rows, put_given, lambda t: raw[t], giver)

    def own_step(c, carry):
        @pl.when(c > 0)
        def _():
            wait_edges(own_group + c, q)

        advance(ranks - 1, c, put_cells)
        return carry

    lax.fori_loop(0, nc, own_step, 0)

    lane = lane_index((full, width))
    coriolis = coriolis_base + beta_plane * lane.astype(jnp.float32) / width

    def momentum(i, carry):
        lev = r * per + i
        u, v, heat_ext = fext[0, lev], fext[1, lev], hext[i]
        wet = jnp.where(lev < dext[...], 1.0, 0.0)
        v_east, u_west = east(v), west(u)
        v_bar = 0.25 * (v + v_east + south(v) + south(v_east))
        u_bar = 0.25 * (u + u_west + north(u) + north(u_west))
        new_u = u + step_duration * (
            coriolis * v_bar - gravity * (east(heat_ext) - heat_ext) + viscosity * laplacian(u)
        )
        new_v = v + step_duration * (
            -coriolis * u_bar - gravity * (north(heat_ext) - heat_ext) + viscosity * laplacian(v)
        )
        vel[0, i] = (wet * east(wet) * new_u)[PAD:PAD + rows]
        vel[1, i] = (wet * north(wet) * new_v)[PAD:PAD + rows]
        warmer = heat_ext + step_duration * spreading_coefficient * laplacian(heat_ext)
        heat[i] = warmer[PAD:PAD + rows]
        return carry

    def move():
        th_local.wait()
        sun_local.wait()
        settle(hext.at[:, pl.ds(0, 2 * EDGE)], s_recv.at[0])
        lax.fori_loop(0, per, momentum, 0)

    above = jnp.zeros((rows, width), jnp.float32)
    for place in range(ranks):
        pre[place // cores, place % cores] = above
        above = above + tot[place]
    if cores > 1:
        part_copy().start()

        @pl.when(jnp.logical_not(late))
        def _():
            move()

        part_copy().wait()
        for k in range(chips):
            joined[k] = pre[k, b] + part[k]
    else:
        for k in range(chips):
            joined[k] = pre[k, b]
    for k in range(1, chips):
        @pl.when(gets_over(k))
        def _():
            over_copy(k).start()

    block_copy(cross - 1, nc - 1).start()

    @pl.when(late)
    def _():
        move()

    depth = dext[PAD:PAD + rows].astype(jnp.float32)
    aux[2] = depth
    scale = column_optical / nl
    clear = (r * per).astype(jnp.float32) * water_clear

    @pl.when(r == 0)
    def _():
        aux[0] = jnp.zeros((rows, width), jnp.float32)

    @pl.when(r > 0)
    def _():
        above = joined[a]
        for k in range(1, chips):
            over_copy(k).wait_recv()
            above = above + over[k - 1]
        aux[0] = (above + clear) * scale

    def react_chunk(c, carry):
        @pl.when(c == 0)
        def _():
            wait_first()

        @pl.when(c > 0)
        def _():
            wait_blocks(c)

        def one_level(j, carry):
            i = c * q + j

            def put(t, x):
                cells[t, i] = x

            level = (r * per + i).astype(jnp.float32)
            wet, caught, below = react_level(
                count, level, aux[2], aux[1], aux[0], cells, i,
                eaten, eater, att, rate, scale, sat, pull, put,
            )
            aux[0] = below
            heat[i] = wet * (heat[i] + warming_coefficient * (caught * wet))
            return carry

        lax.fori_loop(0, q, one_level, 0)
        return carry

    lax.fori_loop(0, nc - 1, react_chunk, 0)

    settle(edge_rows(nl), edge_send.at[0])
    settle(th.at[:, pl.ds(0, 2 * EDGE)], edge_send.at[1])
    settle(dep.at[pl.ds(0, 2 * EDGE)], edge_send.at[2])
    for k in range(1, chips):
        @pl.when(gets_over(k))
        def _():
            over_copy(k).wait_send()

    for given, mask in ((0, late), (1, jnp.logical_not(late))):
        @pl.when(mask)
        def _():
            settle(adv.at[:, pl.ds(0, (ranks - 1) * per - given)], d_send.at[0])

    @pl.when(jnp.logical_not(late))
    def _():
        settle(raw, r_send.at[0])

    wait_blocks(nc - 1)


def finish_kernel(
    levels, q,
    cells, vel, heat, aux, eaten_in, att_in, rate_in,
    out, vel_out, temp_out,
    eaten, att, rate, last, warm, sat, pull, eater, sem, t_sem,
):
    count, per = cells.shape[:2]
    r = lax.axis_index("tracer")
    done = per - q
    scale = column_optical / levels
    copies = [
        pltpu.make_async_copy(cells.at[:, pl.ds(0, done)], out.at[:, pl.ds(0, done)], sem.at[0]),
        pltpu.make_async_copy(vel, vel_out, sem.at[1]),
        pltpu.make_async_copy(heat.at[pl.ds(0, done)], temp_out.at[pl.ds(0, done)], sem.at[1]),
    ]
    tables = [
        pltpu.make_async_copy(src, dst, t_sem.at[k])
        for k, (src, dst) in enumerate(((eaten_in, eaten), (att_in, att), (rate_in, rate)))
    ]
    for copy in tables + copies:
        copy.start()
    for copy in tables:
        copy.wait()
    for t in range(count):
        eater[eaten[t]] = t

    def level_copy(j):
        return pltpu.make_async_copy(last.at[j], out.at[:, done + j], sem.at[0])

    def one_level(j, tau):
        def put(t, x):
            last[j, t] = x

        level = (r * per + done + j).astype(jnp.float32)
        wet, caught, below = react_level(
            count, level, aux[2], aux[1], tau, cells, done + j,
            eaten, eater, att, rate, scale, sat, pull, put,
        )
        warm[j] = wet * (heat[done + j] + warming_coefficient * (caught * wet))
        level_copy(j).start()
        return below

    lax.fori_loop(0, q, one_level, aux[0])
    warm_copy = pltpu.make_async_copy(warm, temp_out.at[pl.ds(done, q)], sem.at[1])
    warm_copy.start()
    flows = cells.at[pl.ds(0, 3 * per), 0]
    pltpu.make_async_copy(cells, cells, sem.at[0]).wait()
    pltpu.make_async_copy(flows, flows, sem.at[1]).wait()


def solution(mesh):
    tiles, ranks = mesh.shape["tile"], mesh.shape["tracer"]
    cores = 2 if ranks % 2 == 0 else 1

    def on_device(
        species_amounts,
        face_currents,
        thermal_anomaly,
        layer_total_per_profile,
        consumed_species,
        attenuation_factor,
        intake_speedup,
        incoming_sunshine,
    ):
        nt, nl, rows, width = species_amounts.shape
        per = nl // ranks
        q = 2 if per % 2 == 0 else 1
        nc = per // q
        count = ranks * nt
        cross = ranks - cores
        chips = ranks // cores
        deep = min(DEEP, nc - 1)
        full = rows + PAD
        f32 = jnp.float32
        any_space = pl.BlockSpec(memory_space=pl.ANY)
        vmem = pl.BlockSpec(memory_space=pltpu.VMEM)
        dma = pltpu.SemaphoreType.DMA
        cells, vel, heat, aux = pl.pallas_call(
            functools.partial(transport_kernel, tiles, ranks, cores, q, deep),
            out_shape=(
                pltpu.VMEM((count, per, rows, width), f32),
                pltpu.VMEM((2, per, rows, width), f32),
                pltpu.VMEM((per, rows, width), f32),
                pltpu.VMEM((3, rows, width), f32),
            ),
            in_specs=[any_space] * 8,
            out_specs=(vmem, vmem, vmem, vmem),
            scratch_shapes=[
                pltpu.SMEM((count,), jnp.int32),
                pltpu.SMEM((count,), f32),
                pltpu.SMEM((count,), f32),
                pltpu.VMEM((nt, nl, full, width), f32),
                pltpu.VMEM((2, nl, full, width), f32),
                pltpu.VMEM((per, full, width), f32),
                pltpu.VMEM((full, width), jnp.int32),
                pltpu.VMEM((nt, nl, rows, width), f32),
                pltpu.VMEM((ranks, rows, width), f32),
                pltpu.VMEM((chips, cores, rows, width), f32),
                pltpu.VMEM((chips, rows, width), f32),
                pltpu.VMEM((chips, rows, width), f32),
                pltpu.VMEM((chips, rows, width), f32),
                pltpu.VMEM((count, rows, width), f32),
                pltpu.VMEM((count, rows, width), f32),
                pltpu.SMEM((count,), jnp.int32),
                pltpu.VMEM((nt, full, width), f32),
                dma((3,)), dma((2 * nc + cores - 1,)), dma((2,)),
                dma((1,)), dma((nc,)), dma((chips,)), dma((chips,)),
                dma((deep + cross,)), dma((2,)), dma((3,)), dma((3,)),
                dma((1,)), dma((2,)), pltpu.SemaphoreType.REGULAR,
            ],
            compiler_params=pltpu.CompilerParams(
                collective_id=0, has_side_effects=True, vmem_limit_bytes=48 << 20
            ),
            name="transport",
        )(
            *(pltpu.with_memory_space_constraint(x, HBM) for x in (
                species_amounts, face_currents, thermal_anomaly,
                layer_total_per_profile, incoming_sunshine,
                consumed_species, attenuation_factor, intake_speedup,
            ))
        )
        return pl.pallas_call(
            functools.partial(finish_kernel, nl, q),
            out_shape=(
                jax.ShapeDtypeStruct((count, per, rows, width), f32),
                jax.ShapeDtypeStruct((2, per, rows, width), f32),
                jax.ShapeDtypeStruct((per, rows, width), f32),
            ),
            in_specs=[vmem] * 4 + [any_space] * 3,
            out_specs=(any_space, any_space, any_space),
            scratch_shapes=[
                pltpu.SMEM((count,), jnp.int32),
                pltpu.SMEM((count,), f32),
                pltpu.SMEM((count,), f32),
                pltpu.VMEM((q, count, rows, width), f32),
                pltpu.VMEM((q, rows, width), f32),
                pltpu.VMEM((count, rows, width), f32),
                pltpu.VMEM((count, rows, width), f32),
                pltpu.SMEM((count,), jnp.int32),
                dma((2,)), dma((3,)),
            ],
            compiler_params=pltpu.CompilerParams(vmem_limit_bytes=32 << 20),
            name="finish",
        )(
            cells, vel, heat, aux,
            consumed_species, attenuation_factor, intake_speedup,
        )

    return jax.shard_map(
        on_device,
        mesh=mesh,
        in_specs=(
            P(("groups", "tracer"), None, "tile", None),
            P(None, "groups", "tile", None),
            P(("groups", "tracer"), "tile", None),
            P(("groups", "tile"), None),
            P(),
            P(),
            P(),
            P(("groups", "tile"), None),
        ),
        out_specs=(
            P("groups", "tracer", "tile", None),
            P(None, ("groups", "tracer"), "tile", None),
            P(("groups", "tracer"), "tile", None),
        ),
        check_vma=False,
    )
```

```python
import functools

import jax
import jax.numpy as jnp
from jax import lax
from jax.experimental import pallas as pl
from jax.experimental.pallas import tpu as pltpu
from jax.sharding import PartitionSpec as P

MESH = pl.DeviceIdType.MESH

sub_step = 0.45
step_duration = 0.2
gravity = 0.5
viscosity = 0.2
coriolis_base = 0.5
beta_plane = 0.5
spreading_coefficient = 0.2
water_clear = 0.05
column_optical = 3.0
warming_coefficient = 5.0
light_half = 0.3
nutrient_half = 0.5

PAD = 8
EDGE = 4
TILE = 8
LOW_FLOW, HIGH_FLOW = 3, 2
DEEP = 2

HBM = pltpu.HBM


def lane_index(shape):
    return lax.broadcasted_iota(jnp.int32, shape, len(shape) - 1)


def east(x):
    return pltpu.roll(x, x.shape[0] - 1, 0)


def west(x):
    return pltpu.roll(x, 1, 0)


def north(x):
    return jnp.where(lane_index(x.shape) == x.shape[1] - 1, 0.0, pltpu.roll(x, x.shape[1] - 1, 1))


def south(x):
    return jnp.where(lane_index(x.shape) == 0, 0.0, pltpu.roll(x, 1, 1))


def minmod(a, b):
    return jnp.maximum(jnp.minimum(a, b), jnp.minimum(jnp.maximum(a, b), 0.0))


def laplacian(x):
    return east(x) + west(x) + north(x) + south(x) - 4.0 * x


def substep(c, es, ns, lane):
    last = c.shape[1] - 1
    e = 0.5 * c
    d = east(e) - e
    half = minmod(west(d), d)
    flux = es * jnp.where(es > 0.0, c + half, east(c - half))
    spread = flux - west(flux)
    d = jnp.where(lane == last, 0.0, pltpu.roll(e, last, 1)) - e
    half = minmod(jnp.where(lane == 0, e, pltpu.roll(d, 1, 1)), d)
    flux = ns * jnp.where(ns > 0.0, c + half, pltpu.roll(c - half, last, 1))
    return c - (spread + (flux - pltpu.roll(flux, 1, 1)))


def react_level(count, level, depth, sun, tau, cells, c, eaten, eater, att, rate, scale, sat, pull, put):
    total = jnp.full(depth.shape, water_clear, jnp.float32)
    for t in range(count):
        x = cells[t, c]
        size = jnp.abs(x)
        total = total + att[t] * size
        sat[t] = x / (nutrient_half + size)
        pull[t] = rate[t] * x
    optical = total * scale
    wet = jnp.where(level < depth, 1.0, 0.0)
    caught = sun * jnp.exp(-tau) * (1.0 - jnp.exp(-optical))
    mean_light = caught / optical
    gain = wet * (mean_light / (mean_light + light_half))
    for t in range(count):
        change = pull[t] * sat[eaten[t]] - pull[eater[t]] * sat[t]
        put(t, cells[t, c] + gain * change)
    return wet, caught, tau + optical


def transport_kernel(
    tiles, ranks, cores, q, deep,
    sp, fc, th, dep, sun, eaten_in, att_in, rate_in,
    cells, vel, heat, aux,
    eaten, att, rate, ext, fext, hext, dext, adv, tot, pre, part, joined, over, sat, pull, eater, raw,
    edge_send, g_recv, s_recv, d_send, d_recv, o_send, o_recv,
    l_sem, lf_sem, ls_sem, t_sem, r_send, r_recv, ready,
):
    nt, nl, rows, width = sp.shape
    per = nl // ranks
    nc = per // q
    count = ranks * nt
    chips = ranks // cores
    cross = ranks - cores
    full = rows + PAD
    early = deep + cross - 1
    r = lax.axis_index("tracer")
    z = lax.axis_index("tile")
    a, b = r // cores, lax.rem(r, cores)
    up, down = lax.rem(z + 1, tiles), lax.rem(z + tiles - 1, tiles)

    def target(s):
        k = lax.rem(s, cores)
        chip = lax.rem(a + 1 + s // cores, chips)
        core = jnp.where(s < cross, k, lax.rem(b + cores - 1 - k, cores))
        return chip * cores + core

    def first_level(s, c):
        return target(s) * per + c * q

    mine = pl.ds(r * nt, nt)
    body = pl.ds(PAD, rows)
    inner = pl.ds(EDGE, rows - 2 * EDGE)

    def settle(ref, sem):
        pltpu.make_async_copy(ref, ref, sem).wait()

    def pair(src, dst, lead, send, recv, low=EDGE, high=EDGE):
        return (
            pltpu.make_async_remote_copy(
                src.at[lead + (pl.ds(rows - low, low),)],
                dst.at[lead + (pl.ds(PAD - low, low),)],
                send, recv, device_id={"tile": up}, device_id_type=MESH,
            ),
            pltpu.make_async_remote_copy(
                src.at[lead + (pl.ds(0, high),)],
                dst.at[lead + (pl.ds(0, high),)],
                send, recv, device_id={"tile": down}, device_id_type=MESH,
            ),
        )

    def edges(s, c):
        g = jnp.where(s < cross, c, jnp.where(s < ranks - 1, nc + s - cross, own_group + c))
        lead = (slice(None), pl.ds(first_level(s, c), q))
        return (
            pair(fc, fext, lead, edge_send.at[0], g_recv.at[g], LOW_FLOW, HIGH_FLOW)
            + pair(sp, ext, lead, edge_send.at[0], g_recv.at[g])
        )

    own_group = nc + cores - 1

    def edge_rows(levels):
        return fext.at[:, pl.ds(0, levels), pl.ds(0, nt * EDGE + LOW_FLOW + HIGH_FLOW)]

    def wait_edges(g, levels):
        settle(edge_rows(levels), g_recv.at[g])

    def heat_edges():
        return pair(th, hext, (slice(None),), edge_send.at[1], s_recv.at[0])

    def depth_edges():
        return pair(dep, dext, (), edge_send.at[2], s_recv.at[1])

    def flow_local(s):
        lev = pl.ds(target(s) * per, per)
        sem = lf_sem.at[0] if s == 0 else lf_sem.at[1]
        return pltpu.make_async_copy(fc.at[:, lev], fext.at[:, lev, body], sem)

    def early_chunk(k):
        return jnp.where(k < deep, 0, k - deep + 1), jnp.where(k < deep, k, 0)

    def edge_chunk(k):
        return jnp.where(k < cross, k, 0), jnp.where(k < cross, 0, k - cross + 1)

    def early_local(k):
        lev = pl.ds(first_level(*early_chunk(k)), q)
        return pltpu.make_async_copy(sp.at[:, lev], ext.at[:, lev, body], l_sem.at[k])

    def rest_local(s):
        skip = deep if s == 0 else 1 if s < cross else 0
        lev = pl.ds(first_level(s, skip), per - skip * q)
        return pltpu.make_async_copy(sp.at[:, lev], ext.at[:, lev, body], l_sem.at[early])

    def block_copy(s, c):
        return pltpu.make_async_remote_copy(
            adv.at[:, pl.ds(first_level(s, c), q)],
            cells.at[mine, pl.ds(c * q, q)],
            d_send.at[0], d_recv.at[c],
            device_id={"tracer": target(s)}, device_id_type=MESH,
        )

    def inner_copy(s, c, i):
        return pltpu.make_async_remote_copy(
            adv.at[:, first_level(s, c) + i, inner],
            cells.at[mine, c * q + i, inner],
            d_send.at[1], d_recv.at[jnp.where(c == 0, nc, c)],
            device_id={"tracer": target(s)}, device_id_type=MESH,
        )

    def outer_copy(s, c, side, skip=0):
        edge = pl.ds(side * (rows - EDGE), EDGE)
        return pltpu.make_async_remote_copy(
            adv.at[:, pl.ds(first_level(s, c) + skip, q - skip), edge],
            cells.at[mine, pl.ds(c * q + skip, q - skip), edge],
            d_send.at[2], d_recv.at[c],
            device_id={"tracer": target(s)}, device_id_type=MESH,
        )

    def raw_copy():
        return pltpu.make_async_remote_copy(
            sp.at[:, first_level(0, 0)], raw.at[:, body], r_send.at[0], r_recv.at[0],
            device_id={"tracer": target(0)}, device_id_type=MESH,
        )

    def raw_edges():
        return pair(raw.at[:, body], raw, (slice(None),), r_send.at[1], r_recv.at[1])

    def wait_first():
        for pieces, mask in ((cross * q, late), (cross * q - 1, jnp.logical_not(late))):
            @pl.when(mask)
            def _():
                strips = pl.ds(0, pieces + q * (rows // TILE))
                settle(ext.at[:, strips, pl.ds(0, TILE)], d_recv.at[0])
                settle(ext.at[:, pl.ds(0, pieces), inner], d_recv.at[nc])

    def wait_blocks(c):
        settle(cells.at[pl.ds(0, (ranks - 1) * nt), pl.ds(c * q, q)], d_recv.at[c])

    partner = a * cores + cores - 1 - b

    def part_copy():
        return pltpu.make_async_remote_copy(
            pre.at[:, cores - 1 - b], part, o_send.at[0], o_recv.at[0],
            device_id={"tracer": partner}, device_id_type=MESH,
        )

    def over_copy(k):
        there = lax.rem(a + k, chips)
        return pltpu.make_async_remote_copy(
            joined.at[there], over.at[k - 1], o_send.at[k], o_recv.at[k],
            device_id={"tracer": there * cores + b}, device_id_type=MESH,
        )

    def gets_over(k):
        return lax.rem(a + k, chips) * cores + b > 0

    def in_cross(m):
        return lax.rem(m, cross), m // cross

    def in_near(m):
        return cross + m // nc, lax.rem(m, nc)

    last_core = a * cores + cores - 1
    late = b == cores - 1
    barrier = pltpu.get_barrier_semaphore()
    if cores > 1:
        @pl.when(jnp.logical_not(late))
        def _():
            for s in range(0, cross, cores):
                pl.semaphore_signal(
                    barrier, inc=1, device_id={"tracer": target(s)}, device_id_type=MESH
                )
            pl.semaphore_signal(barrier, inc=1, device_id={"tracer": last_core}, device_id_type=MESH)
    for place in (up, down):
        pl.semaphore_signal(
            barrier, inc=1, device_id={"tile": place, "tracer": last_core}, device_id_type=MESH
        )
    for s in range(cores - 1, cross, cores):
        pl.semaphore_signal(barrier, inc=1, device_id={"tracer": target(s)}, device_id_type=MESH)

    dep_local = pltpu.make_async_copy(dep, dext.at[body], ls_sem.at[0])
    th_local = pltpu.make_async_copy(th, hext.at[:, body], ls_sem.at[1])
    sun_local = pltpu.make_async_copy(sun, aux.at[1], ls_sem.at[2])
    tables = [
        pltpu.make_async_copy(src, dst, t_sem.at[k])
        for k, (src, dst) in enumerate(((eaten_in, eaten), (att_in, att), (rate_in, rate)))
    ]
    dep_local.start()
    tables[1].start()

    flow_local(0).start()

    def start_early(k, carry):
        early_local(k).start()
        return carry

    early_local(0).start()
    @pl.when(jnp.logical_not(late))
    def _():
        pl.semaphore_wait(barrier, chips - 1)
        raw_copy().start()

    lax.fori_loop(1, early, start_early, 0)
    for s in range(1, ranks):
        flow_local(s).start()

    tot[...] = jnp.zeros_like(tot)
    dep_local.wait()
    tables[1].wait()

    def advect(lev, block, base, size, skip, first, keep, put, take=None, owner=r):
        window = pl.ds(base, size)
        kept = pl.ds(first, keep)
        lane = lane_index((size, width))
        wet = jnp.where(lev < dext[window], 1.0, 0.0)
        es = sub_step * (fext[0, lev, window] * wet * east(wet))
        ns = sub_step * (fext[1, lev, window] * wet * north(wet))

        def one_tracer(t, acc):
            c = substep(take(t) if take else ext[t, lev, window], es, ns, lane)
            c = substep(c, es, ns, lane)[skip:skip + keep]
            put(t, lev, kept, c)
            return acc + att[owner * nt + t] * jnp.abs(c)

        tot[block, kept] = lax.fori_loop(0, nt, one_tracer, tot[block, kept], unroll=True)

    def strip(ref, *lead):
        return jnp.concatenate(
            [ref[lead + (pl.ds(full - TILE, TILE),)], ref[lead + (pl.ds(0, PAD + TILE),)]], axis=0
        )

    def put_adv(t, lev, kept, c):
        adv[t, lev, kept] = c

    def put_cells(t, lev, kept, c):
        cells[r * nt + t, lev - r * per, kept] = c

    def advance_inner(s, c, i):
        lev = first_level(s, c) + i
        advect(lev, target(s), PAD, rows, EDGE, EDGE, rows - 2 * EDGE, put_adv)

    def advance_outer(s, c, i):
        lev = first_level(s, c) + i
        block = target(s)
        size = TILE + PAD + TILE
        lane = lane_index((size, width))
        wet = jnp.where(lev < strip(dext), 1.0, 0.0)
        es = sub_step * (strip(fext, 0, lev) * wet * east(wet))
        ns = sub_step * (strip(fext, 1, lev) * wet * north(wet))
        high, low = slice(TILE - EDGE, TILE), slice(TILE + PAD, TILE + PAD + EDGE)
        high_rows, low_rows = pl.ds(rows - EDGE, EDGE), pl.ds(0, EDGE)

        def one_tracer(t, acc):
            c = substep(strip(ext, t, lev), es, ns, lane)
            c = substep(c, es, ns, lane)
            adv[t, lev, high_rows] = c[high]
            adv[t, lev, low_rows] = c[low]
            return acc + att[r * nt + t] * jnp.abs(c)

        acc = lax.fori_loop(0, nt, one_tracer, jnp.zeros((size, width), jnp.float32), unroll=True)
        tot[block, high_rows] += acc[high]
        tot[block, low_rows] += acc[low]

    def advance(s, c, put):
        block = target(s)
        level_0 = first_level(s, c)

        def one_level(i, carry):
            advect(level_0 + i, block, 0, full, PAD, 0, rows, put)
            return carry

        lax.fori_loop(0, q, one_level, 0)

    def start_edges(order):
        def step(m, carry):
            for copy in edges(*order(m)):
                copy.start()
            return carry
        return step

    turn = jnp.where(late, 0, deep * q - 1)

    def inner_step(m, carry):
        k, i = m // q, lax.rem(m, q)
        s, c = early_chunk(k)

        @pl.when(m == 0)
        def _():
            flow_local(0).wait()

        @pl.when(m == deep * q)
        def _():
            settle(fext.at[:, pl.ds(0, (ranks - 1) * per), body], lf_sem.at[1])

        @pl.when(i == 0)
        def _():
            early_local(k).wait()

        @pl.when(jnp.logical_or(late, m > 0))
        def _():
            advance_inner(s, c, i)

            @pl.when(m == 0)
            def _():
                pl.semaphore_wait(barrier, cross + cores - 1 + 2 * cores)

            inner_copy(s, c, i).start()

        @pl.when(m == turn)
        def _():
            if cores > 1:
                @pl.when(late)
                def _():
                    pl.semaphore_signal(
                        ready, inc=1, device_id={"tracer": partner}, device_id_type=MESH
                    )

                @pl.when(jnp.logical_not(late))
                def _():
                    pl.semaphore_wait(ready, 1)

            for copy in depth_edges():
                copy.start()
            lax.fori_loop(0, cross, start_edges(in_cross), 0)

        return carry

    lax.fori_loop(0, early * q, inner_step, 0)
    lax.fori_loop(cross, cross * nc, start_edges(in_cross), 0)
    for s in range(ranks):
        rest_local(s).start()

    @pl.when(jnp.logical_not(late))
    def _():
        raw_copy().wait_recv()
        for copy in raw_edges():
            copy.start()

    lax.fori_loop(0, cores * nc, start_edges(in_near), 0)
    for copy in heat_edges():
        copy.start()
    th_local.start()
    sun_local.start()
    tables[0].start()
    tables[2].start()
    tables[0].wait()
    tables[2].wait()

    def invert(s, carry):
        who = jnp.int32(0)
        for t in range(count):
            who = jnp.where(eaten[t] == s, jnp.int32(t), who)
        eater[s] = who
        return carry

    lax.fori_loop(0, count, invert, 0)

    settle(dext.at[pl.ds(0, 2 * EDGE)], s_recv.at[1])

    def outer_step(k, carry):
        s, c = edge_chunk(k)

        @pl.when(s == 0)
        def _():
            wait_edges(c, cross * q)

        def sides(i, carry):
            advance_outer(s, c, i)
            return carry

        given = jnp.logical_and(jnp.logical_not(late), k == 0)
        lax.fori_loop(jnp.where(given, 1, 0), q, sides, 0)

        @pl.when(jnp.logical_not(given))
        def _():
            for side in range(2):
                outer_copy(s, c, side).start()

        if q > 1:
            @pl.when(given)
            def _():
                for side in range(2):
                    outer_copy(s, c, side, 1).start()

        return carry

    lax.fori_loop(0, early, outer_step, 0)

    settle(ext.at[:, pl.ds(0, nl - early * q), body], l_sem.at[early])

    holds = functools.reduce(jnp.logical_or, [gets_over(k) for k in range(1, chips)])

    def away_step(m, carry):
        far = m < cross * nc
        k = m - cross * nc
        s = jnp.where(far, lax.rem(m, cross), cross + k // nc)
        c = jnp.where(far, m // cross, lax.rem(k, nc))

        @pl.when(jnp.logical_and(far, jnp.logical_and(s == 0, c >= deep)))
        def _():
            wait_edges(c, cross * q)

        @pl.when(jnp.logical_and(jnp.logical_not(far), c == 0))
        def _():
            wait_edges(nc + s - cross, per)

        @pl.when(jnp.logical_or(s > 0, c >= deep))
        def _():
            advance(s, c, put_adv)

            @pl.when(jnp.logical_or(m != cross * nc - 1, jnp.logical_not(holds)))
            def _():
                block_copy(s, c).start()

        return carry

    lax.fori_loop(cross, (ranks - 1) * nc, away_step, 0)

    wait_edges(own_group, q)

    @pl.when(jnp.logical_not(late))
    def _():
        giver = lax.rem(a + chips - 1, chips) * cores

        def put_given(t, lev, kept, c):
            cells[giver * nt + t, 0, kept] = c

        settle(raw.at[:, pl.ds(0, 2 * EDGE)], r_recv.at[1])
        advect(r * per, r, 0, full, PAD, 0, rows, put_given, lambda t: raw[t], giver)

    def own_step(c, carry):
        @pl.when(c > 0)
        def _():
            wait_edges(own_group + c, q)

        advance(ranks - 1, c, put_cells)
        return carry

    lax.fori_loop(0, nc, own_step, 0)

    above = jnp.zeros((rows, width), jnp.float32)
    for place in range(ranks):
        pre[place // cores, place % cores] = above
        above = above + tot[place]
    if cores > 1:
        part_copy().start()
        part_copy().wait()
        for k in range(chips):
            joined[k] = pre[k, b] + part[k]
    else:
        for k in range(chips):
            joined[k] = pre[k, b]
    for k in range(1, chips):
        @pl.when(gets_over(k))
        def _():
            over_copy(k).start()

    @pl.when(holds)
    def _():
        block_copy(cross - 1, nc - 1).start()

    th_local.wait()
    sun_local.wait()
    settle(hext.at[:, pl.ds(0, 2 * EDGE)], s_recv.at[0])
    lane = lane_index((full, width))
    coriolis = coriolis_base + beta_plane * lane.astype(jnp.float32) / width

    def momentum(i, carry):
        lev = r * per + i
        u, v, heat_ext = fext[0, lev], fext[1, lev], hext[i]
        wet = jnp.where(lev < dext[...], 1.0, 0.0)
        v_east, u_west = east(v), west(u)
        v_bar = 0.25 * (v + v_east + south(v) + south(v_east))
        u_bar = 0.25 * (u + u_west + north(u) + north(u_west))
        new_u = u + step_duration * (
            coriolis * v_bar - gravity * (east(heat_ext) - heat_ext) + viscosity * laplacian(u)
        )
        new_v = v + step_duration * (
            -coriolis * u_bar - gravity * (north(heat_ext) - heat_ext) + viscosity * laplacian(v)
        )
        vel[0, i] = (wet * east(wet) * new_u)[PAD:PAD + rows]
        vel[1, i] = (wet * north(wet) * new_v)[PAD:PAD + rows]
        warmer = heat_ext + step_duration * spreading_coefficient * laplacian(heat_ext)
        heat[i] = warmer[PAD:PAD + rows]
        return carry

    lax.fori_loop(0, per, momentum, 0)

    depth = dext[PAD:PAD + rows].astype(jnp.float32)
    aux[2] = depth
    scale = column_optical / nl
    clear = (r * per).astype(jnp.float32) * water_clear

    @pl.when(r == 0)
    def _():
        aux[0] = jnp.zeros((rows, width), jnp.float32)

    @pl.when(r > 0)
    def _():
        above = joined[a]
        for k in range(1, chips):
            over_copy(k).wait_recv()
            above = above + over[k - 1]
        aux[0] = (above + clear) * scale

    def react_chunk(c, carry):
        @pl.when(c == 0)
        def _():
            wait_first()

        @pl.when(c > 0)
        def _():
            wait_blocks(c)

        def one_level(j, carry):
            i = c * q + j

            def put(t, x):
                cells[t, i] = x

            level = (r * per + i).astype(jnp.float32)
            wet, caught, below = react_level(
                count, level, aux[2], aux[1], aux[0], cells, i,
                eaten, eater, att, rate, scale, sat, pull, put,
            )
            aux[0] = below
            heat[i] = wet * (heat[i] + warming_coefficient * (caught * wet))
            return carry

        lax.fori_loop(0, q, one_level, 0)
        return carry

    lax.fori_loop(0, nc - 1, react_chunk, 0)

    settle(edge_rows(nl), edge_send.at[0])
    settle(th.at[:, pl.ds(0, 2 * EDGE)], edge_send.at[1])
    settle(dep.at[pl.ds(0, 2 * EDGE)], edge_send.at[2])
    for k in range(1, chips):
        @pl.when(gets_over(k))
        def _():
            over_copy(k).wait_send()

    settle(adv.at[:, pl.ds(0, (ranks - 1) * per - early * q)], d_send.at[0])
    for pieces, mask in ((early * q, late), (early * q - 1, jnp.logical_not(late))):
        @pl.when(mask)
        def _():
            settle(ext.at[:, pl.ds(0, pieces), pl.ds(0, 2 * EDGE)], d_send.at[2])
            settle(ext.at[:, pl.ds(0, pieces), inner], d_send.at[1])

    @pl.when(jnp.logical_not(late))
    def _():
        raw_copy().wait_send()
        settle(raw.at[:, pl.ds(0, 2 * EDGE)], r_send.at[1])

    wait_blocks(nc - 1)


def finish_kernel(
    levels, q,
    cells, vel, heat, aux, eaten_in, att_in, rate_in,
    out, vel_out, temp_out,
    eaten, att, rate, last, warm, sat, pull, eater, sem, t_sem,
):
    count, per = cells.shape[:2]
    r = lax.axis_index("tracer")
    done = per - q
    scale = column_optical / levels
    copies = [
        pltpu.make_async_copy(cells.at[:, pl.ds(0, done)], out.at[:, pl.ds(0, done)], sem.at[0]),
        pltpu.make_async_copy(vel, vel_out, sem.at[1]),
        pltpu.make_async_copy(heat.at[pl.ds(0, done)], temp_out.at[pl.ds(0, done)], sem.at[2]),
    ]
    tables = [
        pltpu.make_async_copy(src, dst, t_sem.at[k])
        for k, (src, dst) in enumerate(((eaten_in, eaten), (att_in, att), (rate_in, rate)))
    ]
    for copy in tables + copies:
        copy.start()
    for copy in tables:
        copy.wait()
    for t in range(count):
        eater[eaten[t]] = t

    def level_copy(j):
        return pltpu.make_async_copy(last.at[j], out.at[:, done + j], sem.at[4])

    def one_level(j, tau):
        def put(t, x):
            last[j, t] = x

        level = (r * per + done + j).astype(jnp.float32)
        wet, caught, below = react_level(
            count, level, aux[2], aux[1], tau, cells, done + j,
            eaten, eater, att, rate, scale, sat, pull, put,
        )
        warm[j] = wet * (heat[done + j] + warming_coefficient * (caught * wet))
        level_copy(j).start()
        return below

    lax.fori_loop(0, q, one_level, aux[0])
    warm_copy = pltpu.make_async_copy(warm, temp_out.at[pl.ds(done, q)], sem.at[3])
    warm_copy.start()
    for copy in copies:
        copy.wait()
    pltpu.make_async_copy(last, last, sem.at[4]).wait()
    warm_copy.wait()


def solution(mesh):
    tiles, ranks = mesh.shape["tile"], mesh.shape["tracer"]
    cores = 2 if ranks % 2 == 0 else 1

    def on_device(
        species_amounts,
        face_currents,
        thermal_anomaly,
        layer_total_per_profile,
        consumed_species,
        attenuation_factor,
        intake_speedup,
        incoming_sunshine,
    ):
        nt, nl, rows, width = species_amounts.shape
        per = nl // ranks
        q = 2 if per % 2 == 0 else 1
        nc = per // q
        count = ranks * nt
        cross = ranks - cores
        chips = ranks // cores
        deep = min(DEEP, nc - 1)
        full = rows + PAD
        f32 = jnp.float32
        any_space = pl.BlockSpec(memory_space=pl.ANY)
        vmem = pl.BlockSpec(memory_space=pltpu.VMEM)
        dma = pltpu.SemaphoreType.DMA
        cells, vel, heat, aux = pl.pallas_call(
            functools.partial(transport_kernel, tiles, ranks, cores, q, deep),
            out_shape=(
                pltpu.VMEM((count, per, rows, width), f32),
                pltpu.VMEM((2, per, rows, width), f32),
                pltpu.VMEM((per, rows, width), f32),
                pltpu.VMEM((3, rows, width), f32),
            ),
            in_specs=[any_space] * 8,
            out_specs=(vmem, vmem, vmem, vmem),
            scratch_shapes=[
                pltpu.SMEM((count,), jnp.int32),
                pltpu.SMEM((count,), f32),
                pltpu.SMEM((count,), f32),
                pltpu.VMEM((nt, nl, full, width), f32),
                pltpu.VMEM((2, nl, full, width), f32),
                pltpu.VMEM((per, full, width), f32),
                pltpu.VMEM((full, width), jnp.int32),
                pltpu.VMEM((nt, nl, rows, width), f32),
                pltpu.VMEM((ranks, rows, width), f32),
                pltpu.VMEM((chips, cores, rows, width), f32),
                pltpu.VMEM((chips, rows, width), f32),
                pltpu.VMEM((chips, rows, width), f32),
                pltpu.VMEM((chips, rows, width), f32),
                pltpu.VMEM((count, rows, width), f32),
                pltpu.VMEM((count, rows, width), f32),
                pltpu.SMEM((count,), jnp.int32),
                pltpu.VMEM((nt, full, width), f32),
                dma((3,)), dma((2 * nc + cores - 1,)), dma((2,)),
                dma((3,)), dma((nc + 1,)), dma((chips,)), dma((chips,)),
                dma((deep + cross,)), dma((2,)), dma((3,)), dma((3,)),
                dma((2,)), dma((2,)), pltpu.SemaphoreType.REGULAR,
            ],
            compiler_params=pltpu.CompilerParams(
                collective_id=0, has_side_effects=True, vmem_limit_bytes=48 << 20
            ),
            name="transport",
        )(
            *(pltpu.with_memory_space_constraint(x, HBM) for x in (
                species_amounts, face_currents, thermal_anomaly,
                layer_total_per_profile, incoming_sunshine,
                consumed_species, attenuation_factor, intake_speedup,
            ))
        )
        return pl.pallas_call(
            functools.partial(finish_kernel, nl, q),
            out_shape=(
                jax.ShapeDtypeStruct((count, per, rows, width), f32),
                jax.ShapeDtypeStruct((2, per, rows, width), f32),
                jax.ShapeDtypeStruct((per, rows, width), f32),
            ),
            in_specs=[vmem] * 4 + [any_space] * 3,
            out_specs=(any_space, any_space, any_space),
            scratch_shapes=[
                pltpu.SMEM((count,), jnp.int32),
                pltpu.SMEM((count,), f32),
                pltpu.SMEM((count,), f32),
                pltpu.VMEM((q, count, rows, width), f32),
                pltpu.VMEM((q, rows, width), f32),
                pltpu.VMEM((count, rows, width), f32),
                pltpu.VMEM((count, rows, width), f32),
                pltpu.SMEM((count,), jnp.int32),
                dma((5,)), dma((3,)),
            ],
            compiler_params=pltpu.CompilerParams(vmem_limit_bytes=32 << 20),
            name="finish",
        )(
            cells, vel, heat, aux,
            consumed_species, attenuation_factor, intake_speedup,
        )

    return jax.shard_map(
        on_device,
        mesh=mesh,
        in_specs=(
            P(("groups", "tracer"), None, "tile", None),
            P(None, "groups", "tile", None),
            P(("groups", "tracer"), "tile", None),
            P(("groups", "tile"), None),
            P(),
            P(),
            P(),
            P(("groups", "tile"), None),
        ),
        out_specs=(
            P("groups", "tracer", "tile", None),
            P(None, ("groups", "tracer"), "tile", None),
            P(("groups", "tracer"), "tile", None),
        ),
        check_vma=False,
    )
```

```python
import functools

import jax
import jax.numpy as jnp
from jax import lax
from jax.experimental import pallas as pl
from jax.experimental.pallas import tpu as pltpu
from jax.sharding import PartitionSpec as P

MESH = pl.DeviceIdType.MESH

sub_step = 0.45
step_duration = 0.2
gravity = 0.5
viscosity = 0.2
coriolis_base = 0.5
beta_plane = 0.5
spreading_coefficient = 0.2
water_clear = 0.05
column_optical = 3.0
warming_coefficient = 5.0
light_half = 0.3
nutrient_half = 0.5

PAD = 8
EDGE = 4
TILE = 8
LOW_FLOW, HIGH_FLOW = 3, 2
DEEP = 2

HBM = pltpu.HBM


def lane_index(shape):
    return lax.broadcasted_iota(jnp.int32, shape, len(shape) - 1)


def east(x):
    return pltpu.roll(x, x.shape[0] - 1, 0)


def west(x):
    return pltpu.roll(x, 1, 0)


def north(x):
    return jnp.where(lane_index(x.shape) == x.shape[1] - 1, 0.0, pltpu.roll(x, x.shape[1] - 1, 1))


def south(x):
    return jnp.where(lane_index(x.shape) == 0, 0.0, pltpu.roll(x, 1, 1))


def minmod(a, b):
    return jnp.maximum(jnp.minimum(a, b), jnp.minimum(jnp.maximum(a, b), 0.0))


def laplacian(x):
    return east(x) + west(x) + north(x) + south(x) - 4.0 * x


def substep(c, es, ns, lane):
    last = c.shape[1] - 1
    e = 0.5 * c
    d = east(e) - e
    half = minmod(west(d), d)
    flux = es * jnp.where(es > 0.0, c + half, east(c - half))
    spread = flux - west(flux)
    d = jnp.where(lane == last, 0.0, pltpu.roll(e, last, 1)) - e
    half = minmod(jnp.where(lane == 0, e, pltpu.roll(d, 1, 1)), d)
    flux = ns * jnp.where(ns > 0.0, c + half, pltpu.roll(c - half, last, 1))
    return c - (spread + (flux - pltpu.roll(flux, 1, 1)))


def react_level(count, level, depth, sun, tau, cells, c, eaten, eater, att, rate, scale, sat, pull, put):
    total = jnp.full(depth.shape, water_clear, jnp.float32)
    for t in range(count):
        x = cells[t, c]
        size = jnp.abs(x)
        total = total + att[t] * size
        sat[t] = x / (nutrient_half + size)
        pull[t] = rate[t] * x
    optical = total * scale
    wet = jnp.where(level < depth, 1.0, 0.0)
    caught = sun * jnp.exp(-tau) * (1.0 - jnp.exp(-optical))
    mean_light = caught / optical
    gain = wet * (mean_light / (mean_light + light_half))
    for t in range(count):
        change = pull[t] * sat[eaten[t]] - pull[eater[t]] * sat[t]
        put(t, cells[t, c] + gain * change)
    return wet, caught, tau + optical


def transport_kernel(
    tiles, ranks, cores, q, deep,
    sp, fc, th, dep, sun, eaten_in, att_in, rate_in,
    cells, vel, heat, aux,
    eaten, att, rate, ext, fext, hext, dext, adv, tot, pre, part, joined, over, sat, pull, eater, raw,
    edge_send, g_recv, s_recv, d_send, d_recv, o_send, o_recv,
    l_sem, lf_sem, ls_sem, t_sem, r_send, r_recv, ready,
):
    nt, nl, rows, width = sp.shape
    per = nl // ranks
    nc = per // q
    count = ranks * nt
    chips = ranks // cores
    cross = ranks - cores
    full = rows + PAD
    early = deep + cross - 1
    r = lax.axis_index("tracer")
    z = lax.axis_index("tile")
    a, b = r // cores, lax.rem(r, cores)
    up, down = lax.rem(z + 1, tiles), lax.rem(z + tiles - 1, tiles)

    def target(s):
        k = lax.rem(s, cores)
        chip = lax.rem(a + 1 + s // cores, chips)
        core = jnp.where(s < cross, k, lax.rem(b + cores - 1 - k, cores))
        return chip * cores + core

    def first_level(s, c):
        return target(s) * per + c * q

    mine = pl.ds(r * nt, nt)
    body = pl.ds(PAD, rows)
    inner = pl.ds(EDGE, rows - 2 * EDGE)

    def settle(ref, sem):
        pltpu.make_async_copy(ref, ref, sem).wait()

    def pair(src, dst, lead, send, recv, low=EDGE, high=EDGE):
        return (
            pltpu.make_async_remote_copy(
                src.at[lead + (pl.ds(rows - low, low),)],
                dst.at[lead + (pl.ds(PAD - low, low),)],
                send, recv, device_id={"tile": up}, device_id_type=MESH,
            ),
            pltpu.make_async_remote_copy(
                src.at[lead + (pl.ds(0, high),)],
                dst.at[lead + (pl.ds(0, high),)],
                send, recv, device_id={"tile": down}, device_id_type=MESH,
            ),
        )

    def edges(s, c):
        g = jnp.where(s < cross, c, jnp.where(s < ranks - 1, nc + s - cross, own_group + c))
        lead = (slice(None), pl.ds(first_level(s, c), q))
        return (
            pair(fc, fext, lead, edge_send.at[0], g_recv.at[g], LOW_FLOW, HIGH_FLOW)
            + pair(sp, ext, lead, edge_send.at[0], g_recv.at[g])
        )

    own_group = nc + cores - 1

    def edge_rows(levels):
        return fext.at[:, pl.ds(0, levels), pl.ds(0, nt * EDGE + LOW_FLOW + HIGH_FLOW)]

    def wait_edges(g, levels):
        settle(edge_rows(levels), g_recv.at[g])

    def heat_edges():
        return pair(th, hext, (slice(None),), edge_send.at[1], s_recv.at[0])

    def depth_edges():
        return pair(dep, dext, (), edge_send.at[2], s_recv.at[1])

    def flow_local(s):
        lev = pl.ds(target(s) * per, per)
        sem = lf_sem.at[0] if s == 0 else lf_sem.at[1]
        return pltpu.make_async_copy(fc.at[:, lev], fext.at[:, lev, body], sem)

    def early_chunk(k):
        return jnp.where(k < deep, 0, k - deep + 1), jnp.where(k < deep, k, 0)

    def edge_chunk(k):
        return jnp.where(k < cross, k, 0), jnp.where(k < cross, 0, k - cross + 1)

    def early_local(k):
        lev = pl.ds(first_level(*early_chunk(k)), q)
        return pltpu.make_async_copy(sp.at[:, lev], ext.at[:, lev, body], l_sem.at[k])

    def rest_local(s):
        skip = deep if s == 0 else 1 if s < cross else 0
        lev = pl.ds(first_level(s, skip), per - skip * q)
        return pltpu.make_async_copy(sp.at[:, lev], ext.at[:, lev, body], l_sem.at[early])

    def block_copy(s, c):
        return pltpu.make_async_remote_copy(
            adv.at[:, pl.ds(first_level(s, c), q)],
            cells.at[mine, pl.ds(c * q, q)],
            d_send.at[0], d_recv.at[c],
            device_id={"tracer": target(s)}, device_id_type=MESH,
        )

    def inner_copy(s, c, i):
        return pltpu.make_async_remote_copy(
            adv.at[:, first_level(s, c) + i, inner],
            cells.at[mine, c * q + i, inner],
            d_send.at[1], d_recv.at[jnp.where(c == 0, nc, c)],
            device_id={"tracer": target(s)}, device_id_type=MESH,
        )

    def outer_copy(s, c, side, skip=0):
        edge = pl.ds(side * (rows - EDGE), EDGE)
        return pltpu.make_async_remote_copy(
            adv.at[:, pl.ds(first_level(s, c) + skip, q - skip), edge],
            cells.at[mine, pl.ds(c * q + skip, q - skip), edge],
            d_send.at[2], d_recv.at[c],
            device_id={"tracer": target(s)}, device_id_type=MESH,
        )

    def raw_copy():
        return pltpu.make_async_remote_copy(
            sp.at[:, first_level(0, 0)], raw.at[:, body], r_send.at[0], r_recv.at[0],
            device_id={"tracer": target(0)}, device_id_type=MESH,
        )

    def raw_edges():
        return pair(raw.at[:, body], raw, (slice(None),), r_send.at[1], r_recv.at[1])

    def wait_first():
        for pieces, mask in ((cross * q, late), (cross * q - 1, jnp.logical_not(late))):
            @pl.when(mask)
            def _():
                strips = pl.ds(0, pieces + q * (rows // TILE))
                settle(ext.at[:, strips, pl.ds(0, TILE)], d_recv.at[0])
                settle(ext.at[:, pl.ds(0, pieces), inner], d_recv.at[nc])

    def wait_blocks(c):
        settle(cells.at[pl.ds(0, (ranks - 1) * nt), pl.ds(c * q, q)], d_recv.at[c])

    partner = a * cores + cores - 1 - b

    def part_copy():
        return pltpu.make_async_remote_copy(
            pre.at[:, cores - 1 - b], part, o_send.at[0], o_recv.at[0],
            device_id={"tracer": partner}, device_id_type=MESH,
        )

    def over_copy(k):
        there = lax.rem(a + k, chips)
        return pltpu.make_async_remote_copy(
            joined.at[there], over.at[k - 1], o_send.at[k], o_recv.at[k],
            device_id={"tracer": there * cores + b}, device_id_type=MESH,
        )

    def gets_over(k):
        return lax.rem(a + k, chips) * cores + b > 0

    def in_cross(m):
        return lax.rem(m, cross), m // cross

    def in_near(m):
        return cross + m // nc, lax.rem(m, nc)

    last_core = a * cores + cores - 1
    late = b == cores - 1
    barrier = pltpu.get_barrier_semaphore()
    for place in (up, down):
        pl.semaphore_signal(
            barrier, inc=1, device_id={"tile": place, "tracer": last_core}, device_id_type=MESH
        )
    if cores > 1:
        @pl.when(jnp.logical_not(late))
        def _():
            for s in range(0, cross, cores):
                pl.semaphore_signal(
                    barrier, inc=1, device_id={"tracer": target(s)}, device_id_type=MESH
                )
            pl.semaphore_signal(barrier, inc=1, device_id={"tracer": last_core}, device_id_type=MESH)
    for s in range(cores - 1, cross, cores):
        pl.semaphore_signal(barrier, inc=1, device_id={"tracer": target(s)}, device_id_type=MESH)

    dep_local = pltpu.make_async_copy(dep, dext.at[body], ls_sem.at[0])
    th_local = pltpu.make_async_copy(th, hext.at[:, body], ls_sem.at[1])
    sun_local = pltpu.make_async_copy(sun, aux.at[1], ls_sem.at[2])
    tables = [
        pltpu.make_async_copy(src, dst, t_sem.at[k])
        for k, (src, dst) in enumerate(((eaten_in, eaten), (att_in, att), (rate_in, rate)))
    ]
    dep_local.start()
    tables[1].start()

    flow_local(0).start()

    def start_early(k, carry):
        early_local(k).start()
        return carry

    early_local(0).start()
    @pl.when(jnp.logical_not(late))
    def _():
        pl.semaphore_wait(barrier, chips - 1)
        raw_copy().start()

    lax.fori_loop(1, early, start_early, 0)
    for s in range(1, ranks):
        flow_local(s).start()

    tot[...] = jnp.zeros_like(tot)
    dep_local.wait()
    tables[1].wait()

    def advect(lev, block, base, size, skip, first, keep, put, take=None, owner=r):
        window = pl.ds(base, size)
        kept = pl.ds(first, keep)
        lane = lane_index((size, width))
        wet = jnp.where(lev < dext[window], 1.0, 0.0)
        es = sub_step * (fext[0, lev, window] * wet * east(wet))
        ns = sub_step * (fext[1, lev, window] * wet * north(wet))

        def one_tracer(t, acc):
            c = substep(take(t) if take else ext[t, lev, window], es, ns, lane)
            c = substep(c, es, ns, lane)[skip:skip + keep]
            put(t, lev, kept, c)
            return acc + att[owner * nt + t] * jnp.abs(c)

        tot[block, kept] = lax.fori_loop(0, nt, one_tracer, tot[block, kept], unroll=True)

    def strip(ref, *lead):
        return jnp.concatenate(
            [ref[lead + (pl.ds(full - TILE, TILE),)], ref[lead + (pl.ds(0, PAD + TILE),)]], axis=0
        )

    def put_adv(t, lev, kept, c):
        adv[t, lev, kept] = c

    def put_cells(t, lev, kept, c):
        cells[r * nt + t, lev - r * per, kept] = c

    def advance_inner(s, c, i):
        lev = first_level(s, c) + i
        advect(lev, target(s), PAD, rows, EDGE, EDGE, rows - 2 * EDGE, put_adv)

    def advance_outer(s, c, i):
        lev = first_level(s, c) + i
        block = target(s)
        size = TILE + PAD + TILE
        lane = lane_index((size, width))
        wet = jnp.where(lev < strip(dext), 1.0, 0.0)
        es = sub_step * (strip(fext, 0, lev) * wet * east(wet))
        ns = sub_step * (strip(fext, 1, lev) * wet * north(wet))
        high, low = slice(TILE - EDGE, TILE), slice(TILE + PAD, TILE + PAD + EDGE)
        high_rows, low_rows = pl.ds(rows - EDGE, EDGE), pl.ds(0, EDGE)

        def one_tracer(t, acc):
            c = substep(strip(ext, t, lev), es, ns, lane)
            c = substep(c, es, ns, lane)
            adv[t, lev, high_rows] = c[high]
            adv[t, lev, low_rows] = c[low]
            return acc + att[r * nt + t] * jnp.abs(c)

        acc = lax.fori_loop(0, nt, one_tracer, jnp.zeros((size, width), jnp.float32), unroll=True)
        tot[block, high_rows] += acc[high]
        tot[block, low_rows] += acc[low]

    def advance(s, c, put):
        block = target(s)
        level_0 = first_level(s, c)

        def one_level(i, carry):
            advect(level_0 + i, block, 0, full, PAD, 0, rows, put)
            return carry

        lax.fori_loop(0, q, one_level, 0)

    def start_edges(order):
        def step(m, carry):
            for copy in edges(*order(m)):
                copy.start()
            return carry
        return step

    turn = jnp.where(late, 0, deep * q - 1)

    def inner_step(m, carry):
        k, i = m // q, lax.rem(m, q)
        s, c = early_chunk(k)

        @pl.when(m == 0)
        def _():
            flow_local(0).wait()

        @pl.when(m == deep * q)
        def _():
            settle(fext.at[:, pl.ds(0, (ranks - 1) * per), body], lf_sem.at[1])

        @pl.when(i == 0)
        def _():
            early_local(k).wait()

        @pl.when(jnp.logical_or(late, m > 0))
        def _():
            advance_inner(s, c, i)

            @pl.when(m == 0)
            def _():
                pl.semaphore_wait(barrier, cross + cores - 1 + 2 * cores)

            inner_copy(s, c, i).start()

        @pl.when(m == turn)
        def _():
            if cores > 1:
                @pl.when(late)
                def _():
                    pl.semaphore_signal(
                        ready, inc=1, device_id={"tracer": partner}, device_id_type=MESH
                    )

                @pl.when(jnp.logical_not(late))
                def _():
                    pl.semaphore_wait(ready, 1)

            for copy in depth_edges():
                copy.start()
            lax.fori_loop(0, cross, start_edges(in_cross), 0)

        return carry

    lax.fori_loop(0, early * q, inner_step, 0)
    lax.fori_loop(cross, cross * nc, start_edges(in_cross), 0)
    for s in range(ranks):
        rest_local(s).start()

    @pl.when(jnp.logical_not(late))
    def _():
        raw_copy().wait_recv()
        for copy in raw_edges():
            copy.start()

    lax.fori_loop(0, cores * nc, start_edges(in_near), 0)
    for copy in heat_edges():
        copy.start()
    th_local.start()
    sun_local.start()
    tables[0].start()
    tables[2].start()
    tables[0].wait()
    tables[2].wait()

    def invert(s, carry):
        who = jnp.int32(0)
        for t in range(count):
            who = jnp.where(eaten[t] == s, jnp.int32(t), who)
        eater[s] = who
        return carry

    lax.fori_loop(0, count, invert, 0)

    settle(dext.at[pl.ds(0, 2 * EDGE)], s_recv.at[1])

    def outer_step(k, carry):
        s, c = edge_chunk(k)

        @pl.when(s == 0)
        def _():
            wait_edges(c, cross * q)

        def sides(i, carry):
            advance_outer(s, c, i)
            return carry

        given = jnp.logical_and(jnp.logical_not(late), k == 0)
        lax.fori_loop(jnp.where(given, 1, 0), q, sides, 0)

        @pl.when(jnp.logical_not(given))
        def _():
            for side in range(2):
                outer_copy(s, c, side).start()

        if q > 1:
            @pl.when(given)
            def _():
                for side in range(2):
                    outer_copy(s, c, side, 1).start()

        return carry

    lax.fori_loop(0, early, outer_step, 0)

    settle(ext.at[:, pl.ds(0, nl - early * q), body], l_sem.at[early])

    def away_step(m, carry):
        far = m < cross * nc
        k = m - cross * nc
        s = jnp.where(far, lax.rem(m, cross), cross + k // nc)
        c = jnp.where(far, m // cross, lax.rem(k, nc))

        @pl.when(jnp.logical_and(far, jnp.logical_and(s == 0, c >= deep)))
        def _():
            wait_edges(c, cross * q)

        @pl.when(jnp.logical_and(jnp.logical_not(far), c == 0))
        def _():
            wait_edges(nc + s - cross, per)

        @pl.when(jnp.logical_or(s > 0, c >= deep))
        def _():
            advance(s, c, put_adv)

            @pl.when(m != cross * nc - 1)
            def _():
                block_copy(s, c).start()

        return carry

    lax.fori_loop(cross, (ranks - 1) * nc, away_step, 0)

    wait_edges(own_group, q)

    @pl.when(jnp.logical_not(late))
    def _():
        giver = lax.rem(a + chips - 1, chips) * cores

        def put_given(t, lev, kept, c):
            cells[giver * nt + t, 0, kept] = c

        settle(raw.at[:, pl.ds(0, 2 * EDGE)], r_recv.at[1])
        advect(r * per, r, 0, full, PAD, 0, rows, put_given, lambda t: raw[t], giver)

    def own_step(c, carry):
        @pl.when(c > 0)
        def _():
            wait_edges(own_group + c, q)

        advance(ranks - 1, c, put_cells)
        return carry

    lax.fori_loop(0, nc, own_step, 0)

    above = jnp.zeros((rows, width), jnp.float32)
    for place in range(ranks):
        pre[place // cores, place % cores] = above
        above = above + tot[place]
    if cores > 1:
        part_copy().start()
        part_copy().wait()
        for k in range(chips):
            joined[k] = pre[k, b] + part[k]
    else:
        for k in range(chips):
            joined[k] = pre[k, b]
    for k in range(1, chips):
        @pl.when(gets_over(k))
        def _():
            over_copy(k).start()

    block_copy(cross - 1, nc - 1).start()

    th_local.wait()
    sun_local.wait()
    settle(hext.at[:, pl.ds(0, 2 * EDGE)], s_recv.at[0])
    lane = lane_index((full, width))
    coriolis = coriolis_base + beta_plane * lane.astype(jnp.float32) / width

    def momentum(i, carry):
        lev = r * per + i
        u, v, heat_ext = fext[0, lev], fext[1, lev], hext[i]
        wet = jnp.where(lev < dext[...], 1.0, 0.0)
        v_east, u_west = east(v), west(u)
        v_bar = 0.25 * (v + v_east + south(v) + south(v_east))
        u_bar = 0.25 * (u + u_west + north(u) + north(u_west))
        new_u = u + step_duration * (
            coriolis * v_bar - gravity * (east(heat_ext) - heat_ext) + viscosity * laplacian(u)
        )
        new_v = v + step_duration * (
            -coriolis * u_bar - gravity * (north(heat_ext) - heat_ext) + viscosity * laplacian(v)
        )
        vel[0, i] = (wet * east(wet) * new_u)[PAD:PAD + rows]
        vel[1, i] = (wet * north(wet) * new_v)[PAD:PAD + rows]
        warmer = heat_ext + step_duration * spreading_coefficient * laplacian(heat_ext)
        heat[i] = warmer[PAD:PAD + rows]
        return carry

    lax.fori_loop(0, per, momentum, 0)

    depth = dext[PAD:PAD + rows].astype(jnp.float32)
    aux[2] = depth
    scale = column_optical / nl
    clear = (r * per).astype(jnp.float32) * water_clear

    @pl.when(r == 0)
    def _():
        aux[0] = jnp.zeros((rows, width), jnp.float32)

    @pl.when(r > 0)
    def _():
        above = joined[a]
        for k in range(1, chips):
            over_copy(k).wait_recv()
            above = above + over[k - 1]
        aux[0] = (above + clear) * scale

    def react_chunk(c, carry):
        @pl.when(c == 0)
        def _():
            wait_first()

        @pl.when(c > 0)
        def _():
            wait_blocks(c)

        def one_level(j, carry):
            i = c * q + j

            def put(t, x):
                cells[t, i] = x

            level = (r * per + i).astype(jnp.float32)
            wet, caught, below = react_level(
                count, level, aux[2], aux[1], aux[0], cells, i,
                eaten, eater, att, rate, scale, sat, pull, put,
            )
            aux[0] = below
            heat[i] = wet * (heat[i] + warming_coefficient * (caught * wet))
            return carry

        lax.fori_loop(0, q, one_level, 0)
        return carry

    lax.fori_loop(0, nc - 1, react_chunk, 0)

    settle(edge_rows(nl), edge_send.at[0])
    settle(th.at[:, pl.ds(0, 2 * EDGE)], edge_send.at[1])
    settle(dep.at[pl.ds(0, 2 * EDGE)], edge_send.at[2])
    for k in range(1, chips):
        @pl.when(gets_over(k))
        def _():
            over_copy(k).wait_send()

    settle(adv.at[:, pl.ds(0, (ranks - 1) * per - early * q)], d_send.at[0])
    for pieces, mask in ((early * q, late), (early * q - 1, jnp.logical_not(late))):
        @pl.when(mask)
        def _():
            settle(ext.at[:, pl.ds(0, pieces), pl.ds(0, 2 * EDGE)], d_send.at[2])
            settle(ext.at[:, pl.ds(0, pieces), inner], d_send.at[1])

    @pl.when(jnp.logical_not(late))
    def _():
        raw_copy().wait_send()
        settle(raw.at[:, pl.ds(0, 2 * EDGE)], r_send.at[1])

    wait_blocks(nc - 1)


def finish_kernel(
    levels, q,
    cells, vel, heat, aux, eaten_in, att_in, rate_in,
    out, vel_out, temp_out,
    eaten, att, rate, last, warm, sat, pull, eater, sem, t_sem,
):
    count, per = cells.shape[:2]
    r = lax.axis_index("tracer")
    done = per - q
    scale = column_optical / levels
    copies = [
        pltpu.make_async_copy(cells.at[:, pl.ds(0, done)], out.at[:, pl.ds(0, done)], sem.at[0]),
        pltpu.make_async_copy(vel, vel_out, sem.at[1]),
        pltpu.make_async_copy(heat.at[pl.ds(0, done)], temp_out.at[pl.ds(0, done)], sem.at[2]),
    ]
    tables = [
        pltpu.make_async_copy(src, dst, t_sem.at[k])
        for k, (src, dst) in enumerate(((eaten_in, eaten), (att_in, att), (rate_in, rate)))
    ]
    for copy in tables + copies:
        copy.start()
    for copy in tables:
        copy.wait()
    for t in range(count):
        eater[eaten[t]] = t

    def level_copy(j):
        return pltpu.make_async_copy(last.at[j], out.at[:, done + j], sem.at[4])

    def one_level(j, tau):
        def put(t, x):
            last[j, t] = x

        level = (r * per + done + j).astype(jnp.float32)
        wet, caught, below = react_level(
            count, level, aux[2], aux[1], tau, cells, done + j,
            eaten, eater, att, rate, scale, sat, pull, put,
        )
        warm[j] = wet * (heat[done + j] + warming_coefficient * (caught * wet))
        level_copy(j).start()
        return below

    lax.fori_loop(0, q, one_level, aux[0])
    warm_copy = pltpu.make_async_copy(warm, temp_out.at[pl.ds(done, q)], sem.at[3])
    warm_copy.start()
    for copy in copies:
        copy.wait()
    pltpu.make_async_copy(last, last, sem.at[4]).wait()
    warm_copy.wait()


def solution(mesh):
    tiles, ranks = mesh.shape["tile"], mesh.shape["tracer"]
    cores = 2 if ranks % 2 == 0 else 1

    def on_device(
        species_amounts,
        face_currents,
        thermal_anomaly,
        layer_total_per_profile,
        consumed_species,
        attenuation_factor,
        intake_speedup,
        incoming_sunshine,
    ):
        nt, nl, rows, width = species_amounts.shape
        per = nl // ranks
        q = 2 if per % 2 == 0 else 1
        nc = per // q
        count = ranks * nt
        cross = ranks - cores
        chips = ranks // cores
        deep = min(DEEP, nc - 1)
        full = rows + PAD
        f32 = jnp.float32
        any_space = pl.BlockSpec(memory_space=pl.ANY)
        vmem = pl.BlockSpec(memory_space=pltpu.VMEM)
        dma = pltpu.SemaphoreType.DMA
        cells, vel, heat, aux = pl.pallas_call(
            functools.partial(transport_kernel, tiles, ranks, cores, q, deep),
            out_shape=(
                pltpu.VMEM((count, per, rows, width), f32),
                pltpu.VMEM((2, per, rows, width), f32),
                pltpu.VMEM((per, rows, width), f32),
                pltpu.VMEM((3, rows, width), f32),
            ),
            in_specs=[any_space] * 8,
            out_specs=(vmem, vmem, vmem, vmem),
            scratch_shapes=[
                pltpu.SMEM((count,), jnp.int32),
                pltpu.SMEM((count,), f32),
                pltpu.SMEM((count,), f32),
                pltpu.VMEM((nt, nl, full, width), f32),
                pltpu.VMEM((2, nl, full, width), f32),
                pltpu.VMEM((per, full, width), f32),
                pltpu.VMEM((full, width), jnp.int32),
                pltpu.VMEM((nt, nl, rows, width), f32),
                pltpu.VMEM((ranks, rows, width), f32),
                pltpu.VMEM((chips, cores, rows, width), f32),
                pltpu.VMEM((chips, rows, width), f32),
                pltpu.VMEM((chips, rows, width), f32),
                pltpu.VMEM((chips, rows, width), f32),
                pltpu.VMEM((count, rows, width), f32),
                pltpu.VMEM((count, rows, width), f32),
                pltpu.SMEM((count,), jnp.int32),
                pltpu.VMEM((nt, full, width), f32),
                dma((3,)), dma((2 * nc + cores - 1,)), dma((2,)),
                dma((3,)), dma((nc + 1,)), dma((chips,)), dma((chips,)),
                dma((deep + cross,)), dma((2,)), dma((3,)), dma((3,)),
                dma((2,)), dma((2,)), pltpu.SemaphoreType.REGULAR,
            ],
            compiler_params=pltpu.CompilerParams(
                collective_id=0, has_side_effects=True, vmem_limit_bytes=48 << 20
            ),
            name="transport",
        )(
            *(pltpu.with_memory_space_constraint(x, HBM) for x in (
                species_amounts, face_currents, thermal_anomaly,
                layer_total_per_profile, incoming_sunshine,
                consumed_species, attenuation_factor, intake_speedup,
            ))
        )
        return pl.pallas_call(
            functools.partial(finish_kernel, nl, q),
            out_shape=(
                jax.ShapeDtypeStruct((count, per, rows, width), f32),
                jax.ShapeDtypeStruct((2, per, rows, width), f32),
                jax.ShapeDtypeStruct((per, rows, width), f32),
            ),
            in_specs=[vmem] * 4 + [any_space] * 3,
            out_specs=(any_space, any_space, any_space),
            scratch_shapes=[
                pltpu.SMEM((count,), jnp.int32),
                pltpu.SMEM((count,), f32),
                pltpu.SMEM((count,), f32),
                pltpu.VMEM((q, count, rows, width), f32),
                pltpu.VMEM((q, rows, width), f32),
                pltpu.VMEM((count, rows, width), f32),
                pltpu.VMEM((count, rows, width), f32),
                pltpu.SMEM((count,), jnp.int32),
                dma((5,)), dma((3,)),
            ],
            compiler_params=pltpu.CompilerParams(vmem_limit_bytes=32 << 20),
            name="finish",
        )(
            cells, vel, heat, aux,
            consumed_species, attenuation_factor, intake_speedup,
        )

    return jax.shard_map(
        on_device,
        mesh=mesh,
        in_specs=(
            P(("groups", "tracer"), None, "tile", None),
            P(None, "groups", "tile", None),
            P(("groups", "tracer"), "tile", None),
            P(("groups", "tile"), None),
            P(),
            P(),
            P(),
            P(("groups", "tile"), None),
        ),
        out_specs=(
            P("groups", "tracer", "tile", None),
            P(None, ("groups", "tracer"), "tile", None),
            P(("groups", "tracer"), "tile", None),
        ),
        check_vma=False,
    )
```
